16 devices in a mesh: dp: 2 (over y, z), tp: 8 (over x, core).
Axes of the slice: x: 4, y: 2, z: 1, core: 2. Of those that a mesh axis runs over, the one named last changes fastest.
The devices are a block of a 4x4x8 slice.
Arguments:
- x_steps: bfloat16 [4, 1024, 512], P(None, 'dp'), parts along dimension 1
- conv_state: bfloat16 [1024, 1024, 3], P('dp', 'tp'), parts along dimension 0
- ssm_state: float32 [1024, 1024, 16], P('dp', 'tp'), parts along dimension 0
- expert_ids: int32 [4, 1024, 1], P(None, 'dp'), parts along dimension 1
- g_in: bfloat16 [512], replicated
- w_in: bfloat16 [512, 2, 1024], P(None, None, 'tp')
- conv_w: bfloat16 [1024, 4], P('tp')
- conv_b: bfloat16 [1024], P('tp')
- w_xp: bfloat16 [1024, 64], P('tp')
- g_dt: bfloat16 [32], replicated
- g_b: bfloat16 [16], replicated
- g_c: bfloat16 [16], replicated
- w_dt: bfloat16 [32, 1024], P(None, 'tp')
- b_dt: bfloat16 [1024], P('tp')
- a_log: float32 [1024, 16], P('tp')
- d_skip: float32 [1024], P('tp')
- w_out: bfloat16 [1024, 512], P('tp')
- g_ff: bfloat16 [512], replicated
- w_router: bfloat16 [512, 16], replicated
- w_gate: bfloat16 [16, 512, 2048], P(None, None, 'tp')
- w_up: bfloat16 [16, 512, 2048], P(None, None, 'tp')
- w_down: bfloat16 [16, 2048, 512], P(None, 'tp')
Outputs:
- output 1: bfloat16 [4, 1024, 512], P(None, 'dp'), parts along dimension 1
- output 2: bfloat16 [1024, 1024, 3], P('dp', 'tp'), parts along dimension 0
- output 3: float32 [1024, 1024, 16], P('dp', 'tp'), parts along dimension 0
There are 2 independent parts. The reference program is written for one: setup_inputs(seed, part) draws one part's arguments, and reference() takes and returns one part's arrays. A program takes and returns all parts, laid end to end along the dimension named above; an argument that names none is the same for every part.
All inputs are finite; a program needn't handle non-finite values.
Results may differ from the reference program's by a relative error of at most 0.0159064.
Values are sent between devices in bfloat16 or wider.
A program may use at most 768 MiB of HBM per device.

```python
import jax
import jax.numpy as jnp
from jax import lax

D_MODEL = 512
INNER = 1024
STATE_DIM = 16
DT_RANK = 32
FFN_DIM = 2048
EXPERTS = 16
TOP_K = 1
BATCH_SIZE = 512
NUM_STEPS = 4
CONV_WIDTH = 4
EPSILON = 1e-6


def gauss_draw(rng_key, arr_shape, std_scale):
    return jax.random.normal(rng_key, arr_shape, jnp.float32) * std_scale


def range_draw(rng_key, arr_shape, lower_end, upper_end):
    return jax.random.uniform(rng_key, arr_shape, jnp.float32, lower_end, upper_end)


def draw_routes(rng_key):
    key_jitter, key_skew = jax.random.split(rng_key)
    route_jitter = jax.random.randint(key_jitter, (NUM_STEPS, BATCH_SIZE, EXPERTS), 0, 64)
    expert_skew = jax.random.randint(key_skew, (EXPERTS,), 0, 96)
    cover_mask = (jnp.arange(NUM_STEPS)[:, None, None] == 0) & (jnp.arange(BATCH_SIZE)[None, :, None] == jnp.arange(EXPERTS)[None, None, :])
    scores = route_jitter + expert_skew[None, None, :] + jnp.where(cover_mask, 1000, 0)
    scores = scores * EXPERTS + jnp.arange(EXPERTS)[None, None, :]
    return lax.top_k(scores, TOP_K)[1].astype(jnp.int32)


def setup_inputs(seed: int = 0, part: int = 0) -> dict:
    base_key = jax.random.key(seed)
    part_keys = jax.random.split(jax.random.fold_in(base_key, part), 4)
    shared_keys = jax.random.split(base_key, 18)
    return {
        "x_steps": gauss_draw(part_keys[0], (NUM_STEPS, BATCH_SIZE, D_MODEL), 1.0).astype(jnp.bfloat16),
        "conv_state": gauss_draw(part_keys[1], (BATCH_SIZE, INNER, CONV_WIDTH - 1), 1.0).astype(jnp.bfloat16),
        "ssm_state": gauss_draw(part_keys[2], (BATCH_SIZE, INNER, STATE_DIM), 0.2),
        "expert_ids": draw_routes(part_keys[3]),
        "g_in": range_draw(shared_keys[0], (D_MODEL,), 0.4, 1.6).astype(jnp.bfloat16),
        "w_in": gauss_draw(shared_keys[1], (D_MODEL, 2, INNER), D_MODEL ** -0.5).astype(jnp.bfloat16),
        "conv_w": gauss_draw(shared_keys[2], (INNER, CONV_WIDTH), 0.5).astype(jnp.bfloat16),
        "conv_b": gauss_draw(shared_keys[3], (INNER,), 0.5).astype(jnp.bfloat16),
        "w_xp": gauss_draw(shared_keys[4], (INNER, DT_RANK + 2 * STATE_DIM), INNER ** -0.5).astype(jnp.bfloat16),
        "g_dt": range_draw(shared_keys[5], (DT_RANK,), 0.4, 1.6).astype(jnp.bfloat16),
        "g_b": range_draw(shared_keys[6], (STATE_DIM,), 0.4, 1.6).astype(jnp.bfloat16),
        "g_c": range_draw(shared_keys[7], (STATE_DIM,), 0.4, 1.6).astype(jnp.bfloat16),
        "w_dt": gauss_draw(shared_keys[8], (DT_RANK, INNER), 0.8 * DT_RANK ** -0.5).astype(jnp.bfloat16),
        "b_dt": (gauss_draw(shared_keys[9], (INNER,), 0.3) - 2.25).astype(jnp.bfloat16),
        "a_log": range_draw(shared_keys[10], (INNER, STATE_DIM), -0.7, 0.7),
        "d_skip": range_draw(shared_keys[11], (INNER,), 0.5, 1.5),
        "w_out": gauss_draw(shared_keys[12], (INNER, D_MODEL), INNER ** -0.5).astype(jnp.bfloat16),
        "g_ff": range_draw(shared_keys[13], (D_MODEL,), 0.4, 1.6).astype(jnp.bfloat16),
        "w_router": gauss_draw(shared_keys[14], (D_MODEL, EXPERTS), D_MODEL ** -0.5).astype(jnp.bfloat16),
        "w_gate": gauss_draw(shared_keys[15], (EXPERTS, D_MODEL, FFN_DIM), D_MODEL ** -0.5).astype(jnp.bfloat16),
        "w_up": gauss_draw(shared_keys[16], (EXPERTS, D_MODEL, FFN_DIM), D_MODEL ** -0.5).astype(jnp.bfloat16),
        "w_down": gauss_draw(shared_keys[17], (EXPERTS, FFN_DIM, D_MODEL), EXPERTS * (TOP_K * FFN_DIM) ** -0.5).astype(jnp.bfloat16),
    }


def rms_norm(tensor_in, gain_vec):
    in_f32 = tensor_in.astype(jnp.float32)
    return in_f32 * lax.rsqrt(jnp.mean(in_f32 * in_f32, axis=-1, keepdims=True) + EPSILON) * gain_vec.astype(jnp.float32)


def reference(x_steps, conv_state, ssm_state, expert_ids, g_in, w_in, conv_w, conv_b, w_xp, g_dt, g_b, g_c, w_dt, b_dt, a_log, d_skip, w_out, g_ff, w_router, w_gate, w_up, w_down):
    a_mat = -jnp.exp(a_log)
    w_in_flat = w_in.reshape(D_MODEL, 2 * INNER)

    def expert_body(moe_acc, expert_w):
        w_gate_e, w_up_e, w_down_e, coef_e, moe_in = expert_w
        gate_h = jnp.dot(moe_in, w_gate_e, preferred_element_type=jnp.float32)
        up_h = jnp.dot(moe_in, w_up_e, preferred_element_type=jnp.float32)
        hidden = (jax.nn.silu(gate_h) * up_h).astype(jnp.bfloat16)
        return moe_acc + coef_e[:, None] * jnp.dot(hidden, w_down_e, preferred_element_type=jnp.float32), None

    def one_step(state_pair, step_in):
        conv_st, ssm_st = state_pair
        x_now, ids_now = step_in
        norm_in = rms_norm(x_now, g_in).astype(jnp.bfloat16)
        proj_xz = jnp.dot(norm_in, w_in_flat, preferred_element_type=jnp.float32).astype(jnp.bfloat16).reshape(BATCH_SIZE, 2, INNER)
        x_inner = proj_xz[:, 0]
        z_gate = proj_xz[:, 1]
        conv_win = jnp.concatenate([conv_st, x_inner[:, :, None]], axis=2)
        conv_pre = jnp.sum(conv_win.astype(jnp.float32) * conv_w.astype(jnp.float32)[None], axis=2) + conv_b.astype(jnp.float32)[None]
        x_conv = jax.nn.silu(conv_pre).astype(jnp.bfloat16)
        proj_sum = jnp.dot(x_conv, w_xp, preferred_element_type=jnp.float32)
        dt_low = rms_norm(proj_sum[:, :DT_RANK], g_dt)
        b_vec = rms_norm(proj_sum[:, DT_RANK:DT_RANK + STATE_DIM], g_b)
        c_vec = rms_norm(proj_sum[:, DT_RANK + STATE_DIM:], g_c)
        delta_t = jax.nn.softplus(jnp.dot(dt_low.astype(jnp.bfloat16), w_dt, preferred_element_type=jnp.float32) + b_dt.astype(jnp.float32)[None])
        xc_f32 = x_conv.astype(jnp.float32)
        new_ssm = jnp.exp(delta_t[:, :, None] * a_mat[None]) * ssm_st + (delta_t * xc_f32)[:, :, None] * b_vec[:, None, :]
        y_gated = (jnp.sum(new_ssm * c_vec[:, None, :], axis=2) + d_skip[None] * xc_f32) * jax.nn.silu(z_gate.astype(jnp.float32))
        mix_out = jnp.dot(y_gated.astype(jnp.bfloat16), w_out, preferred_element_type=jnp.float32)
        resid_mid = (x_now.astype(jnp.float32) + mix_out).astype(jnp.bfloat16)
        moe_in = rms_norm(resid_mid, g_ff).astype(jnp.bfloat16)
        route_prob = jax.nn.softmax(jnp.dot(moe_in, w_router, preferred_element_type=jnp.float32), axis=-1)
        pick_count = jnp.sum((ids_now[:, :, None] == jnp.arange(EXPERTS)[None, None, :]).astype(jnp.float32), axis=1)
        combine_w = route_prob * pick_count
        moe_stack = jnp.broadcast_to(moe_in[None], (EXPERTS, BATCH_SIZE, D_MODEL))
        moe_out, _ = lax.scan(expert_body, jnp.zeros((BATCH_SIZE, D_MODEL), jnp.float32), (w_gate, w_up, w_down, combine_w.T, moe_stack))
        out_now = (resid_mid.astype(jnp.float32) + moe_out).astype(jnp.bfloat16)
        return (conv_win[:, :, 1:], new_ssm), out_now

    final_pair, y_steps = lax.scan(one_step, (conv_state, ssm_state), (x_steps, expert_ids))
    return y_steps, final_pair[0], final_pair[1]
```

```python
import functools
import math

import jax
import jax.numpy as jnp
from jax import lax
from jax.experimental import pallas as pl
from jax.experimental.pallas import tpu as pltpu
from jax.sharding import PartitionSpec as P

EPSILON = 1e-6
F32 = jnp.float32
BF16 = jnp.bfloat16
CHUNK_ROWS = 64
GROUP = 4
LOG2E = math.log2(math.e)


class Lazy:
    def __init__(self, **makers):
        self.makers = makers

    def __getitem__(self, name):
        return self.makers[name]()


def silu(v):
    return v * jax.nn.sigmoid(v)


def nt_dot(lhs, rhs_t):
    return lax.dot_general(lhs, rhs_t, (((1,), (1,)), ((), ())), preferred_element_type=F32)


def mm(lhs, rhs):
    return jnp.dot(lhs, rhs, preferred_element_type=F32)


def layer_kernel(
    x_hbm, h_hbm, ids_hbm, wg_hbm, wu_hbm, wd_hbm, w_out_hbm,
    conv_ref, w_in_ref, vec_ref, chan_ref, w_xp_ref, w_dt_ref, a_log_ref, w_router_ref,
    y_hbm, h_out_hbm, conv_out_ref,
    xbuf, hbuf, idbuf, wg, wu, wd, w_xp2, w_dt2, a2,
    zbuf, xcbuf, dbuf, pnbuf,
    p_part, p_r0, p_s1, p_r1, p_s2, p_r2, p_sum,
    yg_all, wo_all, ubuf, mbuf, qbuf, acc, prob,
    y_part, y_r0, y_s1, y_r1, y_s2, y_r2, ybuf,
    in_sem, h_sem, out_sem, p_send, p_recv, y_send, y_recv, g_send, g_recv,
):
    steps, batch, d_model = x_hbm.shape
    state_dim, inner = a_log_ref.shape
    dt_rank = w_dt_ref.shape[0]
    p_dim = w_xp_ref.shape[0]
    experts = wg_hbm.shape[0]
    f_loc = wg_hbm.shape[2]
    rows = CHUNK_ROWS
    chunks = batch // rows
    tokens = steps * rows
    half_rows = tokens // 2

    tp = lax.axis_index("tp")
    core = tp % 2
    chip = tp // 2
    other = 1 - core
    chip_a = chip + 1 - 2 * (chip % 2)
    chip_b = 3 - chip
    chip_far = (chip + 2) % 4
    mate = {"tp": 2 * chip + other}
    peer_a = {"tp": 2 * chip_a + core}
    peer_b = {"tp": 2 * chip_b + core}

    def copy_to(src, dst, send_sem, recv_sem, peer):
        return pltpu.make_async_remote_copy(
            src_ref=src, dst_ref=dst, send_sem=send_sem, recv_sem=recv_sem, device_id=peer, device_id_type=pl.DeviceIdType.MESH
        )

    in_copies = [
        pltpu.make_async_copy(x_hbm, xbuf, in_sem.at[0]),
        pltpu.make_async_copy(ids_hbm, idbuf, in_sem.at[1]),
        pltpu.make_async_copy(wg_hbm, wg, in_sem.at[2]),
        pltpu.make_async_copy(wu_hbm, wu, in_sem.at[3]),
        pltpu.make_async_copy(wd_hbm, wd, in_sem.at[4]),
    ]
    h_in = pltpu.make_async_copy(h_hbm, hbuf, h_sem.at[0])
    wo_in = pltpu.make_async_copy(w_out_hbm, wo_all.at[pl.ds(pl.multiple_of((core * 4 + chip) * inner, inner), inner), :], in_sem.at[5])
    in_copies[0].start()
    wo_in.start()
    h_in.start()
    for cp in in_copies[1:]:
        cp.start()

    barrier = pltpu.get_barrier_semaphore()
    for peer in (mate, peer_a, peer_b):
        pl.semaphore_signal(barrier, inc=1, device_id=peer, device_id_type=pl.DeviceIdType.MESH)
    pl.semaphore_wait(barrier, 3)

    def wo_block(c, x):
        return wo_all, lambda lo, n: (pl.ds(pl.multiple_of((c * 4 + x) * inner + lo, n), n), slice(None)), inner

    def yg_block(ch):
        def block(c, x):
            col = pl.ds(pl.multiple_of((c * 4 + x) * inner, inner), inner)
            return yg_all, lambda lo, n: (ch, pl.ds(lo, n), col), tokens
        return block

    def ag_copies(block, k):
        def cut(c, x, part=None):
            ref, index, n = block(c, x)
            if part is None:
                return ref.at[index(0, n)]
            return ref.at[index(part * (n // 2), n // 2)]

        def make(idx, src, peer, part=None):
            return copy_to(cut(core, src, part), cut(core, src, part), g_send.at[k, idx], g_recv.at[k, idx], peer)

        def take(idx, c, src, part=None):
            return copy_to(cut(c, src, part), cut(c, src, part), g_send.at[k, idx], g_recv.at[k, idx], mate)

        sends = Lazy(
            own_a=lambda: make(0, chip, peer_a), own_b=lambda: make(1, chip, peer_b),
            fwd_b=lambda: make(2, chip_a, peer_b, 0), fwd_a=lambda: make(3, chip_b, peer_a, 1),
            m_own=lambda: make(4, chip, mate), m_a=lambda: make(5, chip_a, mate),
            m_b=lambda: make(6, chip_b, mate), m_far=lambda: make(7, chip_far, mate),
        )
        recvs = Lazy(
            a=lambda: take(0, core, chip_a), b=lambda: take(1, core, chip_b),
            far0=lambda: take(2, core, chip_far, 0), far1=lambda: take(3, core, chip_far, 1),
            m_own=lambda: take(4, other, chip), m_a=lambda: take(5, other, chip_a),
            m_b=lambda: take(6, other, chip_b), m_far=lambda: take(7, other, chip_far),
        )
        return sends, recvs

    def ag_first(block, k):
        s, _ = ag_copies(block, k)
        s["own_a"].start()
        s["own_b"].start()
        s["m_own"].start()

    def ag_relay(block, k):
        s, r = ag_copies(block, k)
        r["a"].wait_recv()
        s["fwd_b"].start()
        s["m_a"].start()
        r["b"].wait_recv()
        s["fwd_a"].start()
        s["m_b"].start()

    def ag_far(block, k):
        s, r = ag_copies(block, k)
        r["far0"].wait_recv()
        r["far1"].wait_recv()
        s["m_far"].start()

    def ag_done(block, k):
        _, r = ag_copies(block, k)
        for name in ("m_own", "m_a", "m_b", "m_far"):
            r[name].wait_recv()

    def ag_drain(block, k):
        s, _ = ag_copies(block, k)
        for name in ("own_a", "own_b", "fwd_b", "fwd_a", "m_own", "m_a", "m_b", "m_far"):
            s[name].wait_send()

    def ar_copies(part, r0, s1, r1, s2, r2, total, send, recv, ch, n):
        q = n // 4
        keep = pl.ds(pl.multiple_of(core * (n // 2), n // 2), n // 2)
        give = pl.ds(pl.multiple_of(other * (n // 2), n // 2), n // 2)
        lo, hi = pl.ds(0, q), pl.ds(q, q)

        def make(idx, src, dst, peer):
            return copy_to(src, dst, send.at[ch, idx], recv.at[ch, idx], peer)

        return Lazy(
            swap=lambda: make(0, part.at[ch, give], r0.at[ch], mate),
            a1=lambda: make(1, s1.at[ch, lo], r1.at[ch, lo], peer_a), b1=lambda: make(2, s1.at[ch, hi], r1.at[ch, hi], peer_b),
            a2=lambda: make(3, s2.at[ch, lo], r2.at[ch, lo], peer_b), b2=lambda: make(4, s2.at[ch, hi], r2.at[ch, hi], peer_a),
            out=lambda: make(5, total.at[ch, keep], total.at[ch, keep], mate),
            back=lambda: make(5, total.at[ch, give], total.at[ch, give], mate),
        ), keep

    def p_ar(ch):
        return ar_copies(p_part, p_r0, p_s1, p_r1, p_s2, p_r2, p_sum, p_send, p_recv, ch, half_rows)

    def y_ar(ch):
        return ar_copies(y_part, y_r0, y_s1, y_r1, y_s2, y_r2, ybuf, y_send, y_recv, ch, tokens)

    def ar_one(cs, keep, part, r0, s1, ch):
        cs["swap"].wait_recv()
        s1[ch] = (part[ch, keep].astype(F32) + r0[ch].astype(F32)).astype(s1.dtype)
        cs["a1"].start()
        cs["b1"].start()

    def ar_two(cs, s1, r1, s2, ch):
        cs["a1"].wait_recv()
        cs["b1"].wait_recv()
        s2[ch] = (s1[ch].astype(F32) + r1[ch].astype(F32)).astype(s2.dtype)
        cs["a2"].start()
        cs["b2"].start()

    def p_one(ch):
        cs, keep = p_ar(ch)
        ar_one(cs, keep, p_part, p_r0, p_s1, ch)

    def p_two(ch):
        cs, _ = p_ar(ch)
        ar_two(cs, p_s1, p_r1, p_s2, ch)

    def p_three(ch):
        cs, keep = p_ar(ch)
        cs["a2"].wait_recv()
        cs["b2"].wait_recv()
        p_sum[ch, keep] = p_s2[ch] + p_r2[ch]
        cs["out"].start()

    def y_one(ch):
        cs, keep = y_ar(ch)
        ar_one(cs, keep, y_part, y_r0, y_s1, ch)

    def y_two(ch):
        cs, _ = y_ar(ch)
        ar_two(cs, y_s1, y_r1, y_s2, ch)

    def y_three(ch):
        cs, keep = y_ar(ch)
        cs["a2"].wait_recv()
        cs["b2"].wait_recv()
        moe_sum = y_s2[ch].astype(F32) + y_r2[ch].astype(F32)
        ybuf[ch, keep] = (ubuf[ch, keep].astype(F32) + moe_sum).astype(BF16)
        cs["out"].start()

    def y_out(ch):
        return [
            pltpu.make_async_copy(
                ybuf.at[ch, pl.ds(s * rows, rows)], y_hbm.at[s, pl.ds(pl.multiple_of(ch * rows, rows), rows)], out_sem.at[1 + s, ch]
            )
            for s in range(steps)
        ]

    def y_four(ch):
        cs, _ = y_ar(ch)
        cs["back"].wait_recv()
        for cp in y_out(ch):
            cp.start()

    def h_out(ch):
        n = rows * state_dim
        part = pl.ds(pl.multiple_of(ch * n, n), n)
        return pltpu.make_async_copy(hbuf.at[part], h_out_hbm.at[part], out_sem.at[0, ch])

    def chunk_rows(ch):
        return pl.ds(pl.multiple_of(ch * rows, rows), rows)

    def stage_in(ch):
        xf = xbuf[:, chunk_rows(ch), :].reshape(tokens, d_model).astype(F32)
        scale = lax.rsqrt(jnp.mean(xf * xf, axis=-1, keepdims=True) + EPSILON)
        norm = (xf * scale * vec_ref[0:1, :]).astype(BF16)
        proj = mm(norm, w_in_ref[...]).astype(BF16)
        zbuf[ch] = proj[:, inner:]
        xi = proj[:, :inner]
        win = [conv_ref[j, chunk_rows(ch), :].astype(F32) for j in range(3)]
        win += [xi[s * rows:(s + 1) * rows].astype(F32) for s in range(steps)]
        for s in range(steps):
            pre = chan_ref[4:5, :]
            for j in range(4):
                pre = pre + win[s + j] * chan_ref[j:j + 1, :]
            lane = (s // 2) * inner
            xcbuf[ch, (s % 2) * rows:(s % 2 + 1) * rows, lane:lane + inner] = silu(pre).astype(BF16)
        for j in range(3):
            conv_out_ref[j, chunk_rows(ch), :] = xi[(j + 1) * rows:(j + 2) * rows]
        p_part[ch] = nt_dot(xcbuf[ch], w_xp2[...])
        cs, _ = p_ar(ch)
        cs["swap"].start()

    def stage_ssm(ch):
        cs, _ = p_ar(ch)
        cs["back"].wait_recv()
        p = p_sum[ch]
        lane = lax.broadcasted_iota(jnp.int32, p.shape, 1)
        sq = p * p
        mean = jnp.zeros_like(p)
        for base in (0, p_dim):
            for lo, n in ((0, dt_rank), (dt_rank, state_dim), (dt_rank + state_dim, state_dim)):
                inside = (lane >= base + lo) & (lane < base + lo + n)
                total = jnp.sum(jnp.where(inside, sq, 0.0), axis=-1, keepdims=True) * (1.0 / n)
                mean = jnp.where(inside, total, mean)
        pn = p * lax.rsqrt(mean + EPSILON) * chan_ref[7:8, :]
        pnbuf[...] = pn
        pre = mm(pn.astype(BF16), w_dt2[...])
        bias = chan_ref[5:6, :]
        pre = pre + jnp.concatenate([bias, bias], axis=1)
        dbuf[...] = jnp.maximum(pre, 0.0) + jnp.log1p(jnp.exp(-jnp.abs(pre)))
        my_col = pl.ds(pl.multiple_of((core * 4 + chip) * inner, inner), inner)
        tile = 16

        def tile_body(bt, carry):
            r0 = pl.multiple_of(bt * tile, tile)
            d, dx, y, pns = [], [], [], []
            for s in range(steps):
                at = pl.ds(pl.multiple_of((s % 2) * rows + r0, tile), tile)
                cols = slice((s // 2) * inner, (s // 2 + 1) * inner)
                ds_ = dbuf[at, cols]
                xc = xcbuf[ch, at, cols].astype(F32)
                d.append(ds_)
                dx.append(ds_ * xc)
                y.append(chan_ref[6:7, :] * xc)
                pns.append(pnbuf[at, :])
            for n in range(state_dim):
                where = pl.ds((ch * rows + r0) * state_dim + n, tile, stride=state_dim)
                h = hbuf[where, :]
                a_n = a2[n:n + 1, :]
                for s in range(steps):
                    kb = (s // 2) * p_dim + dt_rank + n
                    kc = kb + state_dim
                    bvec = pns[s][:, kb:kb + 1]
                    cvec = pns[s][:, kc:kc + 1]
                    h = jnp.exp2(d[s] * a_n) * h + dx[s] * bvec
                    y[s] = y[s] + h * cvec
                hbuf[where, :] = h
            for s in range(steps):
                at = pl.ds(pl.multiple_of(s * rows + r0, tile), tile)
                z = zbuf[ch, at, :].astype(F32)
                yg_all[ch, at, my_col] = (y[s] * silu(z)).astype(BF16)
            return carry

        lax.fori_loop(0, rows // tile, tile_body, 0)
        h_out(ch).start()
        ag_first(yg_block(ch), ch)

    def stage_mid(ch):
        ag_done(yg_block(ch), ch)
        mix = mm(yg_all[ch], wo_all[...])
        xf = xbuf[:, chunk_rows(ch), :].reshape(tokens, d_model).astype(F32)
        u = (xf + mix).astype(BF16)
        ubuf[ch] = u
        uf = u.astype(F32)
        scale = lax.rsqrt(jnp.mean(uf * uf, axis=-1, keepdims=True) + EPSILON)
        m = (uf * scale * vec_ref[1:2, :]).astype(BF16)
        mbuf[...] = m
        logits = nt_dot(m, w_router_ref[...])
        peak = jnp.max(logits, axis=-1, keepdims=True)
        ex = jnp.exp(logits - peak)
        ids = idbuf[:, chunk_rows(ch), 0:experts].reshape(tokens, experts)
        hit = ids == lax.broadcasted_iota(jnp.int32, (tokens, experts), 1)
        chosen = jnp.sum(jnp.where(hit, ex, 0.0), axis=-1, keepdims=True) / jnp.sum(ex, axis=-1, keepdims=True)
        prob[...] = jnp.broadcast_to(chosen, prob.shape)

    def stage_experts(ch, g):
        m = mbuf[...]
        ids = idbuf[:, chunk_rows(ch), :].reshape(tokens, inner)
        ids = jnp.concatenate([ids] * (f_loc // inner), axis=1)
        for j in range(GROUP):
            e = g * GROUP + j
            q = silu(mm(m, wg[e])) * mm(m, wu[e])
            qbuf[:, j * f_loc:(j + 1) * f_loc] = jnp.where(ids == e, q, 0.0).astype(BF16)
        part = mm(qbuf[...], wd[g * GROUP * f_loc:(g + 1) * GROUP * f_loc, :])
        if g == 0:
            acc[...] = part
        elif g < experts // GROUP - 1:
            acc[...] += part
        else:
            total = acc[...] + part
            weight = jnp.concatenate([prob[...]] * (d_model // inner), axis=1)
            y_part[ch] = (total * weight).astype(BF16)
            cs, _ = y_ar(ch)
            cs["swap"].start()

    def when_chunk(ch, fn):
        pl.when((ch >= 0) & (ch < chunks))(lambda: fn(ch))

    def loop(n, body):
        def step(i, carry):
            body(i)
            return carry
        lax.fori_loop(0, n, step, 0)

    wo_in.wait()
    ag_first(wo_block, chunks)
    w_xp2[...] = jnp.zeros_like(w_xp2)
    w_dt2[...] = jnp.zeros_like(w_dt2)
    for k in range(2):
        w_xp2[k * p_dim:(k + 1) * p_dim, k * inner:(k + 1) * inner] = w_xp_ref[...]
        w_dt2[k * p_dim:k * p_dim + dt_rank, k * inner:(k + 1) * inner] = w_dt_ref[...]
    a2[...] = jnp.exp(a_log_ref[...]) * (-LOG2E)
    in_copies[0].wait()

    def first_body(t):
        stage_in(t)
        when_chunk(t - 2, p_one)

    loop(chunks, first_body)
    p_one(chunks - 2)
    p_one(chunks - 1)
    for ch in range(4):
        p_two(ch)
    ag_relay(wo_block, chunks)
    for ch in range(4, chunks):
        p_two(ch)
    for ch in range(3):
        p_three(ch)
    h_in.wait()

    def ssm_body(t):
        stage_ssm(t)
        when_chunk(t + 3, p_three)
        when_chunk(t - 4, lambda ch: ag_relay(yg_block(ch), ch))
        when_chunk(t - 6, lambda ch: ag_far(yg_block(ch), ch))

    loop(chunks, ssm_body)
    ag_far(wo_block, chunks)
    for cp in in_copies[1:]:
        cp.wait()
    ag_done(wo_block, chunks)

    def moe_body(t):
        stage_mid(t)
        for g in range(experts // GROUP):
            stage_experts(t, g)
            if g == 0:
                when_chunk(t + 4, lambda ch: ag_relay(yg_block(ch), ch))
                when_chunk(t - 2, y_two)
            elif g == 1:
                when_chunk(t + 2, lambda ch: ag_far(yg_block(ch), ch))
                when_chunk(t - 1, y_one)
            elif g == 2:
                when_chunk(t - 3, y_three)
            else:
                when_chunk(t - 4, y_four)

    loop(chunks, moe_body)
    last = chunks - 1
    y_two(last - 1)
    y_three(last - 2)
    y_one(last)
    y_four(last - 3)
    y_three(last - 1)
    y_two(last)
    y_four(last - 2)
    y_four(last - 1)
    y_three(last)
    y_four(last)

    def drain(ch):
        h_out(ch).wait()
        for cp in y_out(ch):
            cp.wait()
        ag_drain(yg_block(ch), ch)
        for cs, _ in (p_ar(ch), y_ar(ch)):
            for name in ("swap", "a1", "b1", "a2", "b2", "out"):
                cs[name].wait_send()

    loop(chunks, drain)
    ag_drain(wo_block, chunks)


def solution(mesh):
    act_spec = P(None, "dp", None)
    state_spec = P("dp", "tp", None)
    in_specs = (act_spec, state_spec, state_spec, act_spec, P(None), P(None, None, "tp"), P("tp", None), P("tp"), P("tp", None), P(None), P(None), P(None), P(None, "tp"), P("tp"), P("tp", None), P("tp"), P("tp", None), P(None), P(None, None), P(None, None, "tp"), P(None, None, "tp"), P(None, "tp", None))
    out_specs = (act_spec, state_spec, state_spec)

    def layer_steps(x_steps, conv_state, ssm_state, expert_ids, g_in, w_in, conv_w, conv_b, w_xp, g_dt, g_b, g_c, w_dt, b_dt, a_log, d_skip, w_out, g_ff, w_router, w_gate, w_up, w_down):
        steps, batch, d_model = x_steps.shape
        inner = w_in.shape[2]
        state_dim = a_log.shape[1]
        experts, _, f_loc = w_gate.shape
        p_dim = w_xp.shape[1]
        rows = CHUNK_ROWS
        chunks = batch // rows
        tokens = steps * rows
        group_inner = w_out.shape[0] * mesh.shape["tp"]

        w_in2 = w_in.reshape(d_model, 2 * inner)
        vec = jnp.stack([g_in, g_ff]).astype(F32)
        gains = jnp.concatenate([g_dt, g_b, g_c]).astype(F32)
        chan = jnp.concatenate([
            conv_w.T.astype(F32),
            jnp.stack([conv_b.astype(F32), b_dt.astype(F32), d_skip, jnp.concatenate([gains, gains])]),
        ])
        ids = jnp.broadcast_to(expert_ids, (steps, batch, inner))
        h_flat = jnp.swapaxes(ssm_state, 1, 2).reshape(batch * state_dim, inner)
        conv_t = jnp.transpose(conv_state, (2, 0, 1))

        any_spec = pl.BlockSpec(memory_space=pl.ANY)
        vmem_spec = pl.BlockSpec(memory_space=pltpu.VMEM)
        half = tokens // 2
        p_half = (chunks, half // 2, 2 * p_dim)
        y_half = (chunks, half, d_model)
        dma = pltpu.SemaphoreType.DMA
        scratch = [
            pltpu.VMEM(x_steps.shape, BF16),
            pltpu.VMEM(h_flat.shape, F32),
            pltpu.VMEM(ids.shape, jnp.int32),
            pltpu.VMEM(w_gate.shape, BF16),
            pltpu.VMEM(w_up.shape, BF16),
            pltpu.VMEM((experts * f_loc, d_model), BF16),
            pltpu.VMEM((2 * p_dim, 2 * inner), BF16),
            pltpu.VMEM((2 * p_dim, 2 * inner), BF16),
            pltpu.VMEM((state_dim, inner), F32),
            pltpu.VMEM((chunks, tokens, inner), BF16),
            pltpu.VMEM((chunks, half, 2 * inner), BF16),
            pltpu.VMEM((half, 2 * inner), F32),
            pltpu.VMEM((half, 2 * p_dim), F32),
            pltpu.VMEM((chunks, half, 2 * p_dim), F32),
            pltpu.VMEM(p_half, F32),
            pltpu.VMEM(p_half, F32),
            pltpu.VMEM(p_half, F32),
            pltpu.VMEM(p_half, F32),
            pltpu.VMEM(p_half, F32),
            pltpu.VMEM((chunks, half, 2 * p_dim), F32),
            pltpu.VMEM((chunks, tokens, group_inner), BF16),
            pltpu.VMEM((group_inner, d_model), BF16),
            pltpu.VMEM((chunks, tokens, d_model), BF16),
            pltpu.VMEM((tokens, d_model), BF16),
            pltpu.VMEM((tokens, GROUP * f_loc), BF16),
            pltpu.VMEM((tokens, d_model), F32),
            pltpu.VMEM((tokens, inner), F32),
            pltpu.VMEM((chunks, tokens, d_model), BF16),
            pltpu.VMEM(y_half, BF16),
            pltpu.VMEM(y_half, BF16),
            pltpu.VMEM(y_half, BF16),
            pltpu.VMEM(y_half, BF16),
            pltpu.VMEM(y_half, BF16),
            pltpu.VMEM((chunks, tokens, d_model), BF16),
            dma((6,)),
            dma((1,)),
            dma((1 + steps, chunks)),
            dma((chunks, 6)),
            dma((chunks, 6)),
            dma((chunks, 6)),
            dma((chunks, 6)),
            dma((chunks + 1, 8)),
            dma((chunks + 1, 8)),
        ]
        y, h_new, conv_new = pl.pallas_call(
            layer_kernel,
            out_shape=(
                jax.ShapeDtypeStruct(x_steps.shape, BF16),
                jax.ShapeDtypeStruct(h_flat.shape, F32),
                jax.ShapeDtypeStruct(conv_t.shape, BF16),
            ),
            in_specs=[any_spec] * 7 + [vmem_spec] * 8,
            out_specs=(any_spec, any_spec, vmem_spec),
            scratch_shapes=scratch,
            compiler_params=pltpu.CompilerParams(collective_id=0, has_side_effects=True, vmem_limit_bytes=60 * 1024 * 1024),
        )(x_steps, h_flat, ids, w_gate, w_up, w_down.reshape(experts * f_loc, d_model), w_out, conv_t, w_in2, vec, chan, w_xp.T, w_dt, a_log.T, w_router.T)
        h_new = jnp.swapaxes(h_new.reshape(batch, state_dim, inner), 1, 2)
        return y, jnp.transpose(conv_new, (1, 2, 0)), h_new

    return jax.shard_map(layer_steps, mesh=mesh, in_specs=in_specs, out_specs=out_specs, check_vma=False)
```

```python
import functools
import math

import jax
import jax.numpy as jnp
from jax import lax
from jax.experimental import pallas as pl
from jax.experimental.pallas import tpu as pltpu
from jax.sharding import PartitionSpec as P

EPSILON = 1e-6
F32 = jnp.float32
BF16 = jnp.bfloat16
CHUNK_ROWS = 64
GROUP = 4
LOG2E = math.log2(math.e)


class Lazy:
    def __init__(self, **makers):
        self.makers = makers

    def __getitem__(self, name):
        return self.makers[name]()


def silu(v):
    return v * jax.nn.sigmoid(v)


def nt_dot(lhs, rhs_t):
    return lax.dot_general(lhs, rhs_t, (((1,), (1,)), ((), ())), preferred_element_type=F32)


def mm(lhs, rhs):
    return jnp.dot(lhs, rhs, preferred_element_type=F32)


def layer_kernel(
    x_hbm, h_hbm, wg_hbm, wu_hbm, wd_hbm, w_out_hbm,
    ids_ref, conv_ref, w_in_ref, g_in_ref, g_ff_ref, conv_w_ref, conv_b_ref, b_dt_ref, d_skip_ref,
    g_dt_ref, g_b_ref, g_c_ref, w_xp_ref, w_dt_ref, a_log_ref, w_router_ref,
    y_ref, h_ref, conv_out_ref,
    xbuf, hbuf, idbuf, wg, wu, wd, w_in2, w_tmp, vec_ref, chan_ref, w_xp2, w_dt2, a2, spread,
    zbuf, xcbuf, dbuf, pnbuf, bbuf, cbuf,
    p_part, p_r0, p_s1, p_r1, p_s2, p_r2, p_sum,
    yg_all, wo_all, ubuf, mbuf, qbuf, acc, prob,
    y_part, y_r0, y_s1, y_r1, y_s2, y_r2,
    in_sem, p_send, p_recv, y_send, y_recv, g_send, g_recv,
):
    steps, batch, d_model = x_hbm.shape
    state_dim, inner = a_log_ref.shape
    dt_rank = w_dt_ref.shape[0]
    p_dim = w_xp_ref.shape[0]
    experts = wg_hbm.shape[0]
    f_loc = wg_hbm.shape[2]
    rows = CHUNK_ROWS
    chunks = batch // rows
    tokens = steps * rows
    half_rows = tokens // 2

    tp = lax.axis_index("tp")
    core = tp % 2
    chip = tp // 2
    other = 1 - core
    chip_a = chip + 1 - 2 * (chip % 2)
    chip_b = 3 - chip
    chip_far = (chip + 2) % 4
    mate = {"tp": 2 * chip + other}
    peer_a = {"tp": 2 * chip_a + core}
    peer_b = {"tp": 2 * chip_b + core}

    def copy_to(src, dst, send_sem, recv_sem, peer):
        return pltpu.make_async_remote_copy(
            src_ref=src, dst_ref=dst, send_sem=send_sem, recv_sem=recv_sem, device_id=peer, device_id_type=pl.DeviceIdType.MESH
        )

    x_in = pltpu.make_async_copy(x_hbm, xbuf, in_sem.at[0])
    h_in = pltpu.make_async_copy(h_hbm, hbuf, in_sem.at[1])
    w_ins = [pltpu.make_async_copy(src, dst, in_sem.at[2 + i]) for i, (src, dst) in enumerate(((wg_hbm, wg), (wu_hbm, wu), (wd_hbm, wd)))]
    my_rows = pl.ds(pl.multiple_of((core * 4 + chip) * inner, inner), inner)
    wo_in = pltpu.make_async_copy(w_out_hbm, wo_all.at[my_rows, :], in_sem.at[5])
    x_in.start()
    wo_in.start()

    barrier = pltpu.get_barrier_semaphore()
    for peer in (mate, peer_a, peer_b):
        pl.semaphore_signal(barrier, inc=1, device_id=peer, device_id_type=pl.DeviceIdType.MESH)
    pl.semaphore_wait(barrier, 3)

    def wo_block(c, x):
        return wo_all, lambda lo, n: (pl.ds(pl.multiple_of((c * 4 + x) * inner + lo, n), n), slice(None)), inner

    def yg_block(ch):
        def block(c, x):
            col = pl.ds(pl.multiple_of((c * 4 + x) * inner, inner), inner)
            return yg_all, lambda lo, n: (ch, pl.ds(lo, n), col), tokens
        return block

    def ag_copies(block, k):
        def cut(c, x, part=None):
            ref, index, n = block(c, x)
            if part is None:
                return ref.at[index(0, n)]
            return ref.at[index(part * (n // 2), n // 2)]

        def make(idx, src, peer, part=None):
            return copy_to(cut(core, src, part), cut(core, src, part), g_send.at[k, idx], g_recv.at[k, idx], peer)

        def take(idx, c, src, part=None):
            return copy_to(cut(c, src, part), cut(c, src, part), g_send.at[k, idx], g_recv.at[k, idx], mate)

        sends = Lazy(
            own_a=lambda: make(0, chip, peer_a), own_b=lambda: make(1, chip, peer_b),
            fwd_b=lambda: make(2, chip_a, peer_b, 0), fwd_a=lambda: make(3, chip_b, peer_a, 1),
            m_own=lambda: make(4, chip, mate), m_a=lambda: make(5, chip_a, mate),
            m_b=lambda: make(6, chip_b, mate), m_far=lambda: make(7, chip_far, mate),
        )
        recvs = Lazy(
            a=lambda: take(0, core, chip_a), b=lambda: take(1, core, chip_b),
            far0=lambda: take(2, core, chip_far, 0), far1=lambda: take(3, core, chip_far, 1),
            m_own=lambda: take(4, other, chip), m_a=lambda: take(5, other, chip_a),
            m_b=lambda: take(6, other, chip_b), m_far=lambda: take(7, other, chip_far),
        )
        return sends, recvs

    def wo_first():
        for idx, peer in ((0, peer_a), (1, peer_b), (4, mate)):
            copy_to(w_out_hbm, wo_all.at[my_rows, :], g_send.at[chunks, idx], g_recv.at[chunks, idx], peer).start()

    def ag_first(block, k):
        s, _ = ag_copies(block, k)
        s["own_a"].start()
        s["own_b"].start()
        s["m_own"].start()

    def ag_relay(block, k):
        s, r = ag_copies(block, k)
        r["a"].wait_recv()
        s["fwd_b"].start()
        s["m_a"].start()
        r["b"].wait_recv()
        s["fwd_a"].start()
        s["m_b"].start()

    def ag_far(block, k):
        s, r = ag_copies(block, k)
        r["far0"].wait_recv()
        r["far1"].wait_recv()
        s["m_far"].start()

    def ag_done(block, k):
        _, r = ag_copies(block, k)
        for name in ("m_own", "m_a", "m_b", "m_far"):
            r[name].wait_recv()

    def ag_drain(block, k):
        s, _ = ag_copies(block, k)
        for name in ("own_a", "own_b", "fwd_b", "fwd_a", "m_own", "m_a", "m_b", "m_far"):
            s[name].wait_send()

    def ar_copies(part, r0, s1, r1, s2, r2, total_keep, total_give, send, recv, ch, n):
        q = n // 4
        keep = pl.ds(pl.multiple_of(core * (n // 2), n // 2), n // 2)
        give = pl.ds(pl.multiple_of(other * (n // 2), n // 2), n // 2)
        lo, hi = pl.ds(0, q), pl.ds(q, q)

        def make(idx, src, dst, peer):
            return copy_to(src, dst, send.at[ch, idx], recv.at[ch, idx], peer)

        return Lazy(
            swap=lambda: make(0, part.at[ch, give], r0.at[ch], mate),
            a1=lambda: make(1, s1.at[ch, lo], r1.at[ch, lo], peer_a), b1=lambda: make(2, s1.at[ch, hi], r1.at[ch, hi], peer_b),
            a2=lambda: make(3, s2.at[ch, lo], r2.at[ch, lo], peer_b), b2=lambda: make(4, s2.at[ch, hi], r2.at[ch, hi], peer_a),
            out=lambda: make(5, total_keep(), total_keep(), mate),
            back=lambda: make(5, total_give(), total_give(), mate),
        ), keep

    def p_ar(ch):
        def total(c):
            return lambda: p_sum.at[ch, pl.ds(pl.multiple_of(c * (half_rows // 2), half_rows // 2), half_rows // 2)]
        return ar_copies(p_part, p_r0, p_s1, p_r1, p_s2, p_r2, total(core), total(other), p_send, p_recv, ch, half_rows)

    def y_ar(ch):
        def total(c):
            return lambda: y_ref.at[pl.ds(c * (steps // 2), steps // 2), chunk_rows(ch)]
        return ar_copies(y_part, y_r0, y_s1, y_r1, y_s2, y_r2, total(core), total(other), y_send, y_recv, ch, tokens)

    def ar_one(cs, keep, part, r0, s1, ch):
        cs["swap"].wait_recv()
        s1[ch] = (part[ch, keep].astype(F32) + r0[ch].astype(F32)).astype(s1.dtype)
        cs["a1"].start()
        cs["b1"].start()

    def ar_two(cs, s1, r1, s2, ch):
        cs["a1"].wait_recv()
        cs["b1"].wait_recv()
        s2[ch] = (s1[ch].astype(F32) + r1[ch].astype(F32)).astype(s2.dtype)
        cs["a2"].start()
        cs["b2"].start()

    def p_one(ch):
        cs, keep = p_ar(ch)
        ar_one(cs, keep, p_part, p_r0, p_s1, ch)

    def p_two(ch):
        cs, _ = p_ar(ch)
        ar_two(cs, p_s1, p_r1, p_s2, ch)

    def p_three(ch):
        cs, keep = p_ar(ch)
        cs["a2"].wait_recv()
        cs["b2"].wait_recv()
        p_sum[ch, keep] = p_s2[ch] + p_r2[ch]
        cs["out"].start()

    def y_one(ch):
        cs, keep = y_ar(ch)
        ar_one(cs, keep, y_part, y_r0, y_s1, ch)

    def y_two(ch):
        cs, _ = y_ar(ch)
        ar_two(cs, y_s1, y_r1, y_s2, ch)

    def y_three(ch):
        cs, keep = y_ar(ch)
        cs["a2"].wait_recv()
        cs["b2"].wait_recv()
        moe_sum = y_s2[ch].astype(F32) + y_r2[ch].astype(F32)
        y_new = (ubuf[ch, keep].astype(F32) + moe_sum).astype(BF16)
        y_ref[pl.ds(core * (steps // 2), steps // 2), chunk_rows(ch), :] = y_new.reshape(steps // 2, rows, d_model)
        cs["out"].start()

    def y_four(ch):
        cs, _ = y_ar(ch)
        cs["back"].wait_recv()

    def chunk_rows(ch):
        return pl.ds(pl.multiple_of(ch * rows, rows), rows)

    def stage_in(ch):
        xf = xbuf[:, chunk_rows(ch), :].reshape(tokens, d_model).astype(F32)
        scale = lax.rsqrt(jnp.mean(xf * xf, axis=-1, keepdims=True) + EPSILON)
        norm = (xf * scale * vec_ref[0:1, :]).astype(BF16)
        proj = mm(norm, w_in2[...]).astype(BF16)
        zbuf[ch] = proj[:, inner:]
        xi = proj[:, :inner]
        win = [conv_ref[j, chunk_rows(ch), :].astype(F32) for j in range(3)]
        win += [xi[s * rows:(s + 1) * rows].astype(F32) for s in range(steps)]
        for s in range(steps):
            pre = chan_ref[4:5, :]
            for j in range(4):
                pre = pre + win[s + j] * chan_ref[j:j + 1, :]
            lane = (s // 2) * inner
            xcbuf[ch, (s % 2) * rows:(s % 2 + 1) * rows, lane:lane + inner] = silu(pre).astype(BF16)
        for j in range(3):
            conv_out_ref[j, chunk_rows(ch), :] = xi[(j + 1) * rows:(j + 2) * rows]
        p_part[ch] = nt_dot(xcbuf[ch], w_xp2[...])
        cs, _ = p_ar(ch)
        cs["swap"].start()

    def stage_ssm(ch):
        cs, _ = p_ar(ch)
        cs["back"].wait_recv()
        p = p_sum[ch]
        lane = lax.broadcasted_iota(jnp.int32, p.shape, 1)
        sq = p * p
        mean = jnp.zeros_like(p)
        for base in (0, p_dim):
            for lo, n in ((0, dt_rank), (dt_rank, state_dim), (dt_rank + state_dim, state_dim)):
                inside = (lane >= base + lo) & (lane < base + lo + n)
                total = jnp.sum(jnp.where(inside, sq, 0.0), axis=-1, keepdims=True) * (1.0 / n)
                mean = jnp.where(inside, total, mean)
        pn = p * lax.rsqrt(mean + EPSILON) * chan_ref[7:8, :]
        pnbuf[...] = pn
        low = dt_rank + state_dim
        is_c = (lane % p_dim) >= low
        first = pn.astype(BF16).astype(F32)
        second = (pn - first).astype(BF16).astype(F32)
        third = pn - first - second
        parts = [jnp.where(is_c, v, 0.0) for v in (first, second, third)]
        split = parts[0] + pltpu.roll(parts[1], state_dim, 1) + pltpu.roll(parts[2], 2 * state_dim, 1)
        cbuf[...] = mm(split.astype(BF16), spread[...])
        for k in range(2 * state_dim):
            at = (k // state_dim) * p_dim + dt_rank + k % state_dim
            bbuf[:, k * inner:(k + 1) * inner] = jnp.broadcast_to(pn[:, at:at + 1], (half_rows, inner))
        pre = mm(pn.astype(BF16), w_dt2[...])
        bias = chan_ref[5:6, :]
        pre = pre + jnp.concatenate([bias, bias], axis=1)
        dbuf[...] = jnp.maximum(pre, 0.0) + jnp.log1p(jnp.exp(-jnp.abs(pre)))
        my_col = pl.ds(pl.multiple_of((core * 4 + chip) * inner, inner), inner)
        tile = 16

        def tile_body(bt, carry):
            r0 = pl.multiple_of(bt * tile, tile)
            d, dx, y, ats = [], [], [], []
            for s in range(steps):
                at = pl.ds(pl.multiple_of((s % 2) * rows + r0, tile), tile)
                cols = slice((s // 2) * inner, (s // 2 + 1) * inner)
                ds_ = dbuf[at, cols]
                xc = xcbuf[ch, at, cols].astype(F32)
                d.append(ds_)
                dx.append(ds_ * xc)
                y.append(chan_ref[6:7, :] * xc)
                ats.append(at)
            for n in range(state_dim):
                where = pl.ds((ch * rows + r0) * state_dim + n, tile, stride=state_dim)
                h = hbuf[where, :]
                a_n = a2[n:n + 1, :]
                for s in range(steps):
                    k = (s // 2) * state_dim + n
                    h = jnp.exp2(d[s] * a_n) * h + dx[s] * bbuf[ats[s], k * inner:(k + 1) * inner]
                    y[s] = y[s] + h * cbuf[ats[s], k * inner:(k + 1) * inner]
                h_ref[where, :] = h
            for s in range(steps):
                at = pl.ds(pl.multiple_of(s * rows + r0, tile), tile)
                z = zbuf[ch, at, :].astype(F32)
                yg_all[ch, at, my_col] = (y[s] * silu(z)).astype(BF16)
            return carry

        lax.fori_loop(0, rows // tile, tile_body, 0)
        ag_first(yg_block(ch), ch)

    def stage_mid(ch):
        ag_done(yg_block(ch), ch)
        mix = mm(yg_all[ch], wo_all[...])
        xf = xbuf[:, chunk_rows(ch), :].reshape(tokens, d_model).astype(F32)
        u = (xf + mix).astype(BF16)
        ubuf[ch] = u
        uf = u.astype(F32)
        scale = lax.rsqrt(jnp.mean(uf * uf, axis=-1, keepdims=True) + EPSILON)
        m = (uf * scale * vec_ref[1:2, :]).astype(BF16)
        mbuf[...] = m
        logits = nt_dot(m, w_router_ref[...])
        peak = jnp.max(logits, axis=-1, keepdims=True)
        ex = jnp.exp(logits - peak)
        ids = idbuf[:, chunk_rows(ch), 0:experts].reshape(tokens, experts)
        hit = ids == lax.broadcasted_iota(jnp.int32, (tokens, experts), 1)
        chosen = jnp.sum(jnp.where(hit, ex, 0.0), axis=-1, keepdims=True) / jnp.sum(ex, axis=-1, keepdims=True)
        prob[...] = jnp.broadcast_to(chosen, prob.shape)

    def stage_experts(ch, g):
        m = mbuf[...]
        ids = idbuf[:, chunk_rows(ch), :].reshape(tokens, inner)
        ids = jnp.concatenate([ids] * (f_loc // inner), axis=1)
        for j in range(GROUP):
            e = g * GROUP + j
            q = silu(mm(m, wg[e])) * mm(m, wu[e])
            qbuf[:, j * f_loc:(j + 1) * f_loc] = jnp.where(ids == e, q, 0.0).astype(BF16)
        part = mm(qbuf[...], wd[g * GROUP * f_loc:(g + 1) * GROUP * f_loc, :])
        if g == 0:
            acc[...] = part
        elif g < experts // GROUP - 1:
            acc[...] += part
        else:
            total = acc[...] + part
            weight = jnp.concatenate([prob[...]] * (d_model // inner), axis=1)
            y_part[ch] = (total * weight).astype(BF16)
            cs, _ = y_ar(ch)
            cs["swap"].start()

    def when_chunk(ch, fn):
        pl.when((ch >= 0) & (ch < chunks))(lambda: fn(ch))

    def loop(n, body):
        def step(i, carry):
            body(i)
            return carry
        lax.fori_loop(0, n, step, 0)

    wo_first()
    for cp in (h_in, *w_ins):
        cp.start()
    w_xp2[...] = jnp.zeros_like(w_xp2)
    w_dt2[...] = jnp.zeros_like(w_dt2)
    for k in range(2):
        w_xp2[k * p_dim:(k + 1) * p_dim, k * inner:(k + 1) * inner] = w_xp_ref[...]
        w_dt2[k * p_dim:k * p_dim + dt_rank, k * inner:(k + 1) * inner] = w_dt_ref[...]
    a2[...] = jnp.exp(a_log_ref[...]) * (-LOG2E)
    w_tmp[...] = w_in_ref[...].astype(F32)
    for k in range(2):
        w_in2[:, k * inner:(k + 1) * inner] = w_tmp[pl.ds(k, d_model, stride=2), :].astype(BF16)
    vec_ref[0:1, :] = g_in_ref[...].astype(F32).reshape(1, d_model)
    vec_ref[1:2, :] = g_ff_ref[...].astype(F32).reshape(1, d_model)
    chan_ref[0:4, :] = conv_w_ref[...].astype(F32)
    chan_ref[4:5, :] = conv_b_ref[...].astype(F32).reshape(1, inner)
    chan_ref[5:6, :] = b_dt_ref[...].astype(F32).reshape(1, inner)
    chan_ref[6:7, :] = d_skip_ref[...].reshape(1, inner)
    gains = [g[...].astype(F32).reshape(1, g.shape[0]) for g in (g_dt_ref, g_b_ref, g_c_ref)]
    chan_ref[7:8, :] = jnp.concatenate(gains + gains, axis=1)
    row = lax.broadcasted_iota(jnp.int32, (2 * p_dim, inner), 0)
    for k in range(2 * state_dim):
        at = (k // state_dim) * p_dim + dt_rank + state_dim + k % state_dim
        hit = (row == at) | (row == (at + state_dim) % (2 * p_dim)) | (row == (at + 2 * state_dim) % (2 * p_dim))
        spread[:, k * inner:(k + 1) * inner] = jnp.where(hit, 1.0, 0.0).astype(BF16)
    for s in range(steps):
        idbuf[s] = jnp.broadcast_to(ids_ref[s].astype(F32), (inner, batch)).T.astype(jnp.int32)
    x_in.wait()

    def first_body(t):
        stage_in(t)
        when_chunk(t - 2, p_one)

    loop(chunks, first_body)
    p_one(chunks - 2)
    p_one(chunks - 1)
    for ch in range(4):
        p_two(ch)
    ag_relay(wo_block, chunks)
    for ch in range(4, chunks):
        p_two(ch)
    for ch in range(3):
        p_three(ch)
    h_in.wait()

    def ssm_body(t):
        stage_ssm(t)
        when_chunk(t + 3, p_three)
        when_chunk(t - 4, lambda ch: ag_relay(yg_block(ch), ch))
        when_chunk(t - 6, lambda ch: ag_far(yg_block(ch), ch))

    loop(chunks, ssm_body)
    ag_far(wo_block, chunks)
    wo_in.wait()
    for cp in w_ins:
        cp.wait()
    ag_done(wo_block, chunks)

    def moe_body(t):
        stage_mid(t)
        for g in range(experts // GROUP):
            stage_experts(t, g)
            if g == 0:
                when_chunk(t + 4, lambda ch: ag_relay(yg_block(ch), ch))
                when_chunk(t - 4, y_three)
            elif g == 1:
                when_chunk(t + 2, lambda ch: ag_far(yg_block(ch), ch))
                when_chunk(t - 1, y_one)
            elif g == 2:
                when_chunk(t - 2, y_two)

    loop(chunks, moe_body)
    last = chunks - 1
    y_three(last - 3)
    y_two(last - 1)
    y_three(last - 2)
    y_one(last)
    y_three(last - 1)
    y_two(last)
    y_three(last)

    def drain(ch):
        y_four(ch)
        ag_drain(yg_block(ch), ch)
        for cs, _ in (p_ar(ch), y_ar(ch)):
            for name in ("swap", "a1", "b1", "a2", "b2", "out"):
                cs[name].wait_send()

    loop(chunks, drain)
    ag_drain(wo_block, chunks)


def solution(mesh):
    act_spec = P(None, "dp", None)
    state_spec = P("dp", "tp", None)
    in_specs = (act_spec, state_spec, state_spec, act_spec, P(None), P(None, None, "tp"), P("tp", None), P("tp"), P("tp", None), P(None), P(None), P(None), P(None, "tp"), P("tp"), P("tp", None), P("tp"), P("tp", None), P(None), P(None, None), P(None, None, "tp"), P(None, None, "tp"), P(None, "tp", None))
    out_specs = (act_spec, state_spec, state_spec)

    def layer_steps(x_steps, conv_state, ssm_state, expert_ids, g_in, w_in, conv_w, conv_b, w_xp, g_dt, g_b, g_c, w_dt, b_dt, a_log, d_skip, w_out, g_ff, w_router, w_gate, w_up, w_down):
        steps, batch, d_model = x_steps.shape
        inner = w_in.shape[2]
        state_dim = a_log.shape[1]
        experts, _, f_loc = w_gate.shape
        p_dim = w_xp.shape[1]
        rows = CHUNK_ROWS
        chunks = batch // rows
        tokens = steps * rows
        group_inner = w_out.shape[0] * mesh.shape["tp"]

        h_flat = jnp.swapaxes(ssm_state, 1, 2).reshape(batch * state_dim, inner)
        conv_t = jnp.transpose(conv_state, (2, 0, 1))

        any_spec = pl.BlockSpec(memory_space=pl.ANY)
        vmem_spec = pl.BlockSpec(memory_space=pltpu.VMEM)
        half = tokens // 2
        p_half = (chunks, half // 2, 2 * p_dim)
        y_half = (chunks, half, d_model)
        dma = pltpu.SemaphoreType.DMA
        scratch = [
            pltpu.VMEM(x_steps.shape, BF16),
            pltpu.VMEM(h_flat.shape, F32),
            pltpu.VMEM((steps, batch, inner), jnp.int32),
            pltpu.VMEM(w_gate.shape, BF16),
            pltpu.VMEM(w_up.shape, BF16),
            pltpu.VMEM((experts * f_loc, d_model), BF16),
            pltpu.VMEM((d_model, 2 * inner), BF16),
            pltpu.VMEM((2 * d_model, inner), F32),
            pltpu.VMEM((2, d_model), F32),
            pltpu.VMEM((8, inner), F32),
            pltpu.VMEM((2 * p_dim, 2 * inner), BF16),
            pltpu.VMEM((2 * p_dim, 2 * inner), BF16),
            pltpu.VMEM((state_dim, inner), F32),
            pltpu.VMEM((2 * p_dim, 2 * state_dim * inner), BF16),
            pltpu.VMEM((chunks, tokens, inner), BF16),
            pltpu.VMEM((chunks, half, 2 * inner), BF16),
            pltpu.VMEM((half, 2 * inner), F32),
            pltpu.VMEM((half, 2 * p_dim), F32),
            pltpu.VMEM((half, 2 * state_dim * inner), F32),
            pltpu.VMEM((half, 2 * state_dim * inner), F32),
            pltpu.VMEM((chunks, half, 2 * p_dim), F32),
            pltpu.VMEM(p_half, F32),
            pltpu.VMEM(p_half, F32),
            pltpu.VMEM(p_half, F32),
            pltpu.VMEM(p_half, F32),
            pltpu.VMEM(p_half, F32),
            pltpu.VMEM((chunks, half, 2 * p_dim), F32),
            pltpu.VMEM((chunks, tokens, group_inner), BF16),
            pltpu.VMEM((group_inner, d_model), BF16),
            pltpu.VMEM((chunks, tokens, d_model), BF16),
            pltpu.VMEM((tokens, d_model), BF16),
            pltpu.VMEM((tokens, GROUP * f_loc), BF16),
            pltpu.VMEM((tokens, d_model), F32),
            pltpu.VMEM((tokens, inner), F32),
            pltpu.VMEM((chunks, tokens, d_model), BF16),
            pltpu.VMEM(y_half, BF16),
            pltpu.VMEM(y_half, BF16),
            pltpu.VMEM(y_half, BF16),
            pltpu.VMEM(y_half, BF16),
            pltpu.VMEM(y_half, BF16),
            dma((6,)),
            dma((chunks, 6)),
            dma((chunks, 6)),
            dma((chunks, 6)),
            dma((chunks, 6)),
            dma((chunks + 1, 8)),
            dma((chunks + 1, 8)),
        ]
        y, h_new, conv_new = pl.pallas_call(
            layer_kernel,
            out_shape=(
                pltpu.VMEM(x_steps.shape, BF16),
                pltpu.VMEM(h_flat.shape, F32),
                pltpu.VMEM(conv_t.shape, BF16),
            ),
            in_specs=[any_spec] * 6 + [vmem_spec] * 16,
            out_specs=(vmem_spec,) * 3,
            scratch_shapes=scratch,
            compiler_params=pltpu.CompilerParams(collective_id=0, has_side_effects=True, vmem_limit_bytes=52 * 1024 * 1024),
        )(
            x_steps, h_flat, w_gate, w_up, w_down.reshape(experts * f_loc, d_model), w_out,
            jnp.transpose(expert_ids, (0, 2, 1)), conv_t, w_in.reshape(2 * d_model, inner), g_in, g_ff, conv_w.T, conv_b, b_dt, d_skip,
            g_dt, g_b, g_c, w_xp.T, w_dt, a_log.T, w_router.T,
        )
        h_new = jnp.swapaxes(h_new.reshape(batch, state_dim, inner), 1, 2)
        return y, jnp.transpose(conv_new, (1, 2, 0)), h_new

    return jax.shard_map(layer_steps, mesh=mesh, in_specs=in_specs, out_specs=out_specs, check_vma=False)
```

```python
import functools
import math

import jax
import jax.numpy as jnp
from jax import lax
from jax.experimental import pallas as pl
from jax.experimental.pallas import tpu as pltpu
from jax.sharding import PartitionSpec as P

EPSILON = 1e-6
F32 = jnp.float32
BF16 = jnp.bfloat16
CHUNK_ROWS = 64
GROUP = 4
LOG2E = math.log2(math.e)


class Lazy:
    def __init__(self, **makers):
        self.makers = makers

    def __getitem__(self, name):
        return self.makers[name]()


def silu(v):
    return v * jax.nn.sigmoid(v)


def nt_dot(lhs, rhs_t):
    return lax.dot_general(lhs, rhs_t, (((1,), (1,)), ((), ())), preferred_element_type=F32)


def mm(lhs, rhs):
    return jnp.dot(lhs, rhs, preferred_element_type=F32)


def layer_kernel(
    x_hbm, h_hbm, wg_hbm, wu_hbm, wd_hbm, w_out_hbm,
    ids_ref, conv_ref, w_in_ref, g_in_ref, g_ff_ref, conv_w_ref, conv_b_ref, b_dt_ref, d_skip_ref,
    g_dt_ref, g_b_ref, g_c_ref, w_xp_ref, w_dt_ref, a_log_ref, w_router_ref,
    y_ref, h_ref, conv_out_ref,
    xbuf, hbuf, idbuf, wg, wu, wd, w_in2, w_tmp, vec_ref, chan_ref, w_xp2, w_dt2, a2, spread,
    zbuf, xcbuf, dbuf, pnbuf, cbuf,
    p_part, p_r0, p_s1, p_r1, p_s2, p_r2, p_sum,
    yg_all, wo_all, ubuf, mbuf, qbuf, acc, prob,
    y_part, y_r0, y_s1, y_r1, y_s2, y_r2,
    in_sem, p_send, p_recv, y_send, y_recv, g_send, g_recv,
):
    steps, batch, d_model = x_hbm.shape
    state_dim, inner = a_log_ref.shape
    dt_rank = w_dt_ref.shape[0]
    p_dim = w_xp_ref.shape[0]
    experts = wg_hbm.shape[0]
    f_loc = wg_hbm.shape[2]
    rows = CHUNK_ROWS
    chunks = batch // rows
    tokens = steps * rows
    half_rows = tokens // 2

    tp = lax.axis_index("tp")
    core = tp % 2
    chip = tp // 2
    other = 1 - core
    chip_a = chip + 1 - 2 * (chip % 2)
    chip_b = 3 - chip
    chip_far = (chip + 2) % 4
    mate = {"tp": 2 * chip + other}
    peer_a = {"tp": 2 * chip_a + core}
    peer_b = {"tp": 2 * chip_b + core}

    def copy_to(src, dst, send_sem, recv_sem, peer):
        return pltpu.make_async_remote_copy(
            src_ref=src, dst_ref=dst, send_sem=send_sem, recv_sem=recv_sem, device_id=peer, device_id_type=pl.DeviceIdType.MESH
        )

    x_in = pltpu.make_async_copy(x_hbm, xbuf, in_sem.at[0])
    h_in = pltpu.make_async_copy(h_hbm, hbuf, in_sem.at[1])
    w_ins = [pltpu.make_async_copy(src, dst, in_sem.at[2 + i]) for i, (src, dst) in enumerate(((wg_hbm, wg), (wu_hbm, wu), (wd_hbm, wd)))]
    my_rows = pl.ds(pl.multiple_of((core * 4 + chip) * inner, inner), inner)
    wo_in = pltpu.make_async_copy(w_out_hbm, wo_all.at[my_rows, :], in_sem.at[5])
    x_in.start()
    wo_in.start()

    barrier = pltpu.get_barrier_semaphore()
    for peer in (mate, peer_a, peer_b):
        pl.semaphore_signal(barrier, inc=1, device_id=peer, device_id_type=pl.DeviceIdType.MESH)
    pl.semaphore_wait(barrier, 3)

    def wo_block(c, x):
        return wo_all, lambda lo, n: (pl.ds(pl.multiple_of((c * 4 + x) * inner + lo, n), n), slice(None)), inner

    def yg_block(ch):
        def block(c, x):
            return yg_all, lambda lo, n: (ch, c * 4 + x, pl.ds(lo, n)), tokens
        return block

    def ag_copies(block, k):
        def cut(c, x, part=None):
            ref, index, n = block(c, x)
            if part is None:
                return ref.at[index(0, n)]
            return ref.at[index(part * (n // 2), n // 2)]

        def make(idx, src, peer, part=None):
            return copy_to(cut(core, src, part), cut(core, src, part), g_send.at[k, idx], g_recv.at[k, idx], peer)

        def take(idx, c, src, part=None):
            return copy_to(cut(c, src, part), cut(c, src, part), g_send.at[k, idx], g_recv.at[k, idx], mate)

        sends = Lazy(
            own_a=lambda: make(0, chip, peer_a), own_b=lambda: make(1, chip, peer_b),
            fwd_b=lambda: make(2, chip_a, peer_b, 0), fwd_a=lambda: make(3, chip_b, peer_a, 1),
            m_own=lambda: make(4, chip, mate), m_a=lambda: make(5, chip_a, mate),
            m_b=lambda: make(6, chip_b, mate), m_far=lambda: make(7, chip_far, mate),
        )
        recvs = Lazy(
            a=lambda: take(0, core, chip_a), b=lambda: take(1, core, chip_b),
            far0=lambda: take(2, core, chip_far, 0), far1=lambda: take(3, core, chip_far, 1),
            m_own=lambda: take(4, other, chip), m_a=lambda: take(5, other, chip_a),
            m_b=lambda: take(6, other, chip_b), m_far=lambda: take(7, other, chip_far),
        )
        return sends, recvs

    def wo_first():
        for idx, peer in ((0, peer_a), (1, peer_b), (4, mate)):
            copy_to(w_out_hbm, wo_all.at[my_rows, :], g_send.at[chunks, idx], g_recv.at[chunks, idx], peer).start()

    def ag_first(block, k):
        s, _ = ag_copies(block, k)
        s["own_a"].start()
        s["own_b"].start()
        s["m_own"].start()

    def ag_relay(block, k):
        s, r = ag_copies(block, k)
        r["a"].wait_recv()
        s["fwd_b"].start()
        s["m_a"].start()
        r["b"].wait_recv()
        s["fwd_a"].start()
        s["m_b"].start()

    def ag_far(block, k):
        s, r = ag_copies(block, k)
        r["far0"].wait_recv()
        r["far1"].wait_recv()
        s["m_far"].start()

    def ag_done(block, k):
        _, r = ag_copies(block, k)
        for name in ("m_own", "m_a", "m_b", "m_far"):
            r[name].wait_recv()

    def ag_drain(block, k):
        s, _ = ag_copies(block, k)
        for name in ("own_a", "own_b", "fwd_b", "fwd_a", "m_own", "m_a", "m_b", "m_far"):
            s[name].wait_send()

    def ar_copies(part, r0, s1, r1, s2, r2, total_keep, total_give, send, recv, ch, n):
        q = n // 4
        keep = pl.ds(pl.multiple_of(core * (n // 2), n // 2), n // 2)
        give = pl.ds(pl.multiple_of(other * (n // 2), n // 2), n // 2)
        lo, hi = pl.ds(0, q), pl.ds(q, q)

        def make(idx, src, dst, peer):
            return copy_to(src, dst, send.at[ch, idx], recv.at[ch, idx], peer)

        return Lazy(
            swap=lambda: make(0, part.at[ch, give], r0.at[ch], mate),
            a1=lambda: make(1, s1.at[ch, lo], r1.at[ch, lo], peer_a), b1=lambda: make(2, s1.at[ch, hi], r1.at[ch, hi], peer_b),
            a2=lambda: make(3, s2.at[ch, lo], r2.at[ch, lo], peer_b), b2=lambda: make(4, s2.at[ch, hi], r2.at[ch, hi], peer_a),
            out=lambda: make(5, total_keep(), total_keep(), mate),
            back=lambda: make(5, total_give(), total_give(), mate),
        ), keep

    def p_ar(ch):
        def total(c):
            return lambda: p_sum.at[ch, pl.ds(pl.multiple_of(c * (half_rows // 2), half_rows // 2), half_rows // 2)]
        return ar_copies(p_part, p_r0, p_s1, p_r1, p_s2, p_r2, total(core), total(other), p_send, p_recv, ch, half_rows)

    def y_ar(ch):
        def total(c):
            return lambda: y_ref.at[pl.ds(c * (steps // 2), steps // 2), chunk_rows(ch)]
        return ar_copies(y_part, y_r0, y_s1, y_r1, y_s2, y_r2, total(core), total(other), y_send, y_recv, ch, tokens)

    def ar_one(cs, keep, part, r0, s1, ch):
        cs["swap"].wait_recv()
        s1[ch] = (part[ch, keep].astype(F32) + r0[ch].astype(F32)).astype(s1.dtype)
        cs["a1"].start()
        cs["b1"].start()

    def ar_two(cs, s1, r1, s2, ch):
        cs["a1"].wait_recv()
        cs["b1"].wait_recv()
        s2[ch] = (s1[ch].astype(F32) + r1[ch].astype(F32)).astype(s2.dtype)
        cs["a2"].start()
        cs["b2"].start()

    def p_one(ch):
        cs, keep = p_ar(ch)
        ar_one(cs, keep, p_part, p_r0, p_s1, ch)

    def p_two(ch):
        cs, _ = p_ar(ch)
        ar_two(cs, p_s1, p_r1, p_s2, ch)

    def p_three(ch):
        cs, keep = p_ar(ch)
        cs["a2"].wait_recv()
        cs["b2"].wait_recv()
        p_sum[ch, keep] = p_s2[ch] + p_r2[ch]
        cs["out"].start()

    def y_one(ch):
        cs, keep = y_ar(ch)
        ar_one(cs, keep, y_part, y_r0, y_s1, ch)

    def y_two(ch):
        cs, _ = y_ar(ch)
        ar_two(cs, y_s1, y_r1, y_s2, ch)

    def y_three(ch):
        cs, keep = y_ar(ch)
        cs["a2"].wait_recv()
        cs["b2"].wait_recv()
        moe_sum = y_s2[ch].astype(F32) + y_r2[ch].astype(F32)
        y_new = (ubuf[ch, keep].astype(F32) + moe_sum).astype(BF16)
        y_ref[pl.ds(core * (steps // 2), steps // 2), chunk_rows(ch), :] = y_new.reshape(steps // 2, rows, d_model)
        cs["out"].start()

    def y_four(ch):
        cs, _ = y_ar(ch)
        cs["back"].wait_recv()

    def chunk_rows(ch):
        return pl.ds(pl.multiple_of(ch * rows, rows), rows)

    def stage_in(ch):
        xf = xbuf[:, chunk_rows(ch), :].reshape(tokens, d_model).astype(F32)
        scale = lax.rsqrt(jnp.mean(xf * xf, axis=-1, keepdims=True) + EPSILON)
        norm = (xf * scale * vec_ref[0:1, :]).astype(BF16)
        proj = mm(norm, w_in2[...]).astype(BF16)
        zbuf[ch] = proj[:, inner:]
        xi = proj[:, :inner]
        win = [conv_ref[j, chunk_rows(ch), :].astype(F32) for j in range(3)]
        win += [xi[s * rows:(s + 1) * rows].astype(F32) for s in range(steps)]
        for s in range(steps):
            pre = chan_ref[4:5, :]
            for j in range(4):
                pre = pre + win[s + j] * chan_ref[j:j + 1, :]
            lane = (s // 2) * inner
            xcbuf[ch, (s % 2) * rows:(s % 2 + 1) * rows, lane:lane + inner] = silu(pre).astype(BF16)
        for j in range(3):
            conv_out_ref[j, chunk_rows(ch), :] = xi[(j + 1) * rows:(j + 2) * rows]
        p_part[ch] = nt_dot(xcbuf[ch], w_xp2[...])
        cs, _ = p_ar(ch)
        cs["swap"].start()

    def stage_ssm(ch):
        cs, _ = p_ar(ch)
        cs["back"].wait_recv()
        p = p_sum[ch]
        lane = lax.broadcasted_iota(jnp.int32, p.shape, 1)
        sq = p * p
        mean = jnp.zeros_like(p)
        for base in (0, p_dim):
            for lo, n in ((0, dt_rank), (dt_rank, state_dim), (dt_rank + state_dim, state_dim)):
                inside = (lane >= base + lo) & (lane < base + lo + n)
                total = jnp.sum(jnp.where(inside, sq, 0.0), axis=-1, keepdims=True) * (1.0 / n)
                mean = jnp.where(inside, total, mean)
        pn = p * lax.rsqrt(mean + EPSILON) * chan_ref[7:8, :]
        pnbuf[...] = pn
        low = dt_rank + state_dim
        is_c = (lane % p_dim) >= low
        first = pn.astype(BF16).astype(F32)
        second = (pn - first).astype(BF16).astype(F32)
        third = pn - first - second
        parts = [jnp.where(is_c, v, 0.0) for v in (first, second, third)]
        split = parts[0] + pltpu.roll(parts[1], state_dim, 1) + pltpu.roll(parts[2], 2 * state_dim, 1)
        cbuf[...] = mm(split.astype(BF16), spread[...])
        pre = mm(pn.astype(BF16), w_dt2[...])
        bias = chan_ref[5:6, :]
        pre = pre + jnp.concatenate([bias, bias], axis=1)
        dbuf[...] = jnp.maximum(pre, 0.0) + jnp.log1p(jnp.exp(-jnp.abs(pre)))
        mine = core * 4 + chip
        tile = 16

        def tile_body(bt, carry):
            r0 = pl.multiple_of(bt * tile, tile)
            d, dx, y, ats, pns = [], [], [], [], []
            for s in range(steps):
                at = pl.ds(pl.multiple_of((s % 2) * rows + r0, tile), tile)
                cols = slice((s // 2) * inner, (s // 2 + 1) * inner)
                ds_ = dbuf[at, cols]
                xc = xcbuf[ch, at, cols].astype(F32)
                d.append(ds_)
                dx.append(ds_ * xc)
                y.append(chan_ref[6:7, :] * xc)
                ats.append(at)
                pns.append(pnbuf[at, :])
            for n in range(state_dim):
                where = pl.ds((ch * rows + r0) * state_dim + n, tile, stride=state_dim)
                h = hbuf[where, :]
                a_n = a2[n:n + 1, :]
                for s in range(steps):
                    k = (s // 2) * state_dim + n
                    kb = (s // 2) * p_dim + dt_rank + n
                    h = jnp.exp2(d[s] * a_n) * h + dx[s] * pns[s][:, kb:kb + 1]
                    y[s] = y[s] + h * cbuf[ats[s], k * inner:(k + 1) * inner]
                h_ref[where, :] = h
            for s in range(steps):
                at = pl.ds(pl.multiple_of(s * rows + r0, tile), tile)
                z = zbuf[ch, at, :].astype(F32)
                yg_all[ch, mine, at, :] = (y[s] * silu(z)).astype(BF16)
            return carry

        lax.fori_loop(0, rows // tile, tile_body, 0)
        ag_first(yg_block(ch), ch)

    def stage_mid(ch):
        ag_done(yg_block(ch), ch)
        mix = mm(jnp.concatenate([yg_all[ch, k] for k in range(yg_all.shape[1])], axis=1), wo_all[...])
        xf = xbuf[:, chunk_rows(ch), :].reshape(tokens, d_model).astype(F32)
        u = (xf + mix).astype(BF16)
        ubuf[ch] = u
        uf = u.astype(F32)
        scale = lax.rsqrt(jnp.mean(uf * uf, axis=-1, keepdims=True) + EPSILON)
        m = (uf * scale * vec_ref[1:2, :]).astype(BF16)
        mbuf[...] = m
        logits = nt_dot(m, w_router_ref[...])
        peak = jnp.max(logits, axis=-1, keepdims=True)
        ex = jnp.exp(logits - peak)
        ids = idbuf[:, chunk_rows(ch), 0:experts].reshape(tokens, experts)
        hit = ids == lax.broadcasted_iota(jnp.int32, (tokens, experts), 1)
        chosen = jnp.sum(jnp.where(hit, ex, 0.0), axis=-1, keepdims=True) / jnp.sum(ex, axis=-1, keepdims=True)
        prob[...] = jnp.broadcast_to(chosen, prob.shape)

    def stage_experts(ch, g):
        m = mbuf[...]
        ids = idbuf[:, chunk_rows(ch), :].reshape(tokens, inner)
        ids = jnp.concatenate([ids] * (f_loc // inner), axis=1)
        for j in range(GROUP):
            e = g * GROUP + j
            q = silu(mm(m, wg[e])) * mm(m, wu[e])
            qbuf[:, j * f_loc:(j + 1) * f_loc] = jnp.where(ids == e, q, 0.0).astype(BF16)
        part = mm(qbuf[...], wd[g * GROUP * f_loc:(g + 1) * GROUP * f_loc, :])
        if g == 0:
            acc[...] = part
        elif g < experts // GROUP - 1:
            acc[...] += part
        else:
            total = acc[...] + part
            weight = jnp.concatenate([prob[...]] * (d_model // inner), axis=1)
            y_part[ch] = (total * weight).astype(BF16)
            cs, _ = y_ar(ch)
            cs["swap"].start()

    def when_chunk(ch, fn):
        pl.when((ch >= 0) & (ch < chunks))(lambda: fn(ch))

    def loop(n, body):
        def step(i, carry):
            body(i)
            return carry
        lax.fori_loop(0, n, step, 0)

    wo_first()
    for cp in (h_in, *w_ins):
        cp.start()
    w_xp2[...] = jnp.zeros_like(w_xp2)
    w_dt2[...] = jnp.zeros_like(w_dt2)
    for k in range(2):
        w_xp2[k * p_dim:(k + 1) * p_dim, k * inner:(k + 1) * inner] = w_xp_ref[...]
        w_dt2[k * p_dim:k * p_dim + dt_rank, k * inner:(k + 1) * inner] = w_dt_ref[...]
    a2[...] = jnp.exp(a_log_ref[...]) * (-LOG2E)
    w_tmp[...] = w_in_ref[...].astype(F32)
    for k in range(2):
        w_in2[:, k * inner:(k + 1) * inner] = w_tmp[pl.ds(k, d_model, stride=2), :].astype(BF16)
    vec_ref[0:1, :] = g_in_ref[...].astype(F32).reshape(1, d_model)
    vec_ref[1:2, :] = g_ff_ref[...].astype(F32).reshape(1, d_model)
    chan_ref[0:4, :] = conv_w_ref[...].astype(F32)
    chan_ref[4:5, :] = conv_b_ref[...].astype(F32).reshape(1, inner)
    chan_ref[5:6, :] = b_dt_ref[...].astype(F32).reshape(1, inner)
    chan_ref[6:7, :] = d_skip_ref[...].reshape(1, inner)
    gains = [g[...].astype(F32).reshape(1, g.shape[0]) for g in (g_dt_ref, g_b_ref, g_c_ref)]
    chan_ref[7:8, :] = jnp.concatenate(gains + gains, axis=1)
    row = lax.broadcasted_iota(jnp.int32, (2 * p_dim, inner), 0)
    for k in range(2 * state_dim):
        at = (k // state_dim) * p_dim + dt_rank + state_dim + k % state_dim
        hit = (row == at) | (row == (at + state_dim) % (2 * p_dim)) | (row == (at + 2 * state_dim) % (2 * p_dim))
        spread[:, k * inner:(k + 1) * inner] = jnp.where(hit, 1.0, 0.0).astype(BF16)
    for s in range(steps):
        idbuf[s] = jnp.broadcast_to(ids_ref[s].astype(F32), (inner, batch)).T.astype(jnp.int32)
    x_in.wait()

    def first_body(t):
        stage_in(t)
        when_chunk(t - 3, p_one)

    loop(chunks, first_body)
    for ch in range(chunks - 3, chunks):
        p_one(ch)
    for ch in range(chunks):
        p_two(ch)
    ag_relay(wo_block, chunks)
    for ch in range(3):
        p_three(ch)
    h_in.wait()

    def ssm_body(t):
        stage_ssm(t)
        when_chunk(t + 3, p_three)
        when_chunk(t - 4, lambda ch: ag_relay(yg_block(ch), ch))
        when_chunk(t - 7, lambda ch: ag_far(yg_block(ch), ch))

    loop(chunks, ssm_body)
    ag_far(wo_block, chunks)
    wo_in.wait()
    for cp in w_ins:
        cp.wait()
    ag_done(wo_block, chunks)

    def moe_body(t):
        stage_mid(t)
        for g in range(experts // GROUP):
            stage_experts(t, g)
            if g == 0:
                when_chunk(t + 4, lambda ch: ag_relay(yg_block(ch), ch))
                when_chunk(t - 4, y_three)
            elif g == 1:
                when_chunk(t + 1, lambda ch: ag_far(yg_block(ch), ch))
                when_chunk(t - 1, y_one)
            elif g == 2:
                when_chunk(t - 2, y_two)

    loop(chunks, moe_body)
    last = chunks - 1
    y_three(last - 3)
    y_two(last - 1)
    y_three(last - 2)
    y_one(last)
    y_three(last - 1)
    y_two(last)
    y_three(last)

    def drain(ch):
        y_four(ch)
        ag_drain(yg_block(ch), ch)
        for cs, _ in (p_ar(ch), y_ar(ch)):
            for name in ("swap", "a1", "b1", "a2", "b2", "out"):
                cs[name].wait_send()

    loop(chunks, drain)
    ag_drain(wo_block, chunks)


def solution(mesh):
    act_spec = P(None, "dp", None)
    state_spec = P("dp", "tp", None)
    in_specs = (act_spec, state_spec, state_spec, act_spec, P(None), P(None, None, "tp"), P("tp", None), P("tp"), P("tp", None), P(None), P(None), P(None), P(None, "tp"), P("tp"), P("tp", None), P("tp"), P("tp", None), P(None), P(None, None), P(None, None, "tp"), P(None, None, "tp"), P(None, "tp", None))
    out_specs = (act_spec, state_spec, state_spec)

    def layer_steps(x_steps, conv_state, ssm_state, expert_ids, g_in, w_in, conv_w, conv_b, w_xp, g_dt, g_b, g_c, w_dt, b_dt, a_log, d_skip, w_out, g_ff, w_router, w_gate, w_up, w_down):
        steps, batch, d_model = x_steps.shape
        inner = w_in.shape[2]
        state_dim = a_log.shape[1]
        experts, _, f_loc = w_gate.shape
        p_dim = w_xp.shape[1]
        rows = CHUNK_ROWS
        chunks = batch // rows
        tokens = steps * rows
        group_inner = w_out.shape[0] * mesh.shape["tp"]

        h_flat = jnp.swapaxes(ssm_state, 1, 2).reshape(batch * state_dim, inner)
        conv_t = jnp.transpose(conv_state, (2, 0, 1))

        any_spec = pl.BlockSpec(memory_space=pl.ANY)
        vmem_spec = pl.BlockSpec(memory_space=pltpu.VMEM)
        half = tokens // 2
        p_half = (chunks, half // 2, 2 * p_dim)
        y_half = (chunks, half, d_model)
        dma = pltpu.SemaphoreType.DMA
        scratch = [
            pltpu.VMEM(x_steps.shape, BF16),
            pltpu.VMEM(h_flat.shape, F32),
            pltpu.VMEM((steps, batch, inner), jnp.int32),
            pltpu.VMEM(w_gate.shape, BF16),
            pltpu.VMEM(w_up.shape, BF16),
            pltpu.VMEM((experts * f_loc, d_model), BF16),
            pltpu.VMEM((d_model, 2 * inner), BF16),
            pltpu.VMEM((2 * d_model, inner), F32),
            pltpu.VMEM((2, d_model), F32),
            pltpu.VMEM((8, inner), F32),
            pltpu.VMEM((2 * p_dim, 2 * inner), BF16),
            pltpu.VMEM((2 * p_dim, 2 * inner), BF16),
            pltpu.VMEM((state_dim, inner), F32),
            pltpu.VMEM((2 * p_dim, 2 * state_dim * inner), BF16),
            pltpu.VMEM((chunks, tokens, inner), BF16),
            pltpu.VMEM((chunks, half, 2 * inner), BF16),
            pltpu.VMEM((half, 2 * inner), F32),
            pltpu.VMEM((half, 2 * p_dim), F32),
            pltpu.VMEM((half, 2 * state_dim * inner), F32),
            pltpu.VMEM((chunks, half, 2 * p_dim), F32),
            pltpu.VMEM(p_half, F32),
            pltpu.VMEM(p_half, F32),
            pltpu.VMEM(p_half, F32),
            pltpu.VMEM(p_half, F32),
            pltpu.VMEM(p_half, F32),
            pltpu.VMEM((chunks, half, 2 * p_dim), F32),
            pltpu.VMEM((chunks, group_inner // inner, tokens, inner), BF16),
            pltpu.VMEM((group_inner, d_model), BF16),
            pltpu.VMEM((chunks, tokens, d_model), BF16),
            pltpu.VMEM((tokens, d_model), BF16),
            pltpu.VMEM((tokens, GROUP * f_loc), BF16),
            pltpu.VMEM((tokens, d_model), F32),
            pltpu.VMEM((tokens, inner), F32),
            pltpu.VMEM((chunks, tokens, d_model), BF16),
            pltpu.VMEM(y_half, BF16),
            pltpu.VMEM(y_half, BF16),
            pltpu.VMEM(y_half, BF16),
            pltpu.VMEM(y_half, BF16),
            pltpu.VMEM(y_half, BF16),
            dma((6,)),
            dma((chunks, 6)),
            dma((chunks, 6)),
            dma((chunks, 6)),
            dma((chunks, 6)),
            dma((chunks + 1, 8)),
            dma((chunks + 1, 8)),
        ]
        y, h_new, conv_new = pl.pallas_call(
            layer_kernel,
            out_shape=(
                pltpu.VMEM(x_steps.shape, BF16),
                pltpu.VMEM(h_flat.shape, F32),
                pltpu.VMEM(conv_t.shape, BF16),
            ),
            in_specs=[any_spec] * 6 + [vmem_spec] * 16,
            out_specs=(vmem_spec,) * 3,
            scratch_shapes=scratch,
            compiler_params=pltpu.CompilerParams(collective_id=0, has_side_effects=True, vmem_limit_bytes=52 * 1024 * 1024),
        )(
            x_steps, h_flat, w_gate, w_up, w_down.reshape(experts * f_loc, d_model), w_out,
            jnp.transpose(expert_ids, (0, 2, 1)), conv_t, w_in.reshape(2 * d_model, inner), g_in, g_ff, conv_w.T, conv_b, b_dt, d_skip,
            g_dt, g_b, g_c, w_xp.T, w_dt, a_log.T, w_router.T,
        )
        h_new = jnp.swapaxes(h_new.reshape(batch, state_dim, inner), 1, 2)
        return y, jnp.transpose(conv_new, (1, 2, 0)), h_new

    return jax.shard_map(layer_steps, mesh=mesh, in_specs=in_specs, out_specs=out_specs, check_vma=False)
```

```python
import functools
import math

import jax
import jax.numpy as jnp
from jax import lax
from jax.experimental import pallas as pl
from jax.experimental.pallas import tpu as pltpu
from jax.sharding import PartitionSpec as P

EPSILON = 1e-6
F32 = jnp.float32
BF16 = jnp.bfloat16
CHUNK_ROWS = 64
GROUP = 4
LOG2E = math.log2(math.e)


class Lazy:
    def __init__(self, **makers):
        self.makers = makers

    def __getitem__(self, name):
        return self.makers[name]()


def silu(v):
    return v * jax.nn.sigmoid(v)


def nt_dot(lhs, rhs_t):
    return lax.dot_general(lhs, rhs_t, (((1,), (1,)), ((), ())), preferred_element_type=F32)


def mm(lhs, rhs):
    return jnp.dot(lhs, rhs, preferred_element_type=F32)


def layer_kernel(
    x_hbm, h_hbm, wg_hbm, wu_hbm, wd_hbm, w_out_hbm,
    ids_ref, conv_ref, w_in_ref, g_in_ref, g_ff_ref, conv_w_ref, conv_b_ref, b_dt_ref, d_skip_ref,
    g_dt_ref, g_b_ref, g_c_ref, w_xp_ref, w_dt_ref, a_log_ref, w_router_ref,
    y_ref, h_ref, conv_out_ref,
    xbuf, hbuf, idbuf, wg, wu, wd, w_in2, w_tmp, vec_ref, chan_ref, w_xp2, w_dt2, a2, spread,
    zbuf, xcbuf, dbuf, pnbuf, cbuf,
    p_part, p_r0, p_s1, p_r1, p_s2, p_r2, p_sum,
    yg_all, wo_all, ubuf, mbuf, qbuf, acc, prob,
    y_part, y_r0, y_s1, y_r1, y_s2, y_r2,
    in_sem, p_send, p_recv, y_send, y_recv, g_send, g_recv,
):
    steps, batch, d_model = x_hbm.shape
    state_dim, inner = a_log_ref.shape
    dt_rank = w_dt_ref.shape[0]
    p_dim = w_xp_ref.shape[0]
    experts = wg_hbm.shape[0]
    f_loc = wg_hbm.shape[2]
    rows = CHUNK_ROWS
    chunks = batch // rows
    tokens = steps * rows
    half_rows = tokens // 2

    tp = lax.axis_index("tp")
    core = tp % 2
    chip = tp // 2
    other = 1 - core
    chip_a = chip + 1 - 2 * (chip % 2)
    chip_b = 3 - chip
    chip_far = (chip + 2) % 4
    mate = {"tp": 2 * chip + other}
    peer_a = {"tp": 2 * chip_a + core}
    peer_b = {"tp": 2 * chip_b + core}

    def copy_to(src, dst, send_sem, recv_sem, peer):
        return pltpu.make_async_remote_copy(
            src_ref=src, dst_ref=dst, send_sem=send_sem, recv_sem=recv_sem, device_id=peer, device_id_type=pl.DeviceIdType.MESH
        )

    x_in = pltpu.make_async_copy(x_hbm, xbuf, in_sem.at[0])
    h_in = pltpu.make_async_copy(h_hbm, hbuf, in_sem.at[1])
    w_ins = [pltpu.make_async_copy(src, dst, in_sem.at[2 + i]) for i, (src, dst) in enumerate(((wg_hbm, wg), (wu_hbm, wu), (wd_hbm, wd)))]
    my_rows = pl.ds(pl.multiple_of((core * 4 + chip) * inner, inner), inner)
    wo_in = pltpu.make_async_copy(w_out_hbm, wo_all.at[my_rows, :], in_sem.at[5])
    barrier = pltpu.get_barrier_semaphore()
    for peer in (mate, peer_a, peer_b):
        pl.semaphore_signal(barrier, inc=1, device_id=peer, device_id_type=pl.DeviceIdType.MESH)
    x_in.start()
    wo_in.start()
    h_in.start()

    def wo_block(c, x):
        return wo_all, lambda lo, n, blocks: (pl.ds(pl.multiple_of((c * 4 + x) * inner + lo, n), n * blocks), slice(None)), inner

    def yg_block(ch):
        def block(c, x):
            return yg_all, lambda lo, n, blocks: (ch, pl.ds(c * 4 + x, blocks), pl.ds(lo, n)), tokens
        return block

    def ag_copies(block, k):
        def cut(c, x, part=None, blocks=1):
            ref, index, n = block(c, x)
            if part is None:
                return ref.at[index(0, n, blocks)]
            return ref.at[index(part * (n // 2), n // 2, 1)]

        def make(idx, c, src, peer, part=None, blocks=1):
            ref = cut(c, src, part, blocks)
            return copy_to(ref, ref, g_send.at[k], g_recv.at[k, idx], peer)

        return Lazy(
            own_a=lambda: make(0, core, chip, peer_a), own_b=lambda: make(1, core, chip, peer_b),
            fwd_b=lambda: make(2, core, chip_a, peer_b, 0), fwd_a=lambda: make(2, core, chip_b, peer_a, 1),
            m_own=lambda: make(3, core, chip, mate), m_a=lambda: make(3, core, chip_a, mate),
            m_b=lambda: make(3, core, chip_b, mate), m_far=lambda: make(3, core, chip_far, mate),
            got_a=lambda: make(0, core, chip_a, mate), got_b=lambda: make(1, core, chip_b, mate),
            got_far=lambda: make(2, core, chip_far, mate), got_mate=lambda: make(3, other, 0, mate, blocks=4),
            sent=lambda: make(3, 0, 0, mate, blocks=7),
        )

    def wo_first():
        for idx, peer in ((0, peer_a), (1, peer_b), (3, mate)):
            copy_to(w_out_hbm, wo_all.at[my_rows, :], g_send.at[chunks], g_recv.at[chunks, idx], peer).start()

    def ag_first(block, k):
        cs = ag_copies(block, k)
        cs["own_a"].start()
        cs["own_b"].start()
        cs["m_own"].start()

    def ag_relay(block, k):
        cs = ag_copies(block, k)
        cs["got_a"].wait_recv()
        cs["fwd_b"].start()
        cs["got_b"].wait_recv()
        cs["fwd_a"].start()
        cs["m_a"].start()
        cs["m_b"].start()

    def ag_far(block, k):
        cs = ag_copies(block, k)
        cs["got_far"].wait_recv()
        cs["m_far"].start()

    def ag_done(block, k):
        ag_copies(block, k)["got_mate"].wait_recv()

    def ag_drain(block, k):
        ag_copies(block, k)["sent"].wait_send()

    def ar_copies(part, r0, s1, r1, s2, r2, total_keep, total_give, send, recv, ch, n):
        q = n // 4
        keep = pl.ds(pl.multiple_of(core * (n // 2), n // 2), n // 2)
        give = pl.ds(pl.multiple_of(other * (n // 2), n // 2), n // 2)
        lo, hi = pl.ds(0, q), pl.ds(q, q)

        def make(idx, src, dst, peer):
            return copy_to(src, dst, send.at[ch], recv.at[ch, idx], peer)

        return Lazy(
            swap=lambda: make(0, part.at[ch, give], r0.at[ch], mate),
            a1=lambda: make(1, s1.at[ch, lo], r1.at[ch, lo], peer_a), b1=lambda: make(1, s1.at[ch, hi], r1.at[ch, hi], peer_b),
            a2=lambda: make(2, s2.at[ch, lo], r2.at[ch, lo], peer_b), b2=lambda: make(2, s2.at[ch, hi], r2.at[ch, hi], peer_a),
            out=lambda: make(3, total_keep(), total_keep(), mate),
            got_1=lambda: make(1, s1.at[ch], r1.at[ch], mate), got_2=lambda: make(2, s2.at[ch], r2.at[ch], mate),
            back=lambda: make(3, total_give(), total_give(), mate),
            sent=lambda: make(0, part.at[pl.ds(0, 2)], part.at[pl.ds(0, 2)], mate),
        ), keep

    def p_ar(ch):
        def total(c):
            return lambda: p_sum.at[ch, pl.ds(pl.multiple_of(c * (half_rows // 2), half_rows // 2), half_rows // 2)]
        return ar_copies(p_part, p_r0, p_s1, p_r1, p_s2, p_r2, total(core), total(other), p_send, p_recv, ch, half_rows)

    def y_ar(ch):
        def total(c):
            return lambda: y_ref.at[pl.ds(c * (steps // 2), steps // 2), chunk_rows(ch)]
        return ar_copies(y_part, y_r0, y_s1, y_r1, y_s2, y_r2, total(core), total(other), y_send, y_recv, ch, tokens)

    def ar_one(cs, keep, part, r0, s1, ch):
        cs["swap"].wait_recv()
        s1[ch] = (part[ch, keep].astype(F32) + r0[ch].astype(F32)).astype(s1.dtype)
        cs["a1"].start()
        cs["b1"].start()

    def ar_two(cs, s1, r1, s2, ch):
        cs["got_1"].wait_recv()
        s2[ch] = (s1[ch].astype(F32) + r1[ch].astype(F32)).astype(s2.dtype)
        cs["a2"].start()
        cs["b2"].start()

    def p_one(ch):
        cs, keep = p_ar(ch)
        ar_one(cs, keep, p_part, p_r0, p_s1, ch)

    def p_two(ch):
        cs, _ = p_ar(ch)
        ar_two(cs, p_s1, p_r1, p_s2, ch)

    def p_three(ch):
        cs, keep = p_ar(ch)
        cs["got_2"].wait_recv()
        p_sum[ch, keep] = p_s2[ch] + p_r2[ch]
        cs["out"].start()

    def y_one(ch):
        cs, keep = y_ar(ch)
        ar_one(cs, keep, y_part, y_r0, y_s1, ch)

    def y_two(ch):
        cs, _ = y_ar(ch)
        ar_two(cs, y_s1, y_r1, y_s2, ch)

    def y_three(ch):
        cs, keep = y_ar(ch)
        cs["got_2"].wait_recv()
        moe_sum = y_s2[ch].astype(F32) + y_r2[ch].astype(F32)
        y_new = (ubuf[ch, keep].astype(F32) + moe_sum).astype(BF16)
        y_ref[pl.ds(core * (steps // 2), steps // 2), chunk_rows(ch), :] = y_new.reshape(steps // 2, rows, d_model)
        cs["out"].start()

    def y_four(ch):
        cs, _ = y_ar(ch)
        cs["back"].wait_recv()

    def chunk_rows(ch):
        return pl.ds(pl.multiple_of(ch * rows, rows), rows)

    def stage_in(ch):
        xf = xbuf[:, chunk_rows(ch), :].reshape(tokens, d_model).astype(F32)
        scale = lax.rsqrt(jnp.mean(xf * xf, axis=-1, keepdims=True) + EPSILON)
        norm = (xf * scale * vec_ref[0:1, :]).astype(BF16)
        proj = mm(norm, w_in2[...]).astype(BF16)
        zbuf[ch] = proj[:, inner:]
        xi = proj[:, :inner]
        win = [conv_ref[j, chunk_rows(ch), :].astype(F32) for j in range(3)]
        win += [xi[s * rows:(s + 1) * rows].astype(F32) for s in range(steps)]
        for s in range(steps):
            pre = chan_ref[4:5, :]
            for j in range(4):
                pre = pre + win[s + j] * chan_ref[j:j + 1, :]
            lane = (s // 2) * inner
            xcbuf[ch, (s % 2) * rows:(s % 2 + 1) * rows, lane:lane + inner] = silu(pre).astype(BF16)
        for j in range(3):
            conv_out_ref[j, chunk_rows(ch), :] = xi[(j + 1) * rows:(j + 2) * rows]
        p_part[ch] = nt_dot(xcbuf[ch], w_xp2[...])
        cs, _ = p_ar(ch)
        cs["swap"].start()

    def stage_ssm(ch):
        cs, _ = p_ar(ch)
        cs["back"].wait_recv()
        p = p_sum[ch]
        lane = lax.broadcasted_iota(jnp.int32, p.shape, 1)
        sq = p * p
        mean = jnp.zeros_like(p)
        for base in (0, p_dim):
            for lo, n in ((0, dt_rank), (dt_rank, state_dim), (dt_rank + state_dim, state_dim)):
                inside = (lane >= base + lo) & (lane < base + lo + n)
                total = jnp.sum(jnp.where(inside, sq, 0.0), axis=-1, keepdims=True) * (1.0 / n)
                mean = jnp.where(inside, total, mean)
        pn = p * lax.rsqrt(mean + EPSILON) * chan_ref[7:8, :]
        pnbuf[...] = pn
        low = dt_rank + state_dim
        is_c = (lane % p_dim) >= low
        first = pn.astype(BF16).astype(F32)
        second = (pn - first).astype(BF16).astype(F32)
        third = pn - first - second
        parts = [jnp.where(is_c, v, 0.0) for v in (first, second, third)]
        split = parts[0] + pltpu.roll(parts[1], state_dim, 1) + pltpu.roll(parts[2], 2 * state_dim, 1)
        cbuf[...] = mm(split.astype(BF16), spread[...])
        pre = mm(pn.astype(BF16), w_dt2[...])
        bias = chan_ref[5:6, :]
        pre = pre + jnp.concatenate([bias, bias], axis=1)
        dbuf[...] = jnp.maximum(pre, 0.0) + jnp.log1p(jnp.exp(-jnp.abs(pre)))
        mine = core * 4 + chip
        tile = 16

        def tile_body(bt, carry):
            r0 = pl.multiple_of(bt * tile, tile)
            d, dx, y, ats, pns = [], [], [], [], []
            for s in range(steps):
                at = pl.ds(pl.multiple_of((s % 2) * rows + r0, tile), tile)
                cols = slice((s // 2) * inner, (s // 2 + 1) * inner)
                ds_ = dbuf[at, cols]
                xc = xcbuf[ch, at, cols].astype(F32)
                d.append(ds_)
                dx.append(ds_ * xc)
                y.append(chan_ref[6:7, :] * xc)
                ats.append(at)
                pns.append(pnbuf[at, :])
            for n in range(state_dim):
                where = pl.ds((ch * rows + r0) * state_dim + n, tile, stride=state_dim)
                h = hbuf[where, :]
                a_n = a2[n:n + 1, :]
                for s in range(steps):
                    k = (s // 2) * state_dim + n
                    kb = (s // 2) * p_dim + dt_rank + n
                    h = jnp.exp2(d[s] * a_n) * h + dx[s] * pns[s][:, kb:kb + 1]
                    y[s] = y[s] + h * cbuf[ats[s], k * inner:(k + 1) * inner]
                h_ref[where, :] = h
            for s in range(steps):
                at = pl.ds(pl.multiple_of(s * rows + r0, tile), tile)
                z = zbuf[ch, at, :].astype(F32)
                yg_all[ch, mine, at, :] = (y[s] * silu(z)).astype(BF16)
            return carry

        lax.fori_loop(0, rows // tile, tile_body, 0)
        ag_first(yg_block(ch), ch)

    def stage_mid(ch):
        ag_done(yg_block(ch), ch)
        mix = mm(jnp.concatenate([yg_all[ch, k] for k in range(yg_all.shape[1])], axis=1), wo_all[...])
        xf = xbuf[:, chunk_rows(ch), :].reshape(tokens, d_model).astype(F32)
        u = (xf + mix).astype(BF16)
        ubuf[ch] = u
        uf = u.astype(F32)
        scale = lax.rsqrt(jnp.mean(uf * uf, axis=-1, keepdims=True) + EPSILON)
        m = (uf * scale * vec_ref[1:2, :]).astype(BF16)
        mbuf[...] = m
        logits = nt_dot(m, w_router_ref[...])
        peak = jnp.max(logits, axis=-1, keepdims=True)
        ex = jnp.exp(logits - peak)
        ids = idbuf[:, chunk_rows(ch), 0:experts].reshape(tokens, experts)
        hit = ids == lax.broadcasted_iota(jnp.int32, (tokens, experts), 1)
        chosen = jnp.sum(jnp.where(hit, ex, 0.0), axis=-1, keepdims=True) / jnp.sum(ex, axis=-1, keepdims=True)
        prob[...] = jnp.broadcast_to(chosen, prob.shape)

    def stage_experts(ch, g):
        m = mbuf[...]
        ids = idbuf[:, chunk_rows(ch), :].reshape(tokens, inner)
        ids = jnp.concatenate([ids] * (f_loc // inner), axis=1)
        for j in range(GROUP):
            e = g * GROUP + j
            q = silu(mm(m, wg[e])) * mm(m, wu[e])
            qbuf[:, j * f_loc:(j + 1) * f_loc] = jnp.where(ids == e, q, 0.0).astype(BF16)
        part = mm(qbuf[...], wd[g * GROUP * f_loc:(g + 1) * GROUP * f_loc, :])
        if g == 0:
            acc[...] = part
        elif g < experts // GROUP - 1:
            acc[...] += part
        else:
            total = acc[...] + part
            weight = jnp.concatenate([prob[...]] * (d_model // inner), axis=1)
            y_part[ch] = (total * weight).astype(BF16)
            cs, _ = y_ar(ch)
            cs["swap"].start()

    def when_chunk(ch, fn):
        pl.when((ch >= 0) & (ch < chunks))(lambda: fn(ch))

    def loop(n, body):
        def step(i, carry):
            body(i)
            return carry
        lax.fori_loop(0, n, step, 0)

    w_xp2[...] = jnp.zeros_like(w_xp2)
    w_dt2[...] = jnp.zeros_like(w_dt2)
    for k in range(2):
        w_xp2[k * p_dim:(k + 1) * p_dim, k * inner:(k + 1) * inner] = w_xp_ref[...]
        w_dt2[k * p_dim:k * p_dim + dt_rank, k * inner:(k + 1) * inner] = w_dt_ref[...]
    a2[...] = jnp.exp(a_log_ref[...]) * (-LOG2E)
    w_tmp[...] = w_in_ref[...].astype(F32)
    for k in range(2):
        w_in2[:, k * inner:(k + 1) * inner] = w_tmp[pl.ds(k, d_model, stride=2), :].astype(BF16)
    vec_ref[0:1, :] = g_in_ref[...].astype(F32).reshape(1, d_model)
    vec_ref[1:2, :] = g_ff_ref[...].astype(F32).reshape(1, d_model)
    chan_ref[0:4, :] = conv_w_ref[...].astype(F32)
    chan_ref[4:5, :] = conv_b_ref[...].astype(F32).reshape(1, inner)
    chan_ref[5:6, :] = b_dt_ref[...].astype(F32).reshape(1, inner)
    chan_ref[6:7, :] = d_skip_ref[...].reshape(1, inner)
    gains = [g[...].astype(F32).reshape(1, g.shape[0]) for g in (g_dt_ref, g_b_ref, g_c_ref)]
    chan_ref[7:8, :] = jnp.concatenate(gains + gains, axis=1)
    row = lax.broadcasted_iota(jnp.int32, (2 * p_dim, inner), 0)
    for k in range(2 * state_dim):
        at = (k // state_dim) * p_dim + dt_rank + state_dim + k % state_dim
        hit = (row == at) | (row == (at + state_dim) % (2 * p_dim)) | (row == (at + 2 * state_dim) % (2 * p_dim))
        spread[:, k * inner:(k + 1) * inner] = jnp.where(hit, 1.0, 0.0).astype(BF16)
    for s in range(steps):
        idbuf[s] = jnp.broadcast_to(ids_ref[s].astype(F32), (inner, batch)).T.astype(jnp.int32)
    pl.semaphore_wait(barrier, 3)
    wo_first()
    for cp in w_ins:
        cp.start()
    x_in.wait()

    def first_body(t):
        stage_in(t)
        when_chunk(t - 3, p_one)

    loop(chunks, first_body)
    for ch in range(chunks - 3, chunks):
        p_one(ch)
    for ch in range(chunks):
        p_two(ch)
    for ch in range(3):
        p_three(ch)
    ag_relay(wo_block, chunks)
    h_in.wait()

    def ssm_body(t):
        stage_ssm(t)
        when_chunk(t + 3, p_three)
        when_chunk(t - 3, lambda ch: ag_relay(yg_block(ch), ch))
        when_chunk(t - 6, lambda ch: ag_far(yg_block(ch), ch))

    loop(chunks, ssm_body)
    ag_far(wo_block, chunks)
    wo_in.wait()
    for cp in w_ins:
        cp.wait()
    ag_done(wo_block, chunks)

    def moe_body(t):
        stage_mid(t)
        for g in range(experts // GROUP):
            stage_experts(t, g)
            if g == 0:
                when_chunk(t + 5, lambda ch: ag_relay(yg_block(ch), ch))
                when_chunk(t - 1, y_one)
            elif g == 1:
                when_chunk(t + 2, lambda ch: ag_far(yg_block(ch), ch))
                when_chunk(t - 2, y_two)
            elif g == 2:
                when_chunk(t - 3, y_three)

    loop(chunks, moe_body)
    last = chunks - 1
    y_two(last - 1)
    y_one(last)
    y_three(last - 2)
    y_three(last - 1)
    y_two(last)
    y_three(last)

    def drain(ch):
        y_four(ch)
        ag_drain(yg_block(ch), ch)
        for cs, _ in (p_ar(ch), y_ar(ch)):
            cs["sent"].wait_send()

    loop(chunks, drain)
    ag_drain(wo_block, chunks)


def solution(mesh):
    act_spec = P(None, "dp", None)
    state_spec = P("dp", "tp", None)
    in_specs = (act_spec, state_spec, state_spec, act_spec, P(None), P(None, None, "tp"), P("tp", None), P("tp"), P("tp", None), P(None), P(None), P(None), P(None, "tp"), P("tp"), P("tp", None), P("tp"), P("tp", None), P(None), P(None, None), P(None, None, "tp"), P(None, None, "tp"), P(None, "tp", None))
    out_specs = (act_spec, state_spec, state_spec)

    def layer_steps(x_steps, conv_state, ssm_state, expert_ids, g_in, w_in, conv_w, conv_b, w_xp, g_dt, g_b, g_c, w_dt, b_dt, a_log, d_skip, w_out, g_ff, w_router, w_gate, w_up, w_down):
        steps, batch, d_model = x_steps.shape
        inner = w_in.shape[2]
        state_dim = a_log.shape[1]
        experts, _, f_loc = w_gate.shape
        p_dim = w_xp.shape[1]
        rows = CHUNK_ROWS
        chunks = batch // rows
        tokens = steps * rows
        group_inner = w_out.shape[0] * mesh.shape["tp"]

        h_flat = jnp.swapaxes(ssm_state, 1, 2).reshape(batch * state_dim, inner)
        conv_t = jnp.transpose(conv_state, (2, 0, 1))

        any_spec = pl.BlockSpec(memory_space=pl.ANY)
        vmem_spec = pl.BlockSpec(memory_space=pltpu.VMEM)
        half = tokens // 2
        p_half = (chunks, half // 2, 2 * p_dim)
        y_half = (chunks, half, d_model)
        dma = pltpu.SemaphoreType.DMA
        scratch = [
            pltpu.VMEM(x_steps.shape, BF16),
            pltpu.VMEM(h_flat.shape, F32),
            pltpu.VMEM((steps, batch, inner), jnp.int32),
            pltpu.VMEM(w_gate.shape, BF16),
            pltpu.VMEM(w_up.shape, BF16),
            pltpu.VMEM((experts * f_loc, d_model), BF16),
            pltpu.VMEM((d_model, 2 * inner), BF16),
            pltpu.VMEM((2 * d_model, inner), F32),
            pltpu.VMEM((2, d_model), F32),
            pltpu.VMEM((8, inner), F32),
            pltpu.VMEM((2 * p_dim, 2 * inner), BF16),
            pltpu.VMEM((2 * p_dim, 2 * inner), BF16),
            pltpu.VMEM((state_dim, inner), F32),
            pltpu.VMEM((2 * p_dim, 2 * state_dim * inner), BF16),
            pltpu.VMEM((chunks, tokens, inner), BF16),
            pltpu.VMEM((chunks, half, 2 * inner), BF16),
            pltpu.VMEM((half, 2 * inner), F32),
            pltpu.VMEM((half, 2 * p_dim), F32),
            pltpu.VMEM((half, 2 * state_dim * inner), F32),
            pltpu.VMEM((chunks, half, 2 * p_dim), F32),
            pltpu.VMEM(p_half, F32),
            pltpu.VMEM(p_half, F32),
            pltpu.VMEM(p_half, F32),
            pltpu.VMEM(p_half, F32),
            pltpu.VMEM(p_half, F32),
            pltpu.VMEM((chunks, half, 2 * p_dim), F32),
            pltpu.VMEM((chunks, group_inner // inner, tokens, inner), BF16),
            pltpu.VMEM((group_inner, d_model), BF16),
            pltpu.VMEM((chunks, tokens, d_model), BF16),
            pltpu.VMEM((tokens, d_model), BF16),
            pltpu.VMEM((tokens, GROUP * f_loc), BF16),
            pltpu.VMEM((tokens, d_model), F32),
            pltpu.VMEM((tokens, inner), F32),
            pltpu.VMEM((chunks, tokens, d_model), BF16),
            pltpu.VMEM(y_half, BF16),
            pltpu.VMEM(y_half, BF16),
            pltpu.VMEM(y_half, BF16),
            pltpu.VMEM(y_half, BF16),
            pltpu.VMEM(y_half, BF16),
            dma((6,)),
            dma((chunks,)),
            dma((chunks, 4)),
            dma((chunks,)),
            dma((chunks, 4)),
            dma((chunks + 1,)),
            dma((chunks + 1, 4)),
        ]
        y, h_new, conv_new = pl.pallas_call(
            layer_kernel,
            out_shape=(
                pltpu.VMEM(x_steps.shape, BF16),
                pltpu.VMEM(h_flat.shape, F32),
                pltpu.VMEM(conv_t.shape, BF16),
            ),
            in_specs=[any_spec] * 6 + [vmem_spec] * 16,
            out_specs=(vmem_spec,) * 3,
            scratch_shapes=scratch,
            compiler_params=pltpu.CompilerParams(collective_id=0, has_side_effects=True, vmem_limit_bytes=52 * 1024 * 1024),
        )(
            x_steps, h_flat, w_gate, w_up, w_down.reshape(experts * f_loc, d_model), w_out,
            jnp.transpose(expert_ids, (0, 2, 1)), conv_t, w_in.reshape(2 * d_model, inner), g_in, g_ff, conv_w.T, conv_b, b_dt, d_skip,
            g_dt, g_b, g_c, w_xp.T, w_dt, a_log.T, w_router.T,
        )
        h_new = jnp.swapaxes(h_new.reshape(batch, state_dim, inner), 1, 2)
        return y, jnp.transpose(conv_new, (1, 2, 0)), h_new

    return jax.shard_map(layer_steps, mesh=mesh, in_specs=in_specs, out_specs=out_specs, check_vma=False)
```

```python
import functools
import math

import jax
import jax.numpy as jnp
from jax import lax
from jax.experimental import pallas as pl
from jax.experimental.pallas import tpu as pltpu
from jax.sharding import PartitionSpec as P

EPSILON = 1e-6
F32 = jnp.float32
BF16 = jnp.bfloat16
CHUNK_ROWS = 64
GROUP = 4
LOG2E = math.log2(math.e)


class Lazy:
    def __init__(self, **makers):
        self.makers = makers

    def __getitem__(self, name):
        return self.makers[name]()


def silu(v):
    return v * jax.nn.sigmoid(v)


def nt_dot(lhs, rhs_t):
    return lax.dot_general(lhs, rhs_t, (((1,), (1,)), ((), ())), preferred_element_type=F32)


def mm(lhs, rhs):
    return jnp.dot(lhs, rhs, preferred_element_type=F32)


def layer_kernel(
    x_hbm, h_hbm, wg_hbm, wu_hbm, wd_hbm, w_out_hbm,
    ids_ref, conv_ref, w_in_ref, g_in_ref, g_ff_ref, conv_w_ref, conv_b_ref, b_dt_ref, d_skip_ref,
    g_dt_ref, g_b_ref, g_c_ref, w_xp_ref, w_dt_ref, a_log_ref, w_router_ref,
    y_ref, h_ref, conv_out_ref,
    xbuf, hbuf, idbuf, wg, wu, wd, w_in2, w_tmp, vec_ref, chan_ref, w_xp2, w_dt2, a2, spread,
    zbuf, xcbuf, yacc, pn_a, d_a, dx_a, pn_b, d_b, dx_b,
    p_part, p_r0, p_s1, p_r1, p_s2, p_r2, p_sum,
    yg_all, wo_all, ubuf, mbuf, qbuf, acc, prob,
    y_part, y_r0, y_s1, y_r1, y_s2, y_r2,
    in_sem, p_send, p_recv, y_send, y_recv, g_send, g_recv,
):
    steps, batch, d_model = x_hbm.shape
    state_dim, inner = a_log_ref.shape
    dt_rank = w_dt_ref.shape[0]
    p_dim = w_xp_ref.shape[0]
    experts = wg_hbm.shape[0]
    f_loc = wg_hbm.shape[2]
    rows = CHUNK_ROWS
    chunks = batch // rows
    tokens = steps * rows
    half_rows = tokens // 2

    tp = lax.axis_index("tp")
    core = tp % 2
    chip = tp // 2
    other = 1 - core
    chip_a = chip + 1 - 2 * (chip % 2)
    chip_b = 3 - chip
    chip_far = (chip + 2) % 4
    mate = {"tp": 2 * chip + other}
    peer_a = {"tp": 2 * chip_a + core}
    peer_b = {"tp": 2 * chip_b + core}

    def copy_to(src, dst, send_sem, recv_sem, peer):
        return pltpu.make_async_remote_copy(
            src_ref=src, dst_ref=dst, send_sem=send_sem, recv_sem=recv_sem, device_id=peer, device_id_type=pl.DeviceIdType.MESH
        )

    x_in = pltpu.make_async_copy(x_hbm, xbuf, in_sem.at[0])
    h_in = pltpu.make_async_copy(h_hbm, hbuf, in_sem.at[1])
    w_ins = [pltpu.make_async_copy(src, dst, in_sem.at[2 + i]) for i, (src, dst) in enumerate(((wg_hbm, wg), (wu_hbm, wu), (wd_hbm, wd)))]
    my_rows = pl.ds(pl.multiple_of((core * 4 + chip) * inner, inner), inner)
    wo_in = pltpu.make_async_copy(w_out_hbm, wo_all.at[my_rows, :], in_sem.at[5])
    barrier = pltpu.get_barrier_semaphore()
    for peer in (mate, peer_a, peer_b):
        pl.semaphore_signal(barrier, inc=1, device_id=peer, device_id_type=pl.DeviceIdType.MESH)
    x_in.start()
    wo_in.start()
    h_in.start()

    def wo_block(c, x):
        return wo_all, lambda lo, n, blocks: (pl.ds(pl.multiple_of((c * 4 + x) * inner + lo, n), n * blocks), slice(None)), inner

    def yg_block(ch):
        def block(c, x):
            return yg_all, lambda lo, n, blocks: (ch, pl.ds(c * 4 + x, blocks), pl.ds(lo, n)), tokens
        return block

    def ag_copies(block, k):
        def cut(c, x, part=None, blocks=1):
            ref, index, n = block(c, x)
            if part is None:
                return ref.at[index(0, n, blocks)]
            return ref.at[index(part * (n // 2), n // 2, 1)]

        def make(idx, c, src, peer, part=None, blocks=1):
            ref = cut(c, src, part, blocks)
            return copy_to(ref, ref, g_send.at[k], g_recv.at[k, idx], peer)

        return Lazy(
            own_a=lambda: make(0, core, chip, peer_a), own_b=lambda: make(1, core, chip, peer_b),
            fwd_b=lambda: make(2, core, chip_a, peer_b, 0), fwd_a=lambda: make(2, core, chip_b, peer_a, 1),
            m_own=lambda: make(3, core, chip, mate), m_a=lambda: make(3, core, chip_a, mate),
            m_b=lambda: make(3, core, chip_b, mate), m_far=lambda: make(3, core, chip_far, mate),
            got_a=lambda: make(0, core, chip_a, mate), got_b=lambda: make(1, core, chip_b, mate),
            got_far=lambda: make(2, core, chip_far, mate), got_mate=lambda: make(3, other, 0, mate, blocks=4),
            sent=lambda: make(3, 0, 0, mate, blocks=7),
        )

    def wo_first():
        for idx, peer in ((0, peer_a), (1, peer_b), (3, mate)):
            copy_to(w_out_hbm, wo_all.at[my_rows, :], g_send.at[chunks], g_recv.at[chunks, idx], peer).start()

    def ag_first(block, k):
        cs = ag_copies(block, k)
        cs["own_a"].start()
        cs["own_b"].start()
        cs["m_own"].start()

    def ag_relay(block, k):
        cs = ag_copies(block, k)
        cs["got_a"].wait_recv()
        cs["fwd_b"].start()
        cs["got_b"].wait_recv()
        cs["fwd_a"].start()
        cs["m_a"].start()
        cs["m_b"].start()

    def ag_far(block, k):
        cs = ag_copies(block, k)
        cs["got_far"].wait_recv()
        cs["m_far"].start()

    def ag_done(block, k):
        ag_copies(block, k)["got_mate"].wait_recv()

    def ag_drain(block, k):
        ag_copies(block, k)["sent"].wait_send()

    def ar_copies(part, r0, s1, r1, s2, r2, total_keep, total_give, send, recv, ch, n):
        q = n // 4
        keep = pl.ds(pl.multiple_of(core * (n // 2), n // 2), n // 2)
        give = pl.ds(pl.multiple_of(other * (n // 2), n // 2), n // 2)
        lo, hi = pl.ds(0, q), pl.ds(q, q)

        def make(idx, src, dst, peer):
            return copy_to(src, dst, send.at[ch], recv.at[ch, idx], peer)

        return Lazy(
            swap=lambda: make(0, part.at[ch, give], r0.at[ch], mate),
            a1=lambda: make(1, s1.at[ch, lo], r1.at[ch, lo], peer_a), b1=lambda: make(1, s1.at[ch, hi], r1.at[ch, hi], peer_b),
            a2=lambda: make(2, s2.at[ch, lo], r2.at[ch, lo], peer_b), b2=lambda: make(2, s2.at[ch, hi], r2.at[ch, hi], peer_a),
            out=lambda: make(3, total_keep(), total_keep(), mate),
            got_1=lambda: make(1, s1.at[ch], r1.at[ch], mate), got_2=lambda: make(2, s2.at[ch], r2.at[ch], mate),
            back=lambda: make(3, total_give(), total_give(), mate),
            sent=lambda: make(0, part.at[pl.ds(0, 2)], part.at[pl.ds(0, 2)], mate),
        ), keep

    def p_ar(ch):
        def total(c):
            return lambda: p_sum.at[ch, pl.ds(pl.multiple_of(c * (half_rows // 2), half_rows // 2), half_rows // 2)]
        return ar_copies(p_part, p_r0, p_s1, p_r1, p_s2, p_r2, total(core), total(other), p_send, p_recv, ch, half_rows)

    def y_ar(ch):
        def total(c):
            return lambda: y_ref.at[pl.ds(c * (steps // 2), steps // 2), chunk_rows(ch)]
        return ar_copies(y_part, y_r0, y_s1, y_r1, y_s2, y_r2, total(core), total(other), y_send, y_recv, ch, tokens)

    def ar_one(cs, keep, part, r0, s1, ch):
        cs["swap"].wait_recv()
        s1[ch] = (part[ch, keep].astype(F32) + r0[ch].astype(F32)).astype(s1.dtype)
        cs["a1"].start()
        cs["b1"].start()

    def ar_two(cs, s1, r1, s2, ch):
        cs["got_1"].wait_recv()
        s2[ch] = (s1[ch].astype(F32) + r1[ch].astype(F32)).astype(s2.dtype)
        cs["a2"].start()
        cs["b2"].start()

    def p_one(ch):
        cs, keep = p_ar(ch)
        ar_one(cs, keep, p_part, p_r0, p_s1, ch)

    def p_two(ch):
        cs, _ = p_ar(ch)
        ar_two(cs, p_s1, p_r1, p_s2, ch)

    def p_three(ch):
        cs, keep = p_ar(ch)
        cs["got_2"].wait_recv()
        p_sum[ch, keep] = p_s2[ch] + p_r2[ch]
        cs["out"].start()

    def y_one(ch):
        cs, keep = y_ar(ch)
        ar_one(cs, keep, y_part, y_r0, y_s1, ch)

    def y_two(ch):
        cs, _ = y_ar(ch)
        ar_two(cs, y_s1, y_r1, y_s2, ch)

    def y_three(ch):
        cs, keep = y_ar(ch)
        cs["got_2"].wait_recv()
        moe_sum = y_s2[ch].astype(F32) + y_r2[ch].astype(F32)
        y_new = (ubuf[ch, keep].astype(F32) + moe_sum).astype(BF16)
        y_ref[pl.ds(core * (steps // 2), steps // 2), chunk_rows(ch), :] = y_new.reshape(steps // 2, rows, d_model)
        cs["out"].start()

    def y_four(ch):
        cs, _ = y_ar(ch)
        cs["back"].wait_recv()

    def chunk_rows(ch):
        return pl.ds(pl.multiple_of(ch * rows, rows), rows)

    def stage_in(ch):
        xf = xbuf[:, chunk_rows(ch), :].reshape(tokens, d_model).astype(F32)
        scale = lax.rsqrt(jnp.mean(xf * xf, axis=-1, keepdims=True) + EPSILON)
        norm = (xf * scale * vec_ref[0:1, :]).astype(BF16)
        proj = mm(norm, w_in2[...]).astype(BF16)
        zbuf[ch] = proj[:, inner:]
        xi = proj[:, :inner]
        win = [conv_ref[j, chunk_rows(ch), :].astype(F32) for j in range(3)]
        win += [xi[s * rows:(s + 1) * rows].astype(F32) for s in range(steps)]
        for s in range(steps):
            pre = chan_ref[4:5, :]
            for j in range(4):
                pre = pre + win[s + j] * chan_ref[j:j + 1, :]
            lane = (s // 2) * inner
            xcbuf[ch, (s % 2) * rows:(s % 2 + 1) * rows, lane:lane + inner] = silu(pre).astype(BF16)
        for j in range(3):
            conv_out_ref[j, chunk_rows(ch), :] = xi[(j + 1) * rows:(j + 2) * rows]
        p_part[ch] = nt_dot(xcbuf[ch], w_xp2[...])
        cs, _ = p_ar(ch)
        cs["swap"].start()

    def stage_norm(ch, pnbuf, dbuf, dxbuf):
        p = p_sum[ch]
        lane = lax.broadcasted_iota(jnp.int32, p.shape, 1)
        sq = p * p
        mean = jnp.zeros_like(p)
        for base in (0, p_dim):
            for lo, n in ((0, dt_rank), (dt_rank, state_dim), (dt_rank + state_dim, state_dim)):
                inside = (lane >= base + lo) & (lane < base + lo + n)
                total = jnp.sum(jnp.where(inside, sq, 0.0), axis=-1, keepdims=True) * (1.0 / n)
                mean = jnp.where(inside, total, mean)
        pn = p * lax.rsqrt(mean + EPSILON) * chan_ref[7:8, :]
        pnbuf[...] = pn
        pre = mm(pn.astype(BF16), w_dt2[...])
        bias = chan_ref[5:6, :]
        pre = pre + jnp.concatenate([bias, bias], axis=1)
        delta = jnp.maximum(pre, 0.0) + jnp.log1p(jnp.exp(-jnp.abs(pre)))
        dbuf[...] = delta
        dxbuf[...] = delta * xcbuf[ch].astype(F32)

    def stage_ssm(ch, pnbuf, dbuf, dxbuf):
        pn = pnbuf[...]
        lane = lax.broadcasted_iota(jnp.int32, pn.shape, 1)
        is_c = (lane % p_dim) >= dt_rank + state_dim
        first = pn.astype(BF16).astype(F32)
        second = (pn - first).astype(BF16).astype(F32)
        third = pn - first - second
        parts = [jnp.where(is_c, v, 0.0) for v in (first, second, third)]
        split = (parts[0] + pltpu.roll(parts[1], state_dim, 1) + pltpu.roll(parts[2], 2 * state_dim, 1)).astype(BF16)
        skip = chan_ref[6:7, :]

        def at(s):
            return slice((s % 2) * rows, (s % 2 + 1) * rows), slice((s // 2) * inner, (s // 2 + 1) * inner)

        for s in range(steps):
            yacc[s * rows:(s + 1) * rows, :] = skip * xcbuf[(ch, *at(s))].astype(F32)
        for n in range(state_dim):
            c_all = mm(split, spread[:, 2 * n * inner:2 * (n + 1) * inner])
            b_all = [jnp.broadcast_to(pn[:, k:k + 1], (half_rows, inner)) for k in (dt_rank + n, p_dim + dt_rank + n)]
            where = pl.ds(ch * rows * state_dim + n, rows, stride=state_dim)
            h = hbuf[where, :]
            a_n = a2[n:n + 1, :]
            for s in range(steps):
                r, c = at(s)
                h = jnp.exp2(dbuf[r, c] * a_n) * h + dxbuf[r, c] * b_all[s // 2][r]
                yacc[s * rows:(s + 1) * rows, :] += h * c_all[r, c]
            h_ref[where, :] = h
        yg_all[ch, core * 4 + chip] = (yacc[...] * silu(zbuf[ch].astype(F32))).astype(BF16)

    def stage_mid(ch):
        ag_done(yg_block(ch), ch)
        mix = mm(jnp.concatenate([yg_all[ch, k] for k in range(yg_all.shape[1])], axis=1), wo_all[...])
        xf = xbuf[:, chunk_rows(ch), :].reshape(tokens, d_model).astype(F32)
        u = (xf + mix).astype(BF16)
        ubuf[ch] = u
        uf = u.astype(F32)
        scale = lax.rsqrt(jnp.mean(uf * uf, axis=-1, keepdims=True) + EPSILON)
        m = (uf * scale * vec_ref[1:2, :]).astype(BF16)
        mbuf[...] = m
        logits = nt_dot(m, w_router_ref[...])
        peak = jnp.max(logits, axis=-1, keepdims=True)
        ex = jnp.exp(logits - peak)
        ids = idbuf[:, chunk_rows(ch), 0:experts].reshape(tokens, experts)
        hit = ids == lax.broadcasted_iota(jnp.int32, (tokens, experts), 1)
        chosen = jnp.sum(jnp.where(hit, ex, 0.0), axis=-1, keepdims=True) / jnp.sum(ex, axis=-1, keepdims=True)
        prob[...] = jnp.broadcast_to(chosen, prob.shape)

    def stage_experts(ch, g):
        m = mbuf[...]
        ids = idbuf[:, chunk_rows(ch), :].reshape(tokens, inner)
        ids = jnp.concatenate([ids] * (f_loc // inner), axis=1)
        for j in range(GROUP):
            e = g * GROUP + j
            q = silu(mm(m, wg[e])) * mm(m, wu[e])
            qbuf[:, j * f_loc:(j + 1) * f_loc] = jnp.where(ids == e, q, 0.0).astype(BF16)
        part = mm(qbuf[...], wd[g * GROUP * f_loc:(g + 1) * GROUP * f_loc, :])
        if g == 0:
            acc[...] = part
        elif g < experts // GROUP - 1:
            acc[...] += part
        else:
            total = acc[...] + part
            weight = jnp.concatenate([prob[...]] * (d_model // inner), axis=1)
            y_part[ch] = (total * weight).astype(BF16)
            cs, _ = y_ar(ch)
            cs["swap"].start()

    def when_chunk(ch, fn):
        pl.when((ch >= 0) & (ch < chunks))(lambda: fn(ch))

    def loop(n, body):
        def step(i, carry):
            body(i)
            return carry
        lax.fori_loop(0, n, step, 0)

    w_xp2[...] = jnp.zeros_like(w_xp2)
    w_dt2[...] = jnp.zeros_like(w_dt2)
    for k in range(2):
        w_xp2[k * p_dim:(k + 1) * p_dim, k * inner:(k + 1) * inner] = w_xp_ref[...]
        w_dt2[k * p_dim:k * p_dim + dt_rank, k * inner:(k + 1) * inner] = w_dt_ref[...]
    a2[...] = jnp.exp(a_log_ref[...]) * (-LOG2E)
    w_tmp[...] = w_in_ref[...].astype(F32)
    for k in range(2):
        w_in2[:, k * inner:(k + 1) * inner] = w_tmp[pl.ds(k, d_model, stride=2), :].astype(BF16)
    vec_ref[0:1, :] = g_in_ref[...].astype(F32).reshape(1, d_model)
    vec_ref[1:2, :] = g_ff_ref[...].astype(F32).reshape(1, d_model)
    chan_ref[0:4, :] = conv_w_ref[...].astype(F32)
    chan_ref[4:5, :] = conv_b_ref[...].astype(F32).reshape(1, inner)
    chan_ref[5:6, :] = b_dt_ref[...].astype(F32).reshape(1, inner)
    chan_ref[6:7, :] = d_skip_ref[...].reshape(1, inner)
    gains = [g[...].astype(F32).reshape(1, g.shape[0]) for g in (g_dt_ref, g_b_ref, g_c_ref)]
    chan_ref[7:8, :] = jnp.concatenate(gains + gains, axis=1)
    row = lax.broadcasted_iota(jnp.int32, (2 * p_dim, inner), 0)
    for k in range(2 * state_dim):
        at = (k % 2) * p_dim + dt_rank + state_dim + k // 2
        hit = (row == at) | (row == (at + state_dim) % (2 * p_dim)) | (row == (at + 2 * state_dim) % (2 * p_dim))
        spread[:, k * inner:(k + 1) * inner] = jnp.where(hit, 1.0, 0.0).astype(BF16)
    for s in range(steps):
        idbuf[s] = jnp.broadcast_to(ids_ref[s].astype(F32), (inner, batch)).T.astype(jnp.int32)
    pl.semaphore_wait(barrier, 3)
    wo_first()
    for cp in w_ins:
        cp.start()
    x_in.wait()

    def first_body(t):
        stage_in(t)
        when_chunk(t - 3, p_one)

    loop(chunks, first_body)
    for ch in range(chunks - 3, chunks):
        p_one(ch)
    for ch in range(chunks):
        p_two(ch)
    for ch in range(3):
        p_three(ch)
    ag_relay(wo_block, chunks)
    h_in.wait()

    even, odd = (pn_a, d_a, dx_a), (pn_b, d_b, dx_b)

    def p_done(ch):
        p_ar(ch)[0]["back"].wait_recv()

    def ssm_tick(t, now, later):
        when_chunk(t + 1, p_done)
        stage_ssm(t, *now)
        stage_norm(jnp.minimum(t + 1, chunks - 1), *later)
        ag_first(yg_block(t), t)
        when_chunk(t + 3, p_three)
        when_chunk(t - 3, lambda ch: ag_relay(yg_block(ch), ch))
        when_chunk(t - 6, lambda ch: ag_far(yg_block(ch), ch))

    def ssm_body(t):
        ssm_tick(2 * t, even, odd)
        ssm_tick(2 * t + 1, odd, even)

    p_done(0)
    stage_norm(0, *even)
    loop(chunks // 2, ssm_body)
    ag_far(wo_block, chunks)
    wo_in.wait()
    for cp in w_ins:
        cp.wait()
    ag_done(wo_block, chunks)

    def moe_body(t):
        stage_mid(t)
        for g in range(experts // GROUP):
            stage_experts(t, g)
            if g == 0:
                when_chunk(t + 5, lambda ch: ag_relay(yg_block(ch), ch))
                when_chunk(t - 1, y_one)
            elif g == 1:
                when_chunk(t + 2, lambda ch: ag_far(yg_block(ch), ch))
                when_chunk(t - 2, y_two)
            elif g == 2:
                when_chunk(t - 3, y_three)

    loop(chunks, moe_body)
    last = chunks - 1
    y_two(last - 1)
    y_one(last)
    y_three(last - 2)
    y_three(last - 1)
    y_two(last)
    y_three(last)

    def drain(ch):
        y_four(ch)
        ag_drain(yg_block(ch), ch)
        for cs, _ in (p_ar(ch), y_ar(ch)):
            cs["sent"].wait_send()

    loop(chunks, drain)
    ag_drain(wo_block, chunks)


def solution(mesh):
    act_spec = P(None, "dp", None)
    state_spec = P("dp", "tp", None)
    in_specs = (act_spec, state_spec, state_spec, act_spec, P(None), P(None, None, "tp"), P("tp", None), P("tp"), P("tp", None), P(None), P(None), P(None), P(None, "tp"), P("tp"), P("tp", None), P("tp"), P("tp", None), P(None), P(None, None), P(None, None, "tp"), P(None, None, "tp"), P(None, "tp", None))
    out_specs = (act_spec, state_spec, state_spec)

    def layer_steps(x_steps, conv_state, ssm_state, expert_ids, g_in, w_in, conv_w, conv_b, w_xp, g_dt, g_b, g_c, w_dt, b_dt, a_log, d_skip, w_out, g_ff, w_router, w_gate, w_up, w_down):
        steps, batch, d_model = x_steps.shape
        inner = w_in.shape[2]
        state_dim = a_log.shape[1]
        experts, _, f_loc = w_gate.shape
        p_dim = w_xp.shape[1]
        rows = CHUNK_ROWS
        chunks = batch // rows
        tokens = steps * rows
        group_inner = w_out.shape[0] * mesh.shape["tp"]

        h_flat = jnp.swapaxes(ssm_state, 1, 2).reshape(batch * state_dim, inner)
        conv_t = jnp.transpose(conv_state, (2, 0, 1))

        any_spec = pl.BlockSpec(memory_space=pl.ANY)
        vmem_spec = pl.BlockSpec(memory_space=pltpu.VMEM)
        half = tokens // 2
        p_half = (chunks, half // 2, 2 * p_dim)
        y_half = (chunks, half, d_model)
        dma = pltpu.SemaphoreType.DMA
        scratch = [
            pltpu.VMEM(x_steps.shape, BF16),
            pltpu.VMEM(h_flat.shape, F32),
            pltpu.VMEM((steps, batch, inner), jnp.int32),
            pltpu.VMEM(w_gate.shape, BF16),
            pltpu.VMEM(w_up.shape, BF16),
            pltpu.VMEM((experts * f_loc, d_model), BF16),
            pltpu.VMEM((d_model, 2 * inner), BF16),
            pltpu.VMEM((2 * d_model, inner), F32),
            pltpu.VMEM((2, d_model), F32),
            pltpu.VMEM((8, inner), F32),
            pltpu.VMEM((2 * p_dim, 2 * inner), BF16),
            pltpu.VMEM((2 * p_dim, 2 * inner), BF16),
            pltpu.VMEM((state_dim, inner), F32),
            pltpu.VMEM((2 * p_dim, 2 * state_dim * inner), BF16),
            pltpu.VMEM((chunks, tokens, inner), BF16),
            pltpu.VMEM((chunks, half, 2 * inner), BF16),
            pltpu.VMEM((tokens, inner), F32),
            pltpu.VMEM((half, 2 * p_dim), F32),
            pltpu.VMEM((half, 2 * inner), F32),
            pltpu.VMEM((half, 2 * inner), F32),
            pltpu.VMEM((half, 2 * p_dim), F32),
            pltpu.VMEM((half, 2 * inner), F32),
            pltpu.VMEM((half, 2 * inner), F32),
            pltpu.VMEM((chunks, half, 2 * p_dim), F32),
            pltpu.VMEM(p_half, F32),
            pltpu.VMEM(p_half, F32),
            pltpu.VMEM(p_half, F32),
            pltpu.VMEM(p_half, F32),
            pltpu.VMEM(p_half, F32),
            pltpu.VMEM((chunks, half, 2 * p_dim), F32),
            pltpu.VMEM((chunks, group_inner // inner, tokens, inner), BF16),
            pltpu.VMEM((group_inner, d_model), BF16),
            pltpu.VMEM((chunks, tokens, d_model), BF16),
            pltpu.VMEM((tokens, d_model), BF16),
            pltpu.VMEM((tokens, GROUP * f_loc), BF16),
            pltpu.VMEM((tokens, d_model), F32),
            pltpu.VMEM((tokens, inner), F32),
            pltpu.VMEM((chunks, tokens, d_model), BF16),
            pltpu.VMEM(y_half, BF16),
            pltpu.VMEM(y_half, BF16),
            pltpu.VMEM(y_half, BF16),
            pltpu.VMEM(y_half, BF16),
            pltpu.VMEM(y_half, BF16),
            dma((6,)),
            dma((chunks,)),
            dma((chunks, 4)),
            dma((chunks,)),
            dma((chunks, 4)),
            dma((chunks + 1,)),
            dma((chunks + 1, 4)),
        ]
        y, h_new, conv_new = pl.pallas_call(
            layer_kernel,
            out_shape=(
                pltpu.VMEM(x_steps.shape, BF16),
                pltpu.VMEM(h_flat.shape, F32),
                pltpu.VMEM(conv_t.shape, BF16),
            ),
            in_specs=[any_spec] * 6 + [vmem_spec] * 16,
            out_specs=(vmem_spec,) * 3,
            scratch_shapes=scratch,
            compiler_params=pltpu.CompilerParams(collective_id=0, has_side_effects=True, vmem_limit_bytes=52 * 1024 * 1024),
        )(
            x_steps, h_flat, w_gate, w_up, w_down.reshape(experts * f_loc, d_model), w_out,
            jnp.transpose(expert_ids, (0, 2, 1)), conv_t, w_in.reshape(2 * d_model, inner), g_in, g_ff, conv_w.T, conv_b, b_dt, d_skip,
            g_dt, g_b, g_c, w_xp.T, w_dt, a_log.T, w_router.T,
        )
        h_new = jnp.swapaxes(h_new.reshape(batch, state_dim, inner), 1, 2)
        return y, jnp.transpose(conv_new, (1, 2, 0)), h_new

    return jax.shard_map(layer_steps, mesh=mesh, in_specs=in_specs, out_specs=out_specs, check_vma=False)
```

```python
import functools
import math

import jax
import jax.numpy as jnp
from jax import lax
from jax.experimental import pallas as pl
from jax.experimental.pallas import tpu as pltpu
from jax.sharding import PartitionSpec as P

EPSILON = 1e-6
F32 = jnp.float32
BF16 = jnp.bfloat16
CHUNK_ROWS = 64
GROUP = 4
LOG2E = math.log2(math.e)


class Lazy:
    def __init__(self, **makers):
        self.makers = makers

    def __getitem__(self, name):
        return self.makers[name]()


def silu(v):
    return v * jax.nn.sigmoid(v)


def nt_dot(lhs, rhs_t):
    return lax.dot_general(lhs, rhs_t, (((1,), (1,)), ((), ())), preferred_element_type=F32)


def mm(lhs, rhs):
    return jnp.dot(lhs, rhs, preferred_element_type=F32)


def layer_kernel(
    x_hbm, h_hbm, wg_hbm, wu_hbm, wd_hbm, w_out_hbm,
    ids_ref, conv_ref, w_in_ref, g_in_ref, g_ff_ref, conv_w_ref, conv_b_ref, b_dt_ref, d_skip_ref,
    g_dt_ref, g_b_ref, g_c_ref, w_xp_ref, w_dt_ref, a_log_ref, w_router_ref,
    y_ref, h_ref, conv_out_ref,
    xbuf, hbuf, idbuf, wg, wu, wd, w_in2, w_tmp, vec_ref, chan_ref, w_xp2, w_dt2, a2, spread,
    zbuf, xcbuf, yacc, pn_a, d_a, dx_a, pn_b, d_b, dx_b,
    p_part, p_r0, p_s1, p_r1, p_s2, p_r2, p_sum,
    yg_all, wo_all, ubuf, m_a, m_b, qbuf, acc, prob_a, prob_b,
    y_part, y_r0, y_s1, y_r1, y_s2, y_r2,
    in_sem, p_send, p_recv, y_send, y_recv, g_send, g_recv,
):
    steps, batch, d_model = x_hbm.shape
    state_dim, inner = a_log_ref.shape
    dt_rank = w_dt_ref.shape[0]
    p_dim = w_xp_ref.shape[0]
    experts = wg_hbm.shape[0]
    f_loc = wg_hbm.shape[2]
    rows = CHUNK_ROWS
    chunks = batch // rows
    tokens = steps * rows
    half_rows = tokens // 2

    tp = lax.axis_index("tp")
    core = tp % 2
    chip = tp // 2
    other = 1 - core
    chip_a = chip + 1 - 2 * (chip % 2)
    chip_b = 3 - chip
    chip_far = (chip + 2) % 4
    mate = {"tp": 2 * chip + other}
    peer_a = {"tp": 2 * chip_a + core}
    peer_b = {"tp": 2 * chip_b + core}

    def copy_to(src, dst, send_sem, recv_sem, peer):
        return pltpu.make_async_remote_copy(
            src_ref=src, dst_ref=dst, send_sem=send_sem, recv_sem=recv_sem, device_id=peer, device_id_type=pl.DeviceIdType.MESH
        )

    x_in = pltpu.make_async_copy(x_hbm, xbuf, in_sem.at[0])
    h_in = pltpu.make_async_copy(h_hbm, hbuf, in_sem.at[1])
    w_ins = [pltpu.make_async_copy(src, dst, in_sem.at[2 + i]) for i, (src, dst) in enumerate(((wg_hbm, wg), (wu_hbm, wu), (wd_hbm, wd)))]
    my_rows = pl.ds(pl.multiple_of((core * 4 + chip) * inner, inner), inner)
    wo_in = pltpu.make_async_copy(w_out_hbm, wo_all.at[my_rows, :], in_sem.at[5])
    barrier = pltpu.get_barrier_semaphore()
    for peer in (mate, peer_a, peer_b):
        pl.semaphore_signal(barrier, inc=1, device_id=peer, device_id_type=pl.DeviceIdType.MESH)
    x_in.start()
    wo_in.start()

    def wo_block(c, x):
        return wo_all, lambda lo, n, blocks: (pl.ds(pl.multiple_of((c * 4 + x) * inner + lo, n), n * blocks), slice(None)), inner

    def yg_block(ch):
        def block(c, x):
            return yg_all, lambda lo, n, blocks: (ch, pl.ds(c * 4 + x, blocks), pl.ds(lo, n)), tokens
        return block

    def ag_copies(block, k):
        def cut(c, x, part=None, blocks=1):
            ref, index, n = block(c, x)
            if part is None:
                return ref.at[index(0, n, blocks)]
            return ref.at[index(part * (n // 2), n // 2, 1)]

        def make(idx, c, src, peer, part=None, blocks=1):
            ref = cut(c, src, part, blocks)
            return copy_to(ref, ref, g_send.at[k], g_recv.at[k, idx], peer)

        return Lazy(
            own_a=lambda: make(0, core, chip, peer_a), own_b=lambda: make(1, core, chip, peer_b),
            fwd_b=lambda: make(2, core, chip_a, peer_b, 0), fwd_a=lambda: make(2, core, chip_b, peer_a, 1),
            m_own=lambda: make(3, core, chip, mate), m_a=lambda: make(3, core, chip_a, mate),
            m_b=lambda: make(3, core, chip_b, mate), m_far=lambda: make(3, core, chip_far, mate),
            got_a=lambda: make(0, core, chip_a, mate), got_b=lambda: make(1, core, chip_b, mate),
            got_far=lambda: make(2, core, chip_far, mate), got_mate=lambda: make(3, other, 0, mate, blocks=4),
            sent=lambda: make(3, 0, 0, mate, blocks=7),
        )

    def wo_first():
        for idx, peer in ((0, peer_a), (1, peer_b), (3, mate)):
            copy_to(w_out_hbm, wo_all.at[my_rows, :], g_send.at[chunks], g_recv.at[chunks, idx], peer).start()

    def ag_first(block, k):
        cs = ag_copies(block, k)
        cs["own_a"].start()
        cs["own_b"].start()
        cs["m_own"].start()

    def ag_relay(block, k):
        cs = ag_copies(block, k)
        cs["got_a"].wait_recv()
        cs["fwd_b"].start()
        cs["got_b"].wait_recv()
        cs["fwd_a"].start()
        cs["m_a"].start()
        cs["m_b"].start()

    def ag_far(block, k):
        cs = ag_copies(block, k)
        cs["got_far"].wait_recv()
        cs["m_far"].start()

    def ag_done(block, k):
        ag_copies(block, k)["got_mate"].wait_recv()

    def ag_drain(block, k):
        ag_copies(block, k)["sent"].wait_send()

    def ar_copies(part, r0, s1, r1, s2, r2, total_keep, total_give, send, recv, ch, n):
        q = n // 4
        keep = pl.ds(pl.multiple_of(core * (n // 2), n // 2), n // 2)
        give = pl.ds(pl.multiple_of(other * (n // 2), n // 2), n // 2)
        lo, hi = pl.ds(0, q), pl.ds(q, q)

        def make(idx, src, dst, peer):
            return copy_to(src, dst, send.at[ch], recv.at[ch, idx], peer)

        return Lazy(
            swap=lambda: make(0, part.at[ch, give], r0.at[ch], mate),
            a1=lambda: make(1, s1.at[ch, lo], r1.at[ch, lo], peer_a), b1=lambda: make(1, s1.at[ch, hi], r1.at[ch, hi], peer_b),
            a2=lambda: make(2, s2.at[ch, lo], r2.at[ch, lo], peer_b), b2=lambda: make(2, s2.at[ch, hi], r2.at[ch, hi], peer_a),
            out=lambda: make(3, total_keep(), total_keep(), mate),
            got_1=lambda: make(1, s1.at[ch], r1.at[ch], mate), got_2=lambda: make(2, s2.at[ch], r2.at[ch], mate),
            back=lambda: make(3, total_give(), total_give(), mate),
            sent=lambda: make(0, part.at[pl.ds(0, 2)], part.at[pl.ds(0, 2)], mate),
        ), keep

    def p_ar(ch):
        def total(c):
            return lambda: p_sum.at[ch, pl.ds(pl.multiple_of(c * (half_rows // 2), half_rows // 2), half_rows // 2)]
        return ar_copies(p_part, p_r0, p_s1, p_r1, p_s2, p_r2, total(core), total(other), p_send, p_recv, ch, half_rows)

    def y_ar(ch):
        def total(c):
            return lambda: y_ref.at[pl.ds(c * (steps // 2), steps // 2), chunk_rows(ch)]
        return ar_copies(y_part, y_r0, y_s1, y_r1, y_s2, y_r2, total(core), total(other), y_send, y_recv, ch, tokens)

    def ar_one(cs, keep, part, r0, s1, ch):
        cs["swap"].wait_recv()
        s1[ch] = (part[ch, keep].astype(F32) + r0[ch].astype(F32)).astype(s1.dtype)
        cs["a1"].start()
        cs["b1"].start()

    def ar_two(cs, s1, r1, s2, ch):
        cs["got_1"].wait_recv()
        s2[ch] = (s1[ch].astype(F32) + r1[ch].astype(F32)).astype(s2.dtype)
        cs["a2"].start()
        cs["b2"].start()

    def p_one(ch):
        cs, keep = p_ar(ch)
        ar_one(cs, keep, p_part, p_r0, p_s1, ch)

    def p_two(ch):
        cs, _ = p_ar(ch)
        ar_two(cs, p_s1, p_r1, p_s2, ch)

    def p_three(ch):
        cs, keep = p_ar(ch)
        cs["got_2"].wait_recv()
        p_sum[ch, keep] = p_s2[ch] + p_r2[ch]
        cs["out"].start()

    def y_one(ch):
        cs, keep = y_ar(ch)
        ar_one(cs, keep, y_part, y_r0, y_s1, ch)

    def y_two(ch):
        cs, _ = y_ar(ch)
        ar_two(cs, y_s1, y_r1, y_s2, ch)

    def y_three(ch):
        cs, keep = y_ar(ch)
        cs["got_2"].wait_recv()
        moe_sum = y_s2[ch].astype(F32) + y_r2[ch].astype(F32)
        y_new = (ubuf[ch, keep].astype(F32) + moe_sum).astype(BF16)
        y_ref[pl.ds(core * (steps // 2), steps // 2), chunk_rows(ch), :] = y_new.reshape(steps // 2, rows, d_model)
        cs["out"].start()

    def y_four(ch):
        cs, _ = y_ar(ch)
        cs["back"].wait_recv()

    def chunk_rows(ch):
        return pl.ds(pl.multiple_of(ch * rows, rows), rows)

    def stage_in(ch):
        xf = xbuf[:, chunk_rows(ch), :].reshape(tokens, d_model).astype(F32)
        scale = lax.rsqrt(jnp.mean(xf * xf, axis=-1, keepdims=True) + EPSILON)
        norm = (xf * scale * vec_ref[0:1, :]).astype(BF16)
        proj = mm(norm, w_in2[...]).astype(BF16)
        zbuf[ch] = proj[:, inner:]
        xi = proj[:, :inner]
        win = [conv_ref[j, chunk_rows(ch), :].astype(F32) for j in range(3)]
        win += [xi[s * rows:(s + 1) * rows].astype(F32) for s in range(steps)]
        for s in range(steps):
            pre = chan_ref[4:5, :]
            for j in range(4):
                pre = pre + win[s + j] * chan_ref[j:j + 1, :]
            lane = (s // 2) * inner
            xcbuf[ch, (s % 2) * rows:(s % 2 + 1) * rows, lane:lane + inner] = silu(pre).astype(BF16)
        for j in range(3):
            conv_out_ref[j, chunk_rows(ch), :] = xi[(j + 1) * rows:(j + 2) * rows]
        p_part[ch] = nt_dot(xcbuf[ch], w_xp2[...])
        cs, _ = p_ar(ch)
        cs["swap"].start()

    def stage_norm(ch, pnbuf, dbuf, dxbuf):
        p = p_sum[ch]
        lane = lax.broadcasted_iota(jnp.int32, p.shape, 1)
        sq = p * p
        mean = jnp.zeros_like(p)
        for base in (0, p_dim):
            for lo, n in ((0, dt_rank), (dt_rank, state_dim), (dt_rank + state_dim, state_dim)):
                inside = (lane >= base + lo) & (lane < base + lo + n)
                total = jnp.sum(jnp.where(inside, sq, 0.0), axis=-1, keepdims=True) * (1.0 / n)
                mean = jnp.where(inside, total, mean)
        pn = p * lax.rsqrt(mean + EPSILON) * chan_ref[7:8, :]
        pnbuf[...] = pn
        pre = mm(pn.astype(BF16), w_dt2[...])
        bias = chan_ref[5:6, :]
        pre = pre + jnp.concatenate([bias, bias], axis=1)
        delta = jnp.maximum(pre, 0.0) + jnp.log1p(jnp.exp(-jnp.abs(pre)))
        dbuf[...] = delta
        dxbuf[...] = delta * xcbuf[ch].astype(F32)

    def stage_ssm(ch, pnbuf, dbuf, dxbuf):
        pn = pnbuf[...]
        lane = lax.broadcasted_iota(jnp.int32, pn.shape, 1)
        is_c = (lane % p_dim) >= dt_rank + state_dim
        first = pn.astype(BF16).astype(F32)
        second = (pn - first).astype(BF16).astype(F32)
        third = pn - first - second
        parts = [jnp.where(is_c, v, 0.0) for v in (first, second, third)]
        split = (parts[0] + pltpu.roll(parts[1], state_dim, 1) + pltpu.roll(parts[2], 2 * state_dim, 1)).astype(BF16)
        skip = chan_ref[6:7, :]

        def at(s):
            return slice((s % 2) * rows, (s % 2 + 1) * rows), slice((s // 2) * inner, (s // 2 + 1) * inner)

        for s in range(steps):
            yacc[s * rows:(s + 1) * rows, :] = skip * xcbuf[(ch, *at(s))].astype(F32)
        for n in range(state_dim):
            c_all = mm(split, spread[:, 2 * n * inner:2 * (n + 1) * inner])
            b_all = [jnp.broadcast_to(pn[:, k:k + 1], (half_rows, inner)) for k in (dt_rank + n, p_dim + dt_rank + n)]
            where = pl.ds(ch * rows * state_dim + n, rows, stride=state_dim)
            h = hbuf[where, :]
            a_n = a2[n:n + 1, :]
            for s in range(steps):
                r, c = at(s)
                h = jnp.exp2(dbuf[r, c] * a_n) * h + dxbuf[r, c] * b_all[s // 2][r]
                yacc[s * rows:(s + 1) * rows, :] += h * c_all[r, c]
            h_ref[where, :] = h
        yg_all[ch, core * 4 + chip] = (yacc[...] * silu(zbuf[ch].astype(F32))).astype(BF16)

    def mid_one(ch):
        mix = mm(jnp.concatenate([yg_all[ch, k] for k in range(yg_all.shape[1])], axis=1), wo_all[...])
        xf = xbuf[:, chunk_rows(ch), :].reshape(tokens, d_model).astype(F32)
        u = (xf + mix).astype(BF16)
        ubuf[ch] = u

    def mid_two(ch, mbuf):
        uf = ubuf[ch].astype(F32)
        scale = lax.rsqrt(jnp.mean(uf * uf, axis=-1, keepdims=True) + EPSILON)
        mbuf[...] = (uf * scale * vec_ref[1:2, :]).astype(BF16)

    def mid_three(ch, mbuf, prob):
        logits = nt_dot(mbuf[...], w_router_ref[...])
        peak = jnp.max(logits, axis=-1, keepdims=True)
        ex = jnp.exp(logits - peak)
        ids = idbuf[:, chunk_rows(ch), 0:experts].reshape(tokens, experts)
        hit = ids == lax.broadcasted_iota(jnp.int32, (tokens, experts), 1)
        chosen = jnp.sum(jnp.where(hit, ex, 0.0), axis=-1, keepdims=True) / jnp.sum(ex, axis=-1, keepdims=True)
        prob[...] = jnp.broadcast_to(chosen, prob.shape)

    def mid_parts(ch, mbuf, prob):
        return [lambda: mid_one(ch), lambda: mid_two(ch, mbuf), lambda: mid_three(ch, mbuf, prob)]

    def stage_experts(ch, g, mbuf, prob, between=()):
        m = mbuf[...]
        ids = idbuf[:, chunk_rows(ch), :].reshape(tokens, inner)
        ids = jnp.concatenate([ids] * (f_loc // inner), axis=1)
        for j in range(GROUP):
            e = g * GROUP + j
            q = silu(mm(m, wg[e])) * mm(m, wu[e])
            qbuf[:, j * f_loc:(j + 1) * f_loc] = jnp.where(ids == e, q, 0.0).astype(BF16)
            if j < len(between):
                between[j]()
        part = mm(qbuf[...], wd[g * GROUP * f_loc:(g + 1) * GROUP * f_loc, :])
        if g == 0:
            acc[...] = part
        elif g < experts // GROUP - 1:
            acc[...] += part
        else:
            total = acc[...] + part
            weight = jnp.concatenate([prob[...]] * (d_model // inner), axis=1)
            y_part[ch] = (total * weight).astype(BF16)

    def when_chunk(ch, fn):
        pl.when((ch >= 0) & (ch < chunks))(lambda: fn(ch))

    def loop(n, body):
        def step(i, carry):
            body(i)
            return carry
        lax.fori_loop(0, n, step, 0)

    w_xp2[...] = jnp.zeros_like(w_xp2)
    w_dt2[...] = jnp.zeros_like(w_dt2)
    for k in range(2):
        w_xp2[k * p_dim:(k + 1) * p_dim, k * inner:(k + 1) * inner] = w_xp_ref[...]
        w_dt2[k * p_dim:k * p_dim + dt_rank, k * inner:(k + 1) * inner] = w_dt_ref[...]
    a2[...] = jnp.exp(a_log_ref[...]) * (-LOG2E)
    w_tmp[...] = w_in_ref[...].astype(F32)
    for k in range(2):
        w_in2[:, k * inner:(k + 1) * inner] = w_tmp[pl.ds(k, d_model, stride=2), :].astype(BF16)
    vec_ref[0:1, :] = g_in_ref[...].astype(F32).reshape(1, d_model)
    vec_ref[1:2, :] = g_ff_ref[...].astype(F32).reshape(1, d_model)
    chan_ref[0:4, :] = conv_w_ref[...].astype(F32)
    chan_ref[4:5, :] = conv_b_ref[...].astype(F32).reshape(1, inner)
    chan_ref[5:6, :] = b_dt_ref[...].astype(F32).reshape(1, inner)
    chan_ref[6:7, :] = d_skip_ref[...].reshape(1, inner)
    gains = [g[...].astype(F32).reshape(1, g.shape[0]) for g in (g_dt_ref, g_b_ref, g_c_ref)]
    chan_ref[7:8, :] = jnp.concatenate(gains + gains, axis=1)
    row = lax.broadcasted_iota(jnp.int32, (2 * p_dim, inner), 0)
    for k in range(2 * state_dim):
        at = (k % 2) * p_dim + dt_rank + state_dim + k // 2
        hit = (row == at) | (row == (at + state_dim) % (2 * p_dim)) | (row == (at + 2 * state_dim) % (2 * p_dim))
        spread[:, k * inner:(k + 1) * inner] = jnp.where(hit, 1.0, 0.0).astype(BF16)
    for s in range(steps):
        idbuf[s] = jnp.broadcast_to(ids_ref[s].astype(F32), (inner, batch)).T.astype(jnp.int32)
    pl.semaphore_wait(barrier, 3)
    for cp in (h_in, *w_ins):
        cp.start()
    x_in.wait()

    def first_body(t):
        stage_in(t)
        when_chunk(t - 3, p_one)

    loop(chunks, first_body)
    for ch in range(chunks - 3, chunks):
        p_one(ch)
    for ch in range(chunks):
        p_two(ch)
    wo_first()
    for ch in range(3):
        p_three(ch)
    h_in.wait()

    even, odd = (pn_a, d_a, dx_a), (pn_b, d_b, dx_b)

    def p_done(ch):
        p_ar(ch)[0]["back"].wait_recv()

    def ssm_tick(t, now, later):
        when_chunk(t + 1, p_done)
        stage_ssm(t, *now)
        stage_norm(jnp.minimum(t + 1, chunks - 1), *later)
        ag_first(yg_block(t), t)
        when_chunk(t + 3, p_three)
        pl.when(t == 3)(lambda: ag_relay(wo_block, chunks))
        when_chunk(t - 3, lambda ch: ag_relay(yg_block(ch), ch))
        when_chunk(t - 6, lambda ch: ag_far(yg_block(ch), ch))

    def ssm_body(t):
        ssm_tick(2 * t, even, odd)
        ssm_tick(2 * t + 1, odd, even)

    p_done(0)
    stage_norm(0, *even)
    loop(chunks // 2, ssm_body)
    ag_far(wo_block, chunks)
    wo_in.wait()
    for cp in w_ins:
        cp.wait()
    ag_done(wo_block, chunks)

    def got_yg(ch):
        ag_done(yg_block(ch), ch)

    def moe_tick(t, now, later):
        for g in range(experts // GROUP - 1):
            stage_experts(t, g, *now)
            if g == 0:
                when_chunk(t + 5, lambda ch: ag_relay(yg_block(ch), ch))
                when_chunk(t - 1, y_one)
            elif g == 1:
                when_chunk(t + 2, lambda ch: ag_far(yg_block(ch), ch))
                when_chunk(t - 2, y_two)
            else:
                when_chunk(t - 3, y_three)
        if later is not None:
            got_yg(t + 1)
        stage_experts(t, experts // GROUP - 1, *now, mid_parts(t + 1, *later) if later is not None else ())
        y_ar(t)[0]["swap"].start()

    even, odd = (m_a, prob_a), (m_b, prob_b)

    def moe_body(i):
        moe_tick(2 * i, even, odd)
        moe_tick(2 * i + 1, odd, even)

    got_yg(0)
    for part in mid_parts(0, *even):
        part()
    loop(chunks // 2 - 1, moe_body)
    moe_tick(chunks - 2, even, odd)
    moe_tick(chunks - 1, odd, None)
    last = chunks - 1
    y_two(last - 1)
    y_one(last)
    y_three(last - 2)
    y_three(last - 1)
    y_two(last)
    y_three(last)

    def drain(ch):
        y_four(ch)
        ag_drain(yg_block(ch), ch)
        for cs, _ in (p_ar(ch), y_ar(ch)):
            cs["sent"].wait_send()

    loop(chunks, drain)
    ag_drain(wo_block, chunks)


def store_kernel(y_in, h_in, conv_in, y_out, h_out, conv_out, sem):
    pairs = ((h_in, h_out), (y_in, y_out), (conv_in, conv_out))
    copies = [pltpu.make_async_copy(src, dst, sem.at[i]) for i, (src, dst) in enumerate(pairs)]
    for cp in copies:
        cp.start()
    for cp in copies:
        cp.wait()


def solution(mesh):
    act_spec = P(None, "dp", None)
    state_spec = P("dp", "tp", None)
    in_specs = (act_spec, state_spec, state_spec, act_spec, P(None), P(None, None, "tp"), P("tp", None), P("tp"), P("tp", None), P(None), P(None), P(None), P(None, "tp"), P("tp"), P("tp", None), P("tp"), P("tp", None), P(None), P(None, None), P(None, None, "tp"), P(None, None, "tp"), P(None, "tp", None))
    out_specs = (act_spec, state_spec, state_spec)

    def layer_steps(x_steps, conv_state, ssm_state, expert_ids, g_in, w_in, conv_w, conv_b, w_xp, g_dt, g_b, g_c, w_dt, b_dt, a_log, d_skip, w_out, g_ff, w_router, w_gate, w_up, w_down):
        steps, batch, d_model = x_steps.shape
        inner = w_in.shape[2]
        state_dim = a_log.shape[1]
        experts, _, f_loc = w_gate.shape
        p_dim = w_xp.shape[1]
        rows = CHUNK_ROWS
        chunks = batch // rows
        tokens = steps * rows
        group_inner = w_out.shape[0] * mesh.shape["tp"]

        h_flat = jnp.swapaxes(ssm_state, 1, 2).reshape(batch * state_dim, inner)
        conv_t = jnp.transpose(conv_state, (2, 0, 1))

        any_spec = pl.BlockSpec(memory_space=pl.ANY)
        vmem_spec = pl.BlockSpec(memory_space=pltpu.VMEM)
        half = tokens // 2
        p_half = (chunks, half // 2, 2 * p_dim)
        y_half = (chunks, half, d_model)
        dma = pltpu.SemaphoreType.DMA
        scratch = [
            pltpu.VMEM(x_steps.shape, BF16),
            pltpu.VMEM(h_flat.shape, F32),
            pltpu.VMEM((steps, batch, inner), jnp.int32),
            pltpu.VMEM(w_gate.shape, BF16),
            pltpu.VMEM(w_up.shape, BF16),
            pltpu.VMEM((experts * f_loc, d_model), BF16),
            pltpu.VMEM((d_model, 2 * inner), BF16),
            pltpu.VMEM((2 * d_model, inner), F32),
            pltpu.VMEM((2, d_model), F32),
            pltpu.VMEM((8, inner), F32),
            pltpu.VMEM((2 * p_dim, 2 * inner), BF16),
            pltpu.VMEM((2 * p_dim, 2 * inner), BF16),
            pltpu.VMEM((state_dim, inner), F32),
            pltpu.VMEM((2 * p_dim, 2 * state_dim * inner), BF16),
            pltpu.VMEM((chunks, tokens, inner), BF16),
            pltpu.VMEM((chunks, half, 2 * inner), BF16),
            pltpu.VMEM((tokens, inner), F32),
            pltpu.VMEM((half, 2 * p_dim), F32),
            pltpu.VMEM((half, 2 * inner), F32),
            pltpu.VMEM((half, 2 * inner), F32),
            pltpu.VMEM((half, 2 * p_dim), F32),
            pltpu.VMEM((half, 2 * inner), F32),
            pltpu.VMEM((half, 2 * inner), F32),
            pltpu.VMEM((chunks, half, 2 * p_dim), F32),
            pltpu.VMEM(p_half, F32),
            pltpu.VMEM(p_half, F32),
            pltpu.VMEM(p_half, F32),
            pltpu.VMEM(p_half, F32),
            pltpu.VMEM(p_half, F32),
            pltpu.VMEM((chunks, half, 2 * p_dim), F32),
            pltpu.VMEM((chunks, group_inner // inner, tokens, inner), BF16),
            pltpu.VMEM((group_inner, d_model), BF16),
            pltpu.VMEM((chunks, tokens, d_model), BF16),
            pltpu.VMEM((tokens, d_model), BF16),
            pltpu.VMEM((tokens, d_model), BF16),
            pltpu.VMEM((tokens, GROUP * f_loc), BF16),
            pltpu.VMEM((tokens, d_model), F32),
            pltpu.VMEM((tokens, inner), F32),
            pltpu.VMEM((tokens, inner), F32),
            pltpu.VMEM((chunks, tokens, d_model), BF16),
            pltpu.VMEM(y_half, BF16),
            pltpu.VMEM(y_half, BF16),
            pltpu.VMEM(y_half, BF16),
            pltpu.VMEM(y_half, BF16),
            pltpu.VMEM(y_half, BF16),
            dma((6,)),
            dma((chunks,)),
            dma((chunks, 4)),
            dma((chunks,)),
            dma((chunks, 4)),
            dma((chunks + 1,)),
            dma((chunks + 1, 4)),
        ]
        y, h_new, conv_new = pl.pallas_call(
            layer_kernel,
            out_shape=(
                pltpu.VMEM(x_steps.shape, BF16),
                pltpu.VMEM(h_flat.shape, F32),
                pltpu.VMEM(conv_t.shape, BF16),
            ),
            in_specs=[any_spec] * 6 + [vmem_spec] * 16,
            out_specs=(vmem_spec,) * 3,
            scratch_shapes=scratch,
            compiler_params=pltpu.CompilerParams(collective_id=0, has_side_effects=True, vmem_limit_bytes=57 * 1024 * 1024),
        )(
            x_steps, h_flat, w_gate, w_up, w_down.reshape(experts * f_loc, d_model), w_out,
            jnp.transpose(expert_ids, (0, 2, 1)), conv_t, w_in.reshape(2 * d_model, inner), g_in, g_ff, conv_w.T, conv_b, b_dt, d_skip,
            g_dt, g_b, g_c, w_xp.T, w_dt, a_log.T, w_router.T,
        )
        y, h_new, conv_new = pl.pallas_call(
            store_kernel,
            out_shape=[jax.ShapeDtypeStruct(v.shape, v.dtype) for v in (y, h_new, conv_new)],
            in_specs=[vmem_spec] * 3,
            out_specs=[any_spec] * 3,
            scratch_shapes=[dma((3,))],
            compiler_params=pltpu.CompilerParams(vmem_limit_bytes=1024 * 1024),
        )(*(pltpu.with_memory_space_constraint(v, pltpu.VMEM) for v in (y, h_new, conv_new)))
        h_new = jnp.swapaxes(h_new.reshape(batch, state_dim, inner), 1, 2)
        return y, jnp.transpose(conv_new, (1, 2, 0)), h_new

    return jax.shard_map(layer_steps, mesh=mesh, in_specs=in_specs, out_specs=out_specs, check_vma=False)
```

```python
import functools
import math

import jax
import jax.numpy as jnp
from jax import lax
from jax.experimental import pallas as pl
from jax.experimental.pallas import tpu as pltpu
from jax.sharding import PartitionSpec as P

EPSILON = 1e-6
F32 = jnp.float32
BF16 = jnp.bfloat16
CHUNK_ROWS = 64
GROUP = 4
LOG2E = math.log2(math.e)


class Lazy:
    def __init__(self, **makers):
        self.makers = makers

    def __getitem__(self, name):
        return self.makers[name]()


def silu(v):
    return v * jax.nn.sigmoid(v)


def nt_dot(lhs, rhs_t):
    return lax.dot_general(lhs, rhs_t, (((1,), (1,)), ((), ())), preferred_element_type=F32)


def mm(lhs, rhs):
    return jnp.dot(lhs, rhs, preferred_element_type=F32)


def layer_kernel(
    x_hbm, h_hbm, wg_hbm, wu_hbm, wd_hbm, w_out_hbm,
    ids_ref, conv_ref, w_in_ref, g_in_ref, g_ff_ref, conv_w_ref, conv_b_ref, b_dt_ref, d_skip_ref,
    g_dt_ref, g_b_ref, g_c_ref, w_xp_ref, w_dt_ref, a_log_ref, w_router_ref,
    y_ref, h_ref, conv_out_ref,
    xbuf, hbuf, idbuf, wg, wu, wd, w_in2, w_tmp, vec_ref, chan_ref, w_xp2, w_dt2, a2, spread,
    zbuf, xcbuf, yacc, pn_a, d_a, dx_a, pn_b, d_b, dx_b,
    p_part, p_r0, p_s1, p_r1, p_s2, p_r2, p_sum,
    yg_all, wo_all, ubuf, m_a, m_b, qbuf, acc, prob_a, prob_b,
    y_part, y_r0, y_s1, y_r1, y_s2, y_r2,
    in_sem, p_send, p_recv, y_send, y_recv, g_send, g_recv,
):
    steps, batch, d_model = x_hbm.shape
    state_dim, inner = a_log_ref.shape
    dt_rank = w_dt_ref.shape[0]
    p_dim = w_xp_ref.shape[0]
    experts = wg_hbm.shape[0]
    f_loc = wg_hbm.shape[2]
    rows = CHUNK_ROWS
    chunks = batch // rows
    tokens = steps * rows
    half_rows = tokens // 2

    tp = lax.axis_index("tp")
    core = tp % 2
    chip = tp // 2
    other = 1 - core
    chip_a = chip + 1 - 2 * (chip % 2)
    chip_b = 3 - chip
    chip_far = (chip + 2) % 4
    mate = {"tp": 2 * chip + other}
    peer_a = {"tp": 2 * chip_a + core}
    peer_b = {"tp": 2 * chip_b + core}

    def copy_to(src, dst, send_sem, recv_sem, peer):
        return pltpu.make_async_remote_copy(
            src_ref=src, dst_ref=dst, send_sem=send_sem, recv_sem=recv_sem, device_id=peer, device_id_type=pl.DeviceIdType.MESH
        )

    x_in = pltpu.make_async_copy(x_hbm, xbuf, in_sem.at[0])
    h_in = pltpu.make_async_copy(h_hbm, hbuf, in_sem.at[1])
    w_ins = [pltpu.make_async_copy(src, dst, in_sem.at[2 + i]) for i, (src, dst) in enumerate(((wg_hbm, wg), (wu_hbm, wu), (wd_hbm, wd)))]
    my_rows = pl.ds(pl.multiple_of((core * 4 + chip) * inner, inner), inner)
    wo_in = pltpu.make_async_copy(w_out_hbm, wo_all.at[my_rows, :], in_sem.at[5])
    barrier = pltpu.get_barrier_semaphore()
    for peer in (mate, peer_a, peer_b):
        pl.semaphore_signal(barrier, inc=1, device_id=peer, device_id_type=pl.DeviceIdType.MESH)
    x_in.start()
    wo_in.start()

    def wo_block(c, x):
        return wo_all, lambda lo, n, blocks: (pl.ds(pl.multiple_of((c * 4 + x) * inner + lo, n), n * blocks), slice(None)), inner

    def yg_block(ch):
        def block(c, x):
            return yg_all, lambda lo, n, blocks: (ch, pl.ds(c * 4 + x, blocks), pl.ds(lo, n)), tokens
        return block

    def ag_copies(block, k):
        def cut(c, x, part=None, blocks=1):
            ref, index, n = block(c, x)
            if part is None:
                return ref.at[index(0, n, blocks)]
            return ref.at[index(part * (n // 2), n // 2, 1)]

        def make(idx, c, src, peer, part=None, blocks=1):
            ref = cut(c, src, part, blocks)
            return copy_to(ref, ref, g_send.at[k], g_recv.at[k, idx], peer)

        return Lazy(
            own_a=lambda: make(0, core, chip, peer_a), own_b=lambda: make(1, core, chip, peer_b),
            fwd_b=lambda: make(2, core, chip_a, peer_b, 0), fwd_a=lambda: make(2, core, chip_b, peer_a, 1),
            m_own=lambda: make(3, core, chip, mate), m_a=lambda: make(3, core, chip_a, mate),
            m_b=lambda: make(3, core, chip_b, mate), m_far=lambda: make(3, core, chip_far, mate),
            got_a=lambda: make(0, core, chip_a, mate), got_b=lambda: make(1, core, chip_b, mate),
            got_far=lambda: make(2, core, chip_far, mate), got_mate=lambda: make(3, other, 0, mate, blocks=4),
            sent=lambda: make(3, 0, 0, mate, blocks=7),
        )

    def wo_first():
        for idx, peer in ((0, peer_a), (1, peer_b), (3, mate)):
            copy_to(w_out_hbm, wo_all.at[my_rows, :], g_send.at[chunks], g_recv.at[chunks, idx], peer).start()

    def ag_first(block, k):
        cs = ag_copies(block, k)
        cs["own_a"].start()
        cs["own_b"].start()
        cs["m_own"].start()

    def ag_relay(block, k):
        cs = ag_copies(block, k)
        cs["got_a"].wait_recv()
        cs["fwd_b"].start()
        cs["got_b"].wait_recv()
        cs["fwd_a"].start()
        cs["m_a"].start()
        cs["m_b"].start()

    def ag_far(block, k):
        cs = ag_copies(block, k)
        cs["got_far"].wait_recv()
        cs["m_far"].start()

    def ag_done(block, k):
        ag_copies(block, k)["got_mate"].wait_recv()

    def ag_drain(block, k):
        ag_copies(block, k)["sent"].wait_send()

    def ar_copies(part, r0, s1, r1, s2, r2, total_keep, total_give, send, recv, ch, n):
        q = n // 4
        keep = pl.ds(pl.multiple_of(core * (n // 2), n // 2), n // 2)
        give = pl.ds(pl.multiple_of(other * (n // 2), n // 2), n // 2)
        lo, hi = pl.ds(0, q), pl.ds(q, q)

        def make(idx, src, dst, peer):
            return copy_to(src, dst, send.at[ch], recv.at[ch, idx], peer)

        return Lazy(
            swap=lambda: make(0, part.at[ch, give], r0.at[ch], mate),
            a1=lambda: make(1, s1.at[ch, lo], r1.at[ch, lo], peer_a), b1=lambda: make(1, s1.at[ch, hi], r1.at[ch, hi], peer_b),
            a2=lambda: make(2, s2.at[ch, lo], r2.at[ch, lo], peer_b), b2=lambda: make(2, s2.at[ch, hi], r2.at[ch, hi], peer_a),
            out=lambda: make(3, total_keep(), total_keep(), mate),
            got_1=lambda: make(1, s1.at[ch], r1.at[ch], mate), got_2=lambda: make(2, s2.at[ch], r2.at[ch], mate),
            back=lambda: make(3, total_give(), total_give(), mate),
            sent=lambda: make(0, part.at[pl.ds(0, 2)], part.at[pl.ds(0, 2)], mate),
        ), keep

    def p_ar(ch):
        def total(c):
            return lambda: p_sum.at[ch, pl.ds(pl.multiple_of(c * (half_rows // 2), half_rows // 2), half_rows // 2)]
        return ar_copies(p_part, p_r0, p_s1, p_r1, p_s2, p_r2, total(core), total(other), p_send, p_recv, ch, half_rows)

    def y_ar(ch):
        def total(c):
            return lambda: y_ref.at[pl.ds(c * (steps // 2), steps // 2), chunk_rows(ch)]
        return ar_copies(y_part, y_r0, y_s1, y_r1, y_s2, y_r2, total(core), total(other), y_send, y_recv, ch, tokens)

    def ar_one(cs, keep, part, r0, s1, ch):
        cs["swap"].wait_recv()
        s1[ch] = (part[ch, keep].astype(F32) + r0[ch].astype(F32)).astype(s1.dtype)
        cs["a1"].start()
        cs["b1"].start()

    def ar_two(cs, s1, r1, s2, ch):
        cs["got_1"].wait_recv()
        s2[ch] = (s1[ch].astype(F32) + r1[ch].astype(F32)).astype(s2.dtype)
        cs["a2"].start()
        cs["b2"].start()

    def p_one(ch):
        cs, keep = p_ar(ch)
        ar_one(cs, keep, p_part, p_r0, p_s1, ch)

    def p_two(ch):
        cs, _ = p_ar(ch)
        ar_two(cs, p_s1, p_r1, p_s2, ch)

    def p_three(ch):
        cs, keep = p_ar(ch)
        cs["got_2"].wait_recv()
        p_sum[ch, keep] = p_s2[ch] + p_r2[ch]
        cs["out"].start()

    def y_one(ch):
        cs, keep = y_ar(ch)
        ar_one(cs, keep, y_part, y_r0, y_s1, ch)

    def y_two(ch):
        cs, _ = y_ar(ch)
        ar_two(cs, y_s1, y_r1, y_s2, ch)

    def y_three(ch):
        cs, keep = y_ar(ch)
        cs["got_2"].wait_recv()
        moe_sum = y_s2[ch].astype(F32) + y_r2[ch].astype(F32)
        y_new = (ubuf[ch, keep].astype(F32) + moe_sum).astype(BF16)
        y_ref[pl.ds(core * (steps // 2), steps // 2), chunk_rows(ch), :] = y_new.reshape(steps // 2, rows, d_model)
        cs["out"].start()

    def y_four(ch):
        cs, _ = y_ar(ch)
        cs["back"].wait_recv()

    def chunk_rows(ch):
        return pl.ds(pl.multiple_of(ch * rows, rows), rows)

    def stage_in(ch):
        xf = xbuf[:, chunk_rows(ch), :].reshape(tokens, d_model).astype(F32)
        scale = lax.rsqrt(jnp.mean(xf * xf, axis=-1, keepdims=True) + EPSILON)
        norm = (xf * scale * vec_ref[0:1, :]).astype(BF16)
        proj = mm(norm, w_in2[...]).astype(BF16)
        zbuf[ch] = proj[:, inner:]
        xi = proj[:, :inner]
        win = [conv_ref[j, chunk_rows(ch), :].astype(F32) for j in range(3)]
        win += [xi[s * rows:(s + 1) * rows].astype(F32) for s in range(steps)]
        for s in range(steps):
            pre = chan_ref[4:5, :]
            for j in range(4):
                pre = pre + win[s + j] * chan_ref[j:j + 1, :]
            lane = (s // 2) * inner
            xcbuf[ch, (s % 2) * rows:(s % 2 + 1) * rows, lane:lane + inner] = silu(pre).astype(BF16)
        for j in range(3):
            conv_out_ref[j, chunk_rows(ch), :] = xi[(j + 1) * rows:(j + 2) * rows]
        p_part[ch] = nt_dot(xcbuf[ch], w_xp2[...])
        cs, _ = p_ar(ch)
        cs["swap"].start()

    def stage_norm(ch, pnbuf, dbuf, dxbuf):
        p = p_sum[ch]
        lane = lax.broadcasted_iota(jnp.int32, p.shape, 1)
        sq = p * p
        mean = jnp.zeros_like(p)
        for base in (0, p_dim):
            for lo, n in ((0, dt_rank), (dt_rank, state_dim), (dt_rank + state_dim, state_dim)):
                inside = (lane >= base + lo) & (lane < base + lo + n)
                total = jnp.sum(jnp.where(inside, sq, 0.0), axis=-1, keepdims=True) * (1.0 / n)
                mean = jnp.where(inside, total, mean)
        pn = p * lax.rsqrt(mean + EPSILON) * chan_ref[7:8, :]
        pnbuf[...] = pn
        pre = mm(pn.astype(BF16), w_dt2[...])
        bias = chan_ref[5:6, :]
        pre = pre + jnp.concatenate([bias, bias], axis=1)
        delta = jnp.maximum(pre, 0.0) + jnp.log1p(jnp.exp(-jnp.abs(pre)))
        dbuf[...] = delta
        dxbuf[...] = delta * xcbuf[ch].astype(F32)

    def stage_ssm(ch, pnbuf, dbuf, dxbuf):
        pn = pnbuf[...]
        lane = lax.broadcasted_iota(jnp.int32, pn.shape, 1)
        is_c = (lane % p_dim) >= dt_rank + state_dim
        first = pn.astype(BF16).astype(F32)
        second = (pn - first).astype(BF16).astype(F32)
        third = pn - first - second
        parts = [jnp.where(is_c, v, 0.0) for v in (first, second, third)]
        split = (parts[0] + pltpu.roll(parts[1], state_dim, 1) + pltpu.roll(parts[2], 2 * state_dim, 1)).astype(BF16)
        skip = chan_ref[6:7, :]

        def at(s):
            return slice((s % 2) * rows, (s % 2 + 1) * rows), slice((s // 2) * inner, (s // 2 + 1) * inner)

        for s in range(steps):
            yacc[s * rows:(s + 1) * rows, :] = skip * xcbuf[(ch, *at(s))].astype(F32)
        for n in range(state_dim):
            c_all = mm(split, spread[:, 2 * n * inner:2 * (n + 1) * inner])
            b_all = [jnp.broadcast_to(pn[:, k:k + 1], (half_rows, inner)) for k in (dt_rank + n, p_dim + dt_rank + n)]
            where = pl.ds(ch * rows * state_dim + n, rows, stride=state_dim)
            h = hbuf[where, :]
            a_n = a2[n:n + 1, :]
            for s in range(steps):
                r, c = at(s)
                h = jnp.exp2(dbuf[r, c] * a_n) * h + dxbuf[r, c] * b_all[s // 2][r]
                yacc[s * rows:(s + 1) * rows, :] += h * c_all[r, c]
            h_ref[where, :] = h
        yg_all[ch, core * 4 + chip] = (yacc[...] * silu(zbuf[ch].astype(F32))).astype(BF16)

    def mid_one(ch):
        mix = mm(jnp.concatenate([yg_all[ch, k] for k in range(yg_all.shape[1])], axis=1), wo_all[...])
        xf = xbuf[:, chunk_rows(ch), :].reshape(tokens, d_model).astype(F32)
        u = (xf + mix).astype(BF16)
        ubuf[ch] = u

    def mid_two(ch, mbuf):
        uf = ubuf[ch].astype(F32)
        scale = lax.rsqrt(jnp.mean(uf * uf, axis=-1, keepdims=True) + EPSILON)
        mbuf[...] = (uf * scale * vec_ref[1:2, :]).astype(BF16)

    def mid_three(ch, mbuf, prob):
        logits = nt_dot(mbuf[...], w_router_ref[...])
        peak = jnp.max(logits, axis=-1, keepdims=True)
        ex = jnp.exp(logits - peak)
        ids = idbuf[:, chunk_rows(ch), 0:experts].reshape(tokens, experts)
        hit = ids == lax.broadcasted_iota(jnp.int32, (tokens, experts), 1)
        chosen = jnp.sum(jnp.where(hit, ex, 0.0), axis=-1, keepdims=True) / jnp.sum(ex, axis=-1, keepdims=True)
        prob[...] = jnp.broadcast_to(chosen, prob.shape)

    def mid_parts(ch, mbuf, prob):
        return [lambda: mid_one(ch), lambda: mid_two(ch, mbuf), lambda: mid_three(ch, mbuf, prob)]

    def stage_experts(ch, g, mbuf, prob, between=()):
        m = mbuf[...]
        ids = idbuf[:, chunk_rows(ch), :].reshape(tokens, inner)
        ids = jnp.concatenate([ids] * (f_loc // inner), axis=1)
        for j in range(GROUP):
            e = g * GROUP + j
            q = silu(mm(m, wg[e])) * mm(m, wu[e])
            qbuf[:, j * f_loc:(j + 1) * f_loc] = jnp.where(ids == e, q, 0.0).astype(BF16)
            if j < len(between):
                between[j]()
        part = mm(qbuf[...], wd[g * GROUP * f_loc:(g + 1) * GROUP * f_loc, :])
        if g == 0:
            acc[...] = part
        elif g < experts // GROUP - 1:
            acc[...] += part
        else:
            total = acc[...] + part
            weight = jnp.concatenate([prob[...]] * (d_model // inner), axis=1)
            y_part[ch] = (total * weight).astype(BF16)

    def when_chunk(ch, fn):
        pl.when((ch >= 0) & (ch < chunks))(lambda: fn(ch))

    def loop(n, body):
        def step(i, carry):
            body(i)
            return carry
        lax.fori_loop(0, n, step, 0)

    w_xp2[...] = jnp.zeros_like(w_xp2)
    w_dt2[...] = jnp.zeros_like(w_dt2)
    for k in range(2):
        w_xp2[k * p_dim:(k + 1) * p_dim, k * inner:(k + 1) * inner] = w_xp_ref[...]
        w_dt2[k * p_dim:k * p_dim + dt_rank, k * inner:(k + 1) * inner] = w_dt_ref[...]
    a2[...] = jnp.exp(a_log_ref[...]) * (-LOG2E)
    w_tmp[...] = w_in_ref[...].astype(F32)
    for k in range(2):
        w_in2[:, k * inner:(k + 1) * inner] = w_tmp[pl.ds(k, d_model, stride=2), :].astype(BF16)
    vec_ref[0:1, :] = g_in_ref[...].astype(F32).reshape(1, d_model)
    vec_ref[1:2, :] = g_ff_ref[...].astype(F32).reshape(1, d_model)
    chan_ref[0:4, :] = conv_w_ref[...].astype(F32)
    chan_ref[4:5, :] = conv_b_ref[...].astype(F32).reshape(1, inner)
    chan_ref[5:6, :] = b_dt_ref[...].astype(F32).reshape(1, inner)
    chan_ref[6:7, :] = d_skip_ref[...].reshape(1, inner)
    gains = [g[...].astype(F32).reshape(1, g.shape[0]) for g in (g_dt_ref, g_b_ref, g_c_ref)]
    chan_ref[7:8, :] = jnp.concatenate(gains + gains, axis=1)
    row = lax.broadcasted_iota(jnp.int32, (2 * p_dim, inner), 0)
    for k in range(2 * state_dim):
        at = (k % 2) * p_dim + dt_rank + state_dim + k // 2
        hit = (row == at) | (row == (at + state_dim) % (2 * p_dim)) | (row == (at + 2 * state_dim) % (2 * p_dim))
        spread[:, k * inner:(k + 1) * inner] = jnp.where(hit, 1.0, 0.0).astype(BF16)
    for s in range(steps):
        idbuf[s] = jnp.broadcast_to(ids_ref[s].astype(F32), (inner, batch)).T.astype(jnp.int32)
    pl.semaphore_wait(barrier, 3)
    wo_first()
    for cp in (h_in, *w_ins):
        cp.start()
    x_in.wait()

    def first_body(t):
        stage_in(t)
        when_chunk(t - 3, p_one)

    loop(chunks, first_body)
    for ch in range(chunks - 3, chunks):
        p_one(ch)
    for ch in range(chunks):
        p_two(ch)
    for ch in range(3):
        p_three(ch)
    ag_relay(wo_block, chunks)
    h_in.wait()

    even, odd = (pn_a, d_a, dx_a), (pn_b, d_b, dx_b)

    def p_done(ch):
        p_ar(ch)[0]["back"].wait_recv()

    def ssm_tick(t, now, later):
        when_chunk(t + 1, p_done)
        stage_ssm(t, *now)
        stage_norm(jnp.minimum(t + 1, chunks - 1), *later)
        ag_first(yg_block(t), t)
        when_chunk(t + 3, p_three)
        pl.when(t == 4)(lambda: ag_far(wo_block, chunks))
        when_chunk(t - 3, lambda ch: ag_relay(yg_block(ch), ch))
        when_chunk(t - 6, lambda ch: ag_far(yg_block(ch), ch))

    def ssm_body(t):
        ssm_tick(2 * t, even, odd)
        ssm_tick(2 * t + 1, odd, even)

    p_done(0)
    stage_norm(0, *even)
    loop(chunks // 2, ssm_body)
    wo_in.wait()
    for cp in w_ins:
        cp.wait()
    ag_done(wo_block, chunks)

    def got_yg(ch):
        ag_done(yg_block(ch), ch)

    def moe_tick(t, now, later):
        for g in range(experts // GROUP - 1):
            stage_experts(t, g, *now)
            if g == 0:
                when_chunk(t + 5, lambda ch: ag_relay(yg_block(ch), ch))
                when_chunk(t - 4, y_three)
            elif g == 1:
                when_chunk(t + 2, lambda ch: ag_far(yg_block(ch), ch))
                when_chunk(t - 1, y_one)
            else:
                when_chunk(t - 2, y_two)
        if later is not None:
            got_yg(t + 1)
        stage_experts(t, experts // GROUP - 1, *now, mid_parts(t + 1, *later) if later is not None else ())
        y_ar(t)[0]["swap"].start()

    even, odd = (m_a, prob_a), (m_b, prob_b)

    def moe_body(i):
        moe_tick(2 * i, even, odd)
        moe_tick(2 * i + 1, odd, even)

    got_yg(0)
    for part in mid_parts(0, *even):
        part()
    loop(chunks // 2 - 1, moe_body)
    moe_tick(chunks - 2, even, odd)
    moe_tick(chunks - 1, odd, None)
    last = chunks - 1
    y_three(last - 3)
    y_one(last)
    y_two(last - 1)
    y_three(last - 2)
    y_two(last)
    y_three(last - 1)
    y_three(last)

    def drain(ch):
        y_four(ch)
        ag_drain(yg_block(ch), ch)
        for cs, _ in (p_ar(ch), y_ar(ch)):
            cs["sent"].wait_send()

    loop(chunks, drain)
    ag_drain(wo_block, chunks)


def store_kernel(y_in, h_in, conv_in, y_out, h_out, conv_out, sem):
    pairs = ((h_in, h_out), (y_in, y_out), (conv_in, conv_out))
    copies = [pltpu.make_async_copy(src, dst, sem.at[i]) for i, (src, dst) in enumerate(pairs)]
    for cp in copies:
        cp.start()
    for cp in copies:
        cp.wait()


def solution(mesh):
    act_spec = P(None, "dp", None)
    state_spec = P("dp", "tp", None)
    in_specs = (act_spec, state_spec, state_spec, act_spec, P(None), P(None, None, "tp"), P("tp", None), P("tp"), P("tp", None), P(None), P(None), P(None), P(None, "tp"), P("tp"), P("tp", None), P("tp"), P("tp", None), P(None), P(None, None), P(None, None, "tp"), P(None, None, "tp"), P(None, "tp", None))
    out_specs = (act_spec, state_spec, state_spec)

    def layer_steps(x_steps, conv_state, ssm_state, expert_ids, g_in, w_in, conv_w, conv_b, w_xp, g_dt, g_b, g_c, w_dt, b_dt, a_log, d_skip, w_out, g_ff, w_router, w_gate, w_up, w_down):
        steps, batch, d_model = x_steps.shape
        inner = w_in.shape[2]
        state_dim = a_log.shape[1]
        experts, _, f_loc = w_gate.shape
        p_dim = w_xp.shape[1]
        rows = CHUNK_ROWS
        chunks = batch // rows
        tokens = steps * rows
        group_inner = w_out.shape[0] * mesh.shape["tp"]

        h_flat = jnp.swapaxes(ssm_state, 1, 2).reshape(batch * state_dim, inner)
        conv_t = jnp.transpose(conv_state, (2, 0, 1))

        any_spec = pl.BlockSpec(memory_space=pl.ANY)
        vmem_spec = pl.BlockSpec(memory_space=pltpu.VMEM)
        half = tokens // 2
        p_half = (chunks, half // 2, 2 * p_dim)
        y_half = (chunks, half, d_model)
        dma = pltpu.SemaphoreType.DMA
        scratch = [
            pltpu.VMEM(x_steps.shape, BF16),
            pltpu.VMEM(h_flat.shape, F32),
            pltpu.VMEM((steps, batch, inner), jnp.int32),
            pltpu.VMEM(w_gate.shape, BF16),
            pltpu.VMEM(w_up.shape, BF16),
            pltpu.VMEM((experts * f_loc, d_model), BF16),
            pltpu.VMEM((d_model, 2 * inner), BF16),
            pltpu.VMEM((2 * d_model, inner), F32),
            pltpu.VMEM((2, d_model), F32),
            pltpu.VMEM((8, inner), F32),
            pltpu.VMEM((2 * p_dim, 2 * inner), BF16),
            pltpu.VMEM((2 * p_dim, 2 * inner), BF16),
            pltpu.VMEM((state_dim, inner), F32),
            pltpu.VMEM((2 * p_dim, 2 * state_dim * inner), BF16),
            pltpu.VMEM((chunks, tokens, inner), BF16),
            pltpu.VMEM((chunks, half, 2 * inner), BF16),
            pltpu.VMEM((tokens, inner), F32),
            pltpu.VMEM((half, 2 * p_dim), F32),
            pltpu.VMEM((half, 2 * inner), F32),
            pltpu.VMEM((half, 2 * inner), F32),
            pltpu.VMEM((half, 2 * p_dim), F32),
            pltpu.VMEM((half, 2 * inner), F32),
            pltpu.VMEM((half, 2 * inner), F32),
            pltpu.VMEM((chunks, half, 2 * p_dim), F32),
            pltpu.VMEM(p_half, F32),
            pltpu.VMEM(p_half, F32),
            pltpu.VMEM(p_half, F32),
            pltpu.VMEM(p_half, F32),
            pltpu.VMEM(p_half, F32),
            pltpu.VMEM((chunks, half, 2 * p_dim), F32),
            pltpu.VMEM((chunks, group_inner // inner, tokens, inner), BF16),
            pltpu.VMEM((group_inner, d_model), BF16),
            pltpu.VMEM((chunks, tokens, d_model), BF16),
            pltpu.VMEM((tokens, d_model), BF16),
            pltpu.VMEM((tokens, d_model), BF16),
            pltpu.VMEM((tokens, GROUP * f_loc), BF16),
            pltpu.VMEM((tokens, d_model), F32),
            pltpu.VMEM((tokens, inner), F32),
            pltpu.VMEM((tokens, inner), F32),
            pltpu.VMEM((chunks, tokens, d_model), BF16),
            pltpu.VMEM(y_half, BF16),
            pltpu.VMEM(y_half, BF16),
            pltpu.VMEM(y_half, BF16),
            pltpu.VMEM(y_half, BF16),
            pltpu.VMEM(y_half, BF16),
            dma((6,)),
            dma((chunks,)),
            dma((chunks, 4)),
            dma((chunks,)),
            dma((chunks, 4)),
            dma((chunks + 1,)),
            dma((chunks + 1, 4)),
        ]
        y, h_new, conv_new = pl.pallas_call(
            layer_kernel,
            out_shape=(
                pltpu.VMEM(x_steps.shape, BF16),
                pltpu.VMEM(h_flat.shape, F32),
                pltpu.VMEM(conv_t.shape, BF16),
            ),
            in_specs=[any_spec] * 6 + [vmem_spec] * 16,
            out_specs=(vmem_spec,) * 3,
            scratch_shapes=scratch,
            compiler_params=pltpu.CompilerParams(collective_id=0, has_side_effects=True, vmem_limit_bytes=57 * 1024 * 1024),
        )(
            x_steps, h_flat, w_gate, w_up, w_down.reshape(experts * f_loc, d_model), w_out,
            jnp.transpose(expert_ids, (0, 2, 1)), conv_t, w_in.reshape(2 * d_model, inner), g_in, g_ff, conv_w.T, conv_b, b_dt, d_skip,
            g_dt, g_b, g_c, w_xp.T, w_dt, a_log.T, w_router.T,
        )
        y, h_new, conv_new = pl.pallas_call(
            store_kernel,
            out_shape=[jax.ShapeDtypeStruct(v.shape, v.dtype) for v in (y, h_new, conv_new)],
            in_specs=[vmem_spec] * 3,
            out_specs=[any_spec] * 3,
            scratch_shapes=[dma((3,))],
            compiler_params=pltpu.CompilerParams(vmem_limit_bytes=1024 * 1024),
        )(*(pltpu.with_memory_space_constraint(v, pltpu.VMEM) for v in (y, h_new, conv_new)))
        h_new = jnp.swapaxes(h_new.reshape(batch, state_dim, inner), 1, 2)
        return y, jnp.transpose(conv_new, (1, 2, 0)), h_new

    return jax.shard_map(layer_steps, mesh=mesh, in_specs=in_specs, out_specs=out_specs, check_vma=False)
```

```python
import functools
import math

import jax
import jax.numpy as jnp
from jax import lax
from jax.experimental import pallas as pl
from jax.experimental.pallas import tpu as pltpu
from jax.sharding import PartitionSpec as P

EPSILON = 1e-6
F32 = jnp.float32
BF16 = jnp.bfloat16
CHUNK_ROWS = 64
GROUP = 4
LOG2E = math.log2(math.e)


class Lazy:
    def __init__(self, **makers):
        self.makers = makers

    def __getitem__(self, name):
        return self.makers[name]()


def silu(v):
    return v * jax.nn.sigmoid(v)


def nt_dot(lhs, rhs_t):
    return lax.dot_general(lhs, rhs_t, (((1,), (1,)), ((), ())), preferred_element_type=F32)


def mm(lhs, rhs):
    return jnp.dot(lhs, rhs, preferred_element_type=F32)


def layer_kernel(
    x_ref, h_hbm, wg_hbm, wu_hbm, wd_hbm, w_out_hbm,
    ids_ref, conv_ref, w_in_ref, g_in_ref, g_ff_ref, conv_w_ref, conv_b_ref, b_dt_ref, d_skip_ref,
    g_dt_ref, g_b_ref, g_c_ref, w_xp_ref, w_dt_ref, a_log_ref, w_router_ref,
    y_ref, h_ref, conv_out_ref,
    hbuf, idbuf, wg, wu, wd, w_in2, w_tmp, vec_ref, chan_ref, w_xp2, w_dt2, a2, spread,
    zbuf, xcbuf, yacc, pn_a, d_a, dx_a, pn_b, d_b, dx_b,
    p_part, p_r0, p_s1, p_r1, p_s2, p_r2, p_sum,
    yg_all, wo_all, ubuf, m_a, m_b, qbuf, acc, prob_a, prob_b,
    y_part, y_r0, y_s1, y_r1, y_s2, y_r2,
    in_sem, p_send, p_recv, y_send, y_recv, l_recv, g_send, g_recv,
):
    steps, batch, d_model = x_ref.shape
    state_dim, inner = a_log_ref.shape
    dt_rank = w_dt_ref.shape[0]
    p_dim = w_xp_ref.shape[0]
    experts = wg_hbm.shape[0]
    f_loc = wg_hbm.shape[2]
    rows = CHUNK_ROWS
    chunks = batch // rows
    tokens = steps * rows
    half_rows = tokens // 2

    tp = lax.axis_index("tp")
    core = tp % 2
    chip = tp // 2
    other = 1 - core
    chip_a = chip + 1 - 2 * (chip % 2)
    chip_b = 3 - chip
    chip_far = (chip + 2) % 4
    mate = {"tp": 2 * chip + other}
    peer_a = {"tp": 2 * chip_a + core}
    peer_b = {"tp": 2 * chip_b + core}

    def copy_to(src, dst, send_sem, recv_sem, peer):
        return pltpu.make_async_remote_copy(
            src_ref=src, dst_ref=dst, send_sem=send_sem, recv_sem=recv_sem, device_id=peer, device_id_type=pl.DeviceIdType.MESH
        )

    h_in = pltpu.make_async_copy(h_hbm, hbuf, in_sem.at[1])
    w_ins = [pltpu.make_async_copy(src, dst, in_sem.at[2 + i]) for i, (src, dst) in enumerate(((wg_hbm, wg), (wu_hbm, wu), (wd_hbm, wd)))]
    my_rows = pl.ds(pl.multiple_of((core * 4 + chip) * inner, inner), inner)
    wo_in = pltpu.make_async_copy(w_out_hbm, wo_all.at[my_rows, :], in_sem.at[5])
    barrier = pltpu.get_barrier_semaphore()
    for peer in (mate, peer_a, peer_b):
        pl.semaphore_signal(barrier, inc=1, device_id=peer, device_id_type=pl.DeviceIdType.MESH)
    wo_in.start()

    def wo_block(c, x):
        return wo_all, lambda lo, n, blocks: (pl.ds(pl.multiple_of((c * 4 + x) * inner + lo, n), n * blocks), slice(None)), inner

    def yg_block(ch):
        def block(c, x):
            return yg_all, lambda lo, n, blocks: (ch, pl.ds(c * 4 + x, blocks), pl.ds(lo, n)), tokens
        return block

    def ag_copies(block, k):
        def cut(c, x, part=None, blocks=1):
            ref, index, n = block(c, x)
            if part is None:
                return ref.at[index(0, n, blocks)]
            return ref.at[index(part * (n // 2), n // 2, 1)]

        def make(idx, c, src, peer, part=None, blocks=1):
            ref = cut(c, src, part, blocks)
            return copy_to(ref, ref, g_send.at[k], g_recv.at[k, idx], peer)

        return Lazy(
            own_a=lambda: make(0, core, chip, peer_a), own_b=lambda: make(1, core, chip, peer_b),
            fwd_b=lambda: make(2, core, chip_a, peer_b, 0), fwd_a=lambda: make(2, core, chip_b, peer_a, 1),
            m_own=lambda: make(3, core, chip, mate), m_a=lambda: make(3, core, chip_a, mate),
            m_b=lambda: make(3, core, chip_b, mate), m_far=lambda: make(3, core, chip_far, mate),
            got_a=lambda: make(0, core, chip_a, mate), got_b=lambda: make(1, core, chip_b, mate),
            got_far=lambda: make(2, core, chip_far, mate), got_mate=lambda: make(3, other, 0, mate, blocks=4),
            sent=lambda: make(3, 0, 0, mate, blocks=7),
        )

    def wo_first():
        for idx, peer in ((0, peer_a), (1, peer_b), (3, mate)):
            copy_to(w_out_hbm, wo_all.at[my_rows, :], g_send.at[chunks], g_recv.at[chunks, idx], peer).start()

    def ag_first(block, k):
        cs = ag_copies(block, k)
        cs["own_a"].start()
        cs["own_b"].start()
        cs["m_own"].start()

    def ag_relay(block, k):
        cs = ag_copies(block, k)
        cs["got_a"].wait_recv()
        cs["fwd_b"].start()
        cs["got_b"].wait_recv()
        cs["fwd_a"].start()
        cs["m_a"].start()
        cs["m_b"].start()

    def ag_far(block, k):
        cs = ag_copies(block, k)
        cs["got_far"].wait_recv()
        cs["m_far"].start()

    def ag_done(block, k):
        ag_copies(block, k)["got_mate"].wait_recv()

    def ag_drain(block, k):
        ag_copies(block, k)["sent"].wait_send()

    def ar_copies(part, r0, s1, r1, s2, r2, total_keep, total_give, send, recv, ch, n):
        q = n // 4
        keep = pl.ds(pl.multiple_of(core * (n // 2), n // 2), n // 2)
        give = pl.ds(pl.multiple_of(other * (n // 2), n // 2), n // 2)
        lo, hi = pl.ds(0, q), pl.ds(q, q)

        def make(idx, src, dst, peer):
            return copy_to(src, dst, send.at[ch], recv.at[ch, idx], peer)

        return Lazy(
            swap=lambda: make(0, part.at[ch, give], r0.at[ch], mate),
            a1=lambda: make(1, s1.at[ch, lo], r1.at[ch, lo], peer_a), b1=lambda: make(1, s1.at[ch, hi], r1.at[ch, hi], peer_b),
            a2=lambda: make(2, s2.at[ch, lo], r2.at[ch, lo], peer_b), b2=lambda: make(2, s2.at[ch, hi], r2.at[ch, hi], peer_a),
            out=lambda: make(3, total_keep(), total_keep(), mate),
            got_1=lambda: make(1, s1.at[ch], r1.at[ch], mate), got_2=lambda: make(2, s2.at[ch], r2.at[ch], mate),
            back=lambda: make(3, total_give(), total_give(), mate),
            sent=lambda: make(0, part.at[pl.ds(0, 2)], part.at[pl.ds(0, 2)], mate),
        ), keep

    def p_ar(ch):
        def total(c):
            return lambda: p_sum.at[ch, pl.ds(pl.multiple_of(c * (half_rows // 2), half_rows // 2), half_rows // 2)]
        return ar_copies(p_part, p_r0, p_s1, p_r1, p_s2, p_r2, total(core), total(other), p_send, p_recv, ch, half_rows)

    def y_ar(ch):
        def total(c):
            return lambda: y_ref.at[pl.ds(c * (steps // 2), steps // 2), chunk_rows(ch)]
        return ar_copies(y_part, y_r0, y_s1, y_r1, y_s2, y_r2, total(core), total(other), y_send, y_recv, ch, tokens)

    def ar_one(cs, keep, part, r0, s1, ch):
        cs["swap"].wait_recv()
        s1[ch] = (part[ch, keep].astype(F32) + r0[ch].astype(F32)).astype(s1.dtype)
        cs["a1"].start()
        cs["b1"].start()

    def ar_two(cs, s1, r1, s2, ch):
        cs["got_1"].wait_recv()
        s2[ch] = (s1[ch].astype(F32) + r1[ch].astype(F32)).astype(s2.dtype)
        cs["a2"].start()
        cs["b2"].start()

    def p_one(ch):
        cs, keep = p_ar(ch)
        ar_one(cs, keep, p_part, p_r0, p_s1, ch)

    def p_two(ch):
        cs, _ = p_ar(ch)
        ar_two(cs, p_s1, p_r1, p_s2, ch)

    def p_three(ch):
        cs, keep = p_ar(ch)
        cs["got_2"].wait_recv()
        p_sum[ch, keep] = p_s2[ch] + p_r2[ch]
        cs["out"].start()

    def y_one(ch):
        cs, keep = y_ar(ch)
        ar_one(cs, keep, y_part, y_r0, y_s1, ch)

    def y_two(ch):
        cs, _ = y_ar(ch)
        ar_two(cs, y_s1, y_r1, y_s2, ch)

    def y_three(ch):
        cs, keep = y_ar(ch)
        cs["got_2"].wait_recv()
        moe_sum = y_s2[ch].astype(F32) + y_r2[ch].astype(F32)
        y_new = (ubuf[ch, keep].astype(F32) + moe_sum).astype(BF16)
        y_ref[pl.ds(core * (steps // 2), steps // 2), chunk_rows(ch), :] = y_new.reshape(steps // 2, rows, d_model)
        cs["out"].start()

    def y_four(ch):
        cs, _ = y_ar(ch)
        cs["back"].wait_recv()

    def chunk_rows(ch):
        return pl.ds(pl.multiple_of(ch * rows, rows), rows)

    def stage_in(ch):
        xf = x_ref[:, chunk_rows(ch), :].reshape(tokens, d_model).astype(F32)
        scale = lax.rsqrt(jnp.mean(xf * xf, axis=-1, keepdims=True) + EPSILON)
        norm = (xf * scale * vec_ref[0:1, :]).astype(BF16)
        proj = mm(norm, w_in2[...]).astype(BF16)
        zbuf[ch] = proj[:, inner:]
        xi = proj[:, :inner]
        win = [conv_ref[j, chunk_rows(ch), :].astype(F32) for j in range(3)]
        win += [xi[s * rows:(s + 1) * rows].astype(F32) for s in range(steps)]
        for s in range(steps):
            pre = chan_ref[4:5, :]
            for j in range(4):
                pre = pre + win[s + j] * chan_ref[j:j + 1, :]
            lane = (s // 2) * inner
            xcbuf[ch, (s % 2) * rows:(s % 2 + 1) * rows, lane:lane + inner] = silu(pre).astype(BF16)
        for j in range(3):
            conv_out_ref[j, chunk_rows(ch), :] = xi[(j + 1) * rows:(j + 2) * rows]
        p_part[ch] = nt_dot(xcbuf[ch], w_xp2[...])
        cs, _ = p_ar(ch)
        cs["swap"].start()

    def stage_norm(ch, pnbuf, dbuf, dxbuf):
        p = p_sum[ch]
        lane = lax.broadcasted_iota(jnp.int32, p.shape, 1)
        sq = p * p
        mean = jnp.zeros_like(p)
        for base in (0, p_dim):
            for lo, n in ((0, dt_rank), (dt_rank, state_dim), (dt_rank + state_dim, state_dim)):
                inside = (lane >= base + lo) & (lane < base + lo + n)
                total = jnp.sum(jnp.where(inside, sq, 0.0), axis=-1, keepdims=True) * (1.0 / n)
                mean = jnp.where(inside, total, mean)
        pn = p * lax.rsqrt(mean + EPSILON) * chan_ref[7:8, :]
        pnbuf[...] = pn
        pre = mm(pn.astype(BF16), w_dt2[...])
        bias = chan_ref[5:6, :]
        pre = pre + jnp.concatenate([bias, bias], axis=1)
        delta = jnp.maximum(pre, 0.0) + jnp.log1p(jnp.exp(-jnp.abs(pre)))
        dbuf[...] = delta
        dxbuf[...] = delta * xcbuf[ch].astype(F32)

    def stage_ssm(ch, pnbuf, dbuf, dxbuf):
        pn = pnbuf[...]
        lane = lax.broadcasted_iota(jnp.int32, pn.shape, 1)
        is_c = (lane % p_dim) >= dt_rank + state_dim
        first = pn.astype(BF16).astype(F32)
        second = (pn - first).astype(BF16).astype(F32)
        third = pn - first - second
        parts = [jnp.where(is_c, v, 0.0) for v in (first, second, third)]
        split = (parts[0] + pltpu.roll(parts[1], state_dim, 1) + pltpu.roll(parts[2], 2 * state_dim, 1)).astype(BF16)
        skip = chan_ref[6:7, :]

        def at(s):
            return slice((s % 2) * rows, (s % 2 + 1) * rows), slice((s // 2) * inner, (s // 2 + 1) * inner)

        for s in range(steps):
            yacc[s * rows:(s + 1) * rows, :] = skip * xcbuf[(ch, *at(s))].astype(F32)
        for n in range(state_dim):
            c_all = mm(split, spread[:, 2 * n * inner:2 * (n + 1) * inner])
            b_all = [jnp.broadcast_to(pn[:, k:k + 1], (half_rows, inner)) for k in (dt_rank + n, p_dim + dt_rank + n)]
            where = pl.ds(ch * rows * state_dim + n, rows, stride=state_dim)
            h = hbuf[where, :]
            a_n = a2[n:n + 1, :]
            for s in range(steps):
                r, c = at(s)
                h = jnp.exp2(dbuf[r, c] * a_n) * h + dxbuf[r, c] * b_all[s // 2][r]
                yacc[s * rows:(s + 1) * rows, :] += h * c_all[r, c]
            h_ref[where, :] = h
        yg_all[ch, core * 4 + chip] = (yacc[...] * silu(zbuf[ch].astype(F32))).astype(BF16)

    def mid_one(ch):
        mix = mm(jnp.concatenate([yg_all[ch, k] for k in range(yg_all.shape[1])], axis=1), wo_all[...])
        xf = x_ref[:, chunk_rows(ch), :].reshape(tokens, d_model).astype(F32)
        u = (xf + mix).astype(BF16)
        ubuf[ch] = u

    def mid_two(ch, mbuf):
        uf = ubuf[ch].astype(F32)
        scale = lax.rsqrt(jnp.mean(uf * uf, axis=-1, keepdims=True) + EPSILON)
        mbuf[...] = (uf * scale * vec_ref[1:2, :]).astype(BF16)

    def mid_three(ch, mbuf, prob):
        logits = nt_dot(mbuf[...], w_router_ref[...])
        peak = jnp.max(logits, axis=-1, keepdims=True)
        ex = jnp.exp(logits - peak)
        ids = idbuf[:, chunk_rows(ch), 0:experts].reshape(tokens, experts)
        hit = ids == lax.broadcasted_iota(jnp.int32, (tokens, experts), 1)
        chosen = jnp.sum(jnp.where(hit, ex, 0.0), axis=-1, keepdims=True) / jnp.sum(ex, axis=-1, keepdims=True)
        prob[...] = jnp.broadcast_to(chosen, prob.shape)

    def mid_parts(ch, mbuf, prob):
        return [lambda: mid_one(ch), lambda: mid_two(ch, mbuf), lambda: mid_three(ch, mbuf, prob)]

    def stage_experts(ch, g, mbuf, prob, between=()):
        m = mbuf[...]
        ids = idbuf[:, chunk_rows(ch), :].reshape(tokens, inner)
        ids = jnp.concatenate([ids] * (f_loc // inner), axis=1)
        for j in range(GROUP):
            e = g * GROUP + j
            q = silu(mm(m, wg[e])) * mm(m, wu[e])
            qbuf[:, j * f_loc:(j + 1) * f_loc] = jnp.where(ids == e, q, 0.0).astype(BF16)
            if j < len(between):
                between[j]()
        part = mm(qbuf[...], wd[g * GROUP * f_loc:(g + 1) * GROUP * f_loc, :])
        if g == 0:
            acc[...] = part
        elif g < experts // GROUP - 1:
            acc[...] += part
        else:
            total = acc[...] + part
            weight = jnp.concatenate([prob[...]] * (d_model // inner), axis=1)
            y_part[ch] = (total * weight).astype(BF16)

    def when_chunk(ch, fn):
        pl.when((ch >= 0) & (ch < chunks))(lambda: fn(ch))

    def loop(n, body):
        def step(i, carry):
            body(i)
            return carry
        lax.fori_loop(0, n, step, 0)

    w_xp2[...] = jnp.zeros_like(w_xp2)
    w_dt2[...] = jnp.zeros_like(w_dt2)
    for k in range(2):
        w_xp2[k * p_dim:(k + 1) * p_dim, k * inner:(k + 1) * inner] = w_xp_ref[...]
        w_dt2[k * p_dim:k * p_dim + dt_rank, k * inner:(k + 1) * inner] = w_dt_ref[...]
    a2[...] = jnp.exp(a_log_ref[...]) * (-LOG2E)
    w_tmp[...] = w_in_ref[...].astype(F32)
    for k in range(2):
        w_in2[:, k * inner:(k + 1) * inner] = w_tmp[pl.ds(k, d_model, stride=2), :].astype(BF16)
    vec_ref[0:1, :] = g_in_ref[...].astype(F32).reshape(1, d_model)
    vec_ref[1:2, :] = g_ff_ref[...].astype(F32).reshape(1, d_model)
    chan_ref[0:4, :] = conv_w_ref[...].astype(F32)
    chan_ref[4:5, :] = conv_b_ref[...].astype(F32).reshape(1, inner)
    chan_ref[5:6, :] = b_dt_ref[...].astype(F32).reshape(1, inner)
    chan_ref[6:7, :] = d_skip_ref[...].reshape(1, inner)
    gains = [g[...].astype(F32).reshape(1, g.shape[0]) for g in (g_dt_ref, g_b_ref, g_c_ref)]
    chan_ref[7:8, :] = jnp.concatenate(gains + gains, axis=1)
    row = lax.broadcasted_iota(jnp.int32, (2 * p_dim, inner), 0)
    for k in range(2 * state_dim):
        at = (k % 2) * p_dim + dt_rank + state_dim + k // 2
        hit = (row == at) | (row == (at + state_dim) % (2 * p_dim)) | (row == (at + 2 * state_dim) % (2 * p_dim))
        spread[:, k * inner:(k + 1) * inner] = jnp.where(hit, 1.0, 0.0).astype(BF16)
    for s in range(steps):
        idbuf[s] = jnp.broadcast_to(ids_ref[s].astype(F32), (inner, batch)).T.astype(jnp.int32)
    pl.semaphore_wait(barrier, 3)
    wo_first()
    for cp in (h_in, *w_ins):
        cp.start()

    def first_body(t):
        stage_in(t)
        when_chunk(t - 3, p_one)

    loop(chunks, first_body)
    for ch in range(chunks - 3, chunks):
        p_one(ch)
    for ch in range(chunks):
        p_two(ch)
    for ch in range(3):
        p_three(ch)
    ag_relay(wo_block, chunks)
    h_in.wait()

    even, odd = (pn_a, d_a, dx_a), (pn_b, d_b, dx_b)

    def p_done(ch):
        p_ar(ch)[0]["back"].wait_recv()

    gather_plan = (
        [(ag_first, 0)],
        [(ag_first, 1)],
        [],
        [(ag_relay, 0), (ag_first, 2)],
        [(ag_first, 3), (ag_far, None)],
        [(ag_relay, 1), (ag_first, 4)],
        [(ag_first, 5), (ag_far, 0)],
        [(ag_relay, 2)] + [(ag_first, ch) for ch in range(6, chunks)],
    )

    def ssm_tick(t, now, later, parity):
        when_chunk(t + 1, p_done)
        stage_ssm(t, *now)
        stage_norm(jnp.minimum(t + 1, chunks - 1), *later)
        when_chunk(t + 3, p_three)
        for tick, events in enumerate(gather_plan):
            if tick % 2 == parity and events:
                def run(events=events):
                    for fn, ch in events:
                        if ch is None:
                            fn(wo_block, chunks)
                        else:
                            fn(yg_block(ch), ch)
                pl.when(t == tick)(run)

    def ssm_body(t):
        ssm_tick(2 * t, even, odd, 0)
        ssm_tick(2 * t + 1, odd, even, 1)

    p_done(0)
    stage_norm(0, *even)
    loop(chunks // 2, ssm_body)
    wo_in.wait()
    for cp in w_ins:
        cp.wait()
    ag_done(wo_block, chunks)

    def got_yg(ch):
        ag_done(yg_block(ch), ch)

    def moe_tick(t, now, later):
        for g in range(experts // GROUP - 1):
            stage_experts(t, g, *now)
            if g == 0:
                pl.when((t >= 1) & (2 * t + 2 < chunks))(lambda: ag_relay(yg_block(2 * t + 2), 2 * t + 2))
                pl.when((t >= 1) & (t + 1 < chunks))(lambda: ag_far(yg_block(t + 1), t + 1))
                when_chunk(t - 4, y_three)
            elif g == 1:
                pl.when(t == 0)(lambda: ag_far(yg_block(1), 1))
                pl.when(2 * t + 3 < chunks)(lambda: ag_relay(yg_block(2 * t + 3), 2 * t + 3))
                when_chunk(t - 1, y_one)
            else:
                when_chunk(t - 2, y_two)
        if later is not None:
            got_yg(t + 1)
        stage_experts(t, experts // GROUP - 1, *now, mid_parts(t + 1, *later) if later is not None else ())
        y_ar(t)[0]["swap"].start()

    even, odd = (m_a, prob_a), (m_b, prob_b)

    def moe_body(i):
        moe_tick(2 * i, even, odd)
        moe_tick(2 * i + 1, odd, even)

    got_yg(0)
    for part in mid_parts(0, *even):
        part()
    loop(chunks // 2 - 1, moe_body)
    moe_tick(chunks - 2, even, odd)
    moe_tick(chunks - 1, odd, None)
    last = chunks - 1
    quarter = tokens // 4
    pieces = 2
    piece = quarter // pieces

    def last_copy(step, i, src, dst, peers):
        for part, peer in enumerate(peers):
            at = pl.ds(part * quarter + i * piece, piece)
            yield copy_to(src.at[last, at], dst.at[last, at], y_send.at[last], l_recv.at[step, part, i], peer)

    def last_one():
        cs, keep = y_ar(last)
        cs["swap"].wait_recv()
        y_s1[last] = (y_part[last, keep].astype(F32) + y_r0[last].astype(F32)).astype(BF16)
        for i in range(pieces):
            for cp in last_copy(0, i, y_s1, y_r1, (peer_a, peer_b)):
                cp.start()

    def last_two():
        for i in range(pieces):
            for cp in last_copy(0, i, y_s1, y_r1, (peer_a, peer_b)):
                cp.wait_recv()
            for part in range(2):
                at = pl.ds(part * quarter + i * piece, piece)
                y_s2[last, at] = (y_s1[last, at].astype(F32) + y_r1[last, at].astype(F32)).astype(BF16)
            for cp in last_copy(1, i, y_s2, y_r2, (peer_b, peer_a)):
                cp.start()

    def last_three():
        for i in range(pieces):
            for cp in last_copy(1, i, y_s2, y_r2, (peer_b, peer_a)):
                cp.wait_recv()
        cs, keep = y_ar(last)
        moe_sum = y_s2[last].astype(F32) + y_r2[last].astype(F32)
        y_new = (ubuf[last, keep].astype(F32) + moe_sum).astype(BF16)
        y_ref[pl.ds(core * (steps // 2), steps // 2), chunk_rows(last), :] = y_new.reshape(steps // 2, rows, d_model)
        cs["out"].start()

    y_three(last - 3)
    last_one()
    y_two(last - 1)
    y_three(last - 2)
    last_two()
    y_three(last - 1)
    last_three()

    def drain(ch):
        y_four(ch)
        ag_drain(yg_block(ch), ch)
        for cs, _ in (p_ar(ch), y_ar(ch)):
            cs["sent"].wait_send()

    loop(chunks, drain)
    ag_drain(wo_block, chunks)


def store_kernel(y_in, h_in, conv_in, y_out, h_out, conv_out, sem):
    pairs = ((h_in, h_out), (y_in, y_out), (conv_in, conv_out))
    copies = [pltpu.make_async_copy(src, dst, sem.at[i]) for i, (src, dst) in enumerate(pairs)]
    for cp in copies:
        cp.start()
    for cp in copies:
        cp.wait()


def solution(mesh):
    act_spec = P(None, "dp", None)
    state_spec = P("dp", "tp", None)
    in_specs = (act_spec, state_spec, state_spec, act_spec, P(None), P(None, None, "tp"), P("tp", None), P("tp"), P("tp", None), P(None), P(None), P(None), P(None, "tp"), P("tp"), P("tp", None), P("tp"), P("tp", None), P(None), P(None, None), P(None, None, "tp"), P(None, None, "tp"), P(None, "tp", None))
    out_specs = (act_spec, state_spec, state_spec)

    def layer_steps(x_steps, conv_state, ssm_state, expert_ids, g_in, w_in, conv_w, conv_b, w_xp, g_dt, g_b, g_c, w_dt, b_dt, a_log, d_skip, w_out, g_ff, w_router, w_gate, w_up, w_down):
        steps, batch, d_model = x_steps.shape
        inner = w_in.shape[2]
        state_dim = a_log.shape[1]
        experts, _, f_loc = w_gate.shape
        p_dim = w_xp.shape[1]
        rows = CHUNK_ROWS
        chunks = batch // rows
        tokens = steps * rows
        group_inner = w_out.shape[0] * mesh.shape["tp"]

        h_flat = jnp.swapaxes(ssm_state, 1, 2).reshape(batch * state_dim, inner)
        conv_t = jnp.transpose(conv_state, (2, 0, 1))

        any_spec = pl.BlockSpec(memory_space=pl.ANY)
        vmem_spec = pl.BlockSpec(memory_space=pltpu.VMEM)
        half = tokens // 2
        p_half = (chunks, half // 2, 2 * p_dim)
        y_half = (chunks, half, d_model)
        dma = pltpu.SemaphoreType.DMA
        scratch = [
            pltpu.VMEM(h_flat.shape, F32),
            pltpu.VMEM((steps, batch, inner), jnp.int32),
            pltpu.VMEM(w_gate.shape, BF16),
            pltpu.VMEM(w_up.shape, BF16),
            pltpu.VMEM((experts * f_loc, d_model), BF16),
            pltpu.VMEM((d_model, 2 * inner), BF16),
            pltpu.VMEM((2 * d_model, inner), F32),
            pltpu.VMEM((2, d_model), F32),
            pltpu.VMEM((8, inner), F32),
            pltpu.VMEM((2 * p_dim, 2 * inner), BF16),
            pltpu.VMEM((2 * p_dim, 2 * inner), BF16),
            pltpu.VMEM((state_dim, inner), F32),
            pltpu.VMEM((2 * p_dim, 2 * state_dim * inner), BF16),
            pltpu.VMEM((chunks, tokens, inner), BF16),
            pltpu.VMEM((chunks, half, 2 * inner), BF16),
            pltpu.VMEM((tokens, inner), F32),
            pltpu.VMEM((half, 2 * p_dim), F32),
            pltpu.VMEM((half, 2 * inner), F32),
            pltpu.VMEM((half, 2 * inner), F32),
            pltpu.VMEM((half, 2 * p_dim), F32),
            pltpu.VMEM((half, 2 * inner), F32),
            pltpu.VMEM((half, 2 * inner), F32),
            pltpu.VMEM((chunks, half, 2 * p_dim), F32),
            pltpu.VMEM(p_half, F32),
            pltpu.VMEM(p_half, F32),
            pltpu.VMEM(p_half, F32),
            pltpu.VMEM(p_half, F32),
            pltpu.VMEM(p_half, F32),
            pltpu.VMEM((chunks, half, 2 * p_dim), F32),
            pltpu.VMEM((chunks, group_inner // inner, tokens, inner), BF16),
            pltpu.VMEM((group_inner, d_model), BF16),
            pltpu.VMEM((chunks, tokens, d_model), BF16),
            pltpu.VMEM((tokens, d_model), BF16),
            pltpu.VMEM((tokens, d_model), BF16),
            pltpu.VMEM((tokens, GROUP * f_loc), BF16),
            pltpu.VMEM((tokens, d_model), F32),
            pltpu.VMEM((tokens, inner), F32),
            pltpu.VMEM((tokens, inner), F32),
            pltpu.VMEM((chunks, tokens, d_model), BF16),
            pltpu.VMEM(y_half, BF16),
            pltpu.VMEM(y_half, BF16),
            pltpu.VMEM(y_half, BF16),
            pltpu.VMEM(y_half, BF16),
            pltpu.VMEM(y_half, BF16),
            dma((6,)),
            dma((chunks,)),
            dma((chunks, 4)),
            dma((chunks,)),
            dma((chunks, 4)),
            dma((2, 2, 2)),
            dma((chunks + 1,)),
            dma((chunks + 1, 4)),
        ]
        y, h_new, conv_new = pl.pallas_call(
            layer_kernel,
            out_shape=(
                pltpu.VMEM(x_steps.shape, BF16),
                pltpu.VMEM(h_flat.shape, F32),
                pltpu.VMEM(conv_t.shape, BF16),
            ),
            in_specs=[vmem_spec] + [any_spec] * 5 + [vmem_spec] * 16,
            out_specs=(vmem_spec,) * 3,
            scratch_shapes=scratch,
            compiler_params=pltpu.CompilerParams(collective_id=0, has_side_effects=True, vmem_limit_bytes=57 * 1024 * 1024),
        )(
            x_steps, h_flat, w_gate, w_up, w_down.reshape(experts * f_loc, d_model), w_out,
            jnp.transpose(expert_ids, (0, 2, 1)), conv_t, w_in.reshape(2 * d_model, inner), g_in, g_ff, conv_w.T, conv_b, b_dt, d_skip,
            g_dt, g_b, g_c, w_xp.T, w_dt, a_log.T, w_router.T,
        )
        y, h_new, conv_new = pl.pallas_call(
            store_kernel,
            out_shape=[jax.ShapeDtypeStruct(v.shape, v.dtype) for v in (y, h_new, conv_new)],
            in_specs=[vmem_spec] * 3,
            out_specs=[any_spec] * 3,
            scratch_shapes=[dma((3,))],
            compiler_params=pltpu.CompilerParams(vmem_limit_bytes=1024 * 1024),
        )(*(pltpu.with_memory_space_constraint(v, pltpu.VMEM) for v in (y, h_new, conv_new)))
        h_new = jnp.swapaxes(h_new.reshape(batch, state_dim, inner), 1, 2)
        return y, jnp.transpose(conv_new, (1, 2, 0)), h_new

    return jax.shard_map(layer_steps, mesh=mesh, in_specs=in_specs, out_specs=out_specs, check_vma=False)
```

```python
import functools
import math

import jax
import jax.numpy as jnp
from jax import lax
from jax.experimental import pallas as pl
from jax.experimental.pallas import tpu as pltpu
from jax.sharding import PartitionSpec as P

EPSILON = 1e-6
F32 = jnp.float32
BF16 = jnp.bfloat16
CHUNK_ROWS = 64
GROUP = 4
LOG2E = math.log2(math.e)


class Lazy:
    def __init__(self, **makers):
        self.makers = makers

    def __getitem__(self, name):
        return self.makers[name]()


def silu(v):
    return v * jax.nn.sigmoid(v)


def nt_dot(lhs, rhs_t):
    return lax.dot_general(lhs, rhs_t, (((1,), (1,)), ((), ())), preferred_element_type=F32)


def mm(lhs, rhs):
    return jnp.dot(lhs, rhs, preferred_element_type=F32)


def layer_kernel(
    x_ref, h_hbm, wg_hbm, wu_hbm, wd_hbm, w_out_hbm,
    ids_ref, conv_ref, w_in_ref, g_in_ref, g_ff_ref, conv_w_ref, conv_b_ref, b_dt_ref, d_skip_ref,
    g_dt_ref, g_b_ref, g_c_ref, w_xp_ref, w_dt_ref, a_log_ref, w_router_ref,
    y_ref, h_ref, conv_out_ref,
    hbuf, idbuf, wg, wu, wd, w_in2, w_tmp, vec_ref, chan_ref, w_xp2, w_dt2, a2, spread,
    zbuf, xcbuf, yacc, pn_a, d_a, dx_a, pn_b, d_b, dx_b,
    p_part, p_r0, p_s1, p_r1, p_s2, p_r2, p_sum,
    yg_all, wo_all, ubuf, m_a, m_b, qbuf, acc, prob_a, prob_b,
    y_part, y_r0, y_s1, y_r1, y_s2, y_r2,
    in_sem, p_send, p_recv, y_send, y_recv, l_recv, g_send, g_recv,
):
    steps, batch, d_model = x_ref.shape
    state_dim, inner = a_log_ref.shape
    dt_rank = w_dt_ref.shape[0]
    p_dim = w_xp_ref.shape[0]
    experts = wg_hbm.shape[0]
    f_loc = wg_hbm.shape[2]
    rows = CHUNK_ROWS
    chunks = batch // rows
    tokens = steps * rows
    half_rows = tokens // 2

    tp = lax.axis_index("tp")
    core = tp % 2
    chip = tp // 2
    other = 1 - core
    chip_a = chip + 1 - 2 * (chip % 2)
    chip_b = 3 - chip
    chip_far = (chip + 2) % 4
    mate = {"tp": 2 * chip + other}
    peer_a = {"tp": 2 * chip_a + core}
    peer_b = {"tp": 2 * chip_b + core}

    def copy_to(src, dst, send_sem, recv_sem, peer):
        return pltpu.make_async_remote_copy(
            src_ref=src, dst_ref=dst, send_sem=send_sem, recv_sem=recv_sem, device_id=peer, device_id_type=pl.DeviceIdType.MESH
        )

    h_in = pltpu.make_async_copy(h_hbm, hbuf, in_sem.at[1])
    w_ins = [pltpu.make_async_copy(src, dst, in_sem.at[2 + i]) for i, (src, dst) in enumerate(((wg_hbm, wg), (wu_hbm, wu), (wd_hbm, wd)))]
    my_rows = pl.ds(pl.multiple_of((core * 4 + chip) * inner, inner), inner)
    wo_in = pltpu.make_async_copy(w_out_hbm, wo_all.at[my_rows, :], in_sem.at[5])
    barrier = pltpu.get_barrier_semaphore()
    for peer in (mate, peer_a, peer_b):
        pl.semaphore_signal(barrier, inc=1, device_id=peer, device_id_type=pl.DeviceIdType.MESH)
    wo_in.start()

    def wo_block(c, x):
        return wo_all, lambda lo, n, blocks: (pl.ds(pl.multiple_of((c * 4 + x) * inner + lo, n), n * blocks), slice(None)), inner

    def yg_block(ch):
        def block(c, x):
            return yg_all, lambda lo, n, blocks: (ch, pl.ds(c * 4 + x, blocks), pl.ds(lo, n)), tokens
        return block

    def ag_copies(block, k):
        def cut(c, x, part=None, blocks=1):
            ref, index, n = block(c, x)
            if part is None:
                return ref.at[index(0, n, blocks)]
            return ref.at[index(part * (n // 2), n // 2, 1)]

        def make(idx, c, src, peer, part=None, blocks=1):
            ref = cut(c, src, part, blocks)
            return copy_to(ref, ref, g_send.at[k], g_recv.at[k, idx], peer)

        return Lazy(
            own_a=lambda: make(0, core, chip, peer_a), own_b=lambda: make(1, core, chip, peer_b),
            fwd_b=lambda: make(2, core, chip_a, peer_b, 0), fwd_a=lambda: make(2, core, chip_b, peer_a, 1),
            m_own=lambda: make(3, core, chip, mate), m_a=lambda: make(3, core, chip_a, mate),
            m_b=lambda: make(3, core, chip_b, mate), m_far=lambda: make(3, core, chip_far, mate),
            got_a=lambda: make(0, core, chip_a, mate), got_b=lambda: make(1, core, chip_b, mate),
            got_far=lambda: make(2, core, chip_far, mate), got_mate=lambda: make(3, other, 0, mate, blocks=4),
            sent=lambda: make(3, 0, 0, mate, blocks=7),
        )

    def wo_first():
        for idx, peer in ((0, peer_a), (1, peer_b), (3, mate)):
            copy_to(w_out_hbm, wo_all.at[my_rows, :], g_send.at[chunks], g_recv.at[chunks, idx], peer).start()

    def ag_first(block, k):
        cs = ag_copies(block, k)
        cs["own_a"].start()
        cs["own_b"].start()
        cs["m_own"].start()

    def ag_relay(block, k):
        cs = ag_copies(block, k)
        cs["got_a"].wait_recv()
        cs["fwd_b"].start()
        cs["got_b"].wait_recv()
        cs["fwd_a"].start()
        cs["m_a"].start()
        cs["m_b"].start()

    def ag_far(block, k):
        cs = ag_copies(block, k)
        cs["got_far"].wait_recv()
        cs["m_far"].start()

    def ag_done(block, k):
        ag_copies(block, k)["got_mate"].wait_recv()

    def ag_drain(block, k):
        ag_copies(block, k)["sent"].wait_send()

    def ar_copies(part, r0, s1, r1, s2, r2, total_keep, total_give, send, recv, ch, n):
        q = n // 4
        keep = pl.ds(pl.multiple_of(core * (n // 2), n // 2), n // 2)
        give = pl.ds(pl.multiple_of(other * (n // 2), n // 2), n // 2)
        lo, hi = pl.ds(0, q), pl.ds(q, q)

        def make(idx, src, dst, peer):
            return copy_to(src, dst, send.at[ch], recv.at[ch, idx], peer)

        return Lazy(
            swap=lambda: make(0, part.at[ch, give], r0.at[ch], mate),
            a1=lambda: make(1, s1.at[ch, lo], r1.at[ch, lo], peer_a), b1=lambda: make(1, s1.at[ch, hi], r1.at[ch, hi], peer_b),
            a2=lambda: make(2, s2.at[ch, lo], r2.at[ch, lo], peer_b), b2=lambda: make(2, s2.at[ch, hi], r2.at[ch, hi], peer_a),
            out=lambda: make(3, total_keep(), total_keep(), mate),
            got_1=lambda: make(1, s1.at[ch], r1.at[ch], mate), got_2=lambda: make(2, s2.at[ch], r2.at[ch], mate),
            back=lambda: make(3, total_give(), total_give(), mate),
            sent=lambda: make(0, part.at[pl.ds(0, 2)], part.at[pl.ds(0, 2)], mate),
        ), keep

    def p_ar(ch):
        def total(c):
            return lambda: p_sum.at[ch, pl.ds(pl.multiple_of(c * (half_rows // 2), half_rows // 2), half_rows // 2)]
        return ar_copies(p_part, p_r0, p_s1, p_r1, p_s2, p_r2, total(core), total(other), p_send, p_recv, ch, half_rows)

    def y_ar(ch):
        def total(c):
            return lambda: y_ref.at[pl.ds(c * (steps // 2), steps // 2), chunk_rows(ch)]
        return ar_copies(y_part, y_r0, y_s1, y_r1, y_s2, y_r2, total(core), total(other), y_send, y_recv, ch, tokens)

    def ar_one(cs, keep, part, r0, s1, ch):
        cs["swap"].wait_recv()
        s1[ch] = (part[ch, keep].astype(F32) + r0[ch].astype(F32)).astype(s1.dtype)
        cs["a1"].start()
        cs["b1"].start()

    def ar_two(cs, s1, r1, s2, ch):
        cs["got_1"].wait_recv()
        s2[ch] = (s1[ch].astype(F32) + r1[ch].astype(F32)).astype(s2.dtype)
        cs["a2"].start()
        cs["b2"].start()

    def p_one(ch):
        cs, keep = p_ar(ch)
        ar_one(cs, keep, p_part, p_r0, p_s1, ch)

    def p_two(ch):
        cs, _ = p_ar(ch)
        ar_two(cs, p_s1, p_r1, p_s2, ch)

    def p_three(ch):
        cs, keep = p_ar(ch)
        cs["got_2"].wait_recv()
        p_sum[ch, keep] = p_s2[ch] + p_r2[ch]
        cs["out"].start()

    def y_one(ch):
        cs, keep = y_ar(ch)
        ar_one(cs, keep, y_part, y_r0, y_s1, ch)

    def y_two(ch):
        cs, _ = y_ar(ch)
        ar_two(cs, y_s1, y_r1, y_s2, ch)

    def y_three(ch):
        cs, keep = y_ar(ch)
        cs["got_2"].wait_recv()
        moe_sum = y_s2[ch].astype(F32) + y_r2[ch].astype(F32)
        y_new = (ubuf[ch, keep].astype(F32) + moe_sum).astype(BF16)
        y_ref[pl.ds(core * (steps // 2), steps // 2), chunk_rows(ch), :] = y_new.reshape(steps // 2, rows, d_model)
        cs["out"].start()

    def y_four(ch):
        cs, _ = y_ar(ch)
        cs["back"].wait_recv()

    def chunk_rows(ch):
        return pl.ds(pl.multiple_of(ch * rows, rows), rows)

    def stage_in(ch):
        xf = x_ref[:, chunk_rows(ch), :].reshape(tokens, d_model).astype(F32)
        scale = lax.rsqrt(jnp.mean(xf * xf, axis=-1, keepdims=True) + EPSILON)
        norm = (xf * scale * vec_ref[0:1, :]).astype(BF16)
        proj = mm(norm, w_in2[...]).astype(BF16)
        zbuf[ch] = proj[:, inner:]
        xi = proj[:, :inner]
        win = [conv_ref[j, chunk_rows(ch), :].astype(F32) for j in range(3)]
        win += [xi[s * rows:(s + 1) * rows].astype(F32) for s in range(steps)]
        for s in range(steps):
            pre = chan_ref[4:5, :]
            for j in range(4):
                pre = pre + win[s + j] * chan_ref[j:j + 1, :]
            lane = (s // 2) * inner
            xcbuf[ch, (s % 2) * rows:(s % 2 + 1) * rows, lane:lane + inner] = silu(pre).astype(BF16)
        for j in range(3):
            conv_out_ref[j, chunk_rows(ch), :] = xi[(j + 1) * rows:(j + 2) * rows]
        p_part[ch] = nt_dot(xcbuf[ch], w_xp2[...])
        cs, _ = p_ar(ch)
        cs["swap"].start()

    def stage_norm(ch, pnbuf, dbuf, dxbuf):
        p = p_sum[ch]
        lane = lax.broadcasted_iota(jnp.int32, p.shape, 1)
        sq = p * p
        mean = jnp.zeros_like(p)
        for base in (0, p_dim):
            for lo, n in ((0, dt_rank), (dt_rank, state_dim), (dt_rank + state_dim, state_dim)):
                inside = (lane >= base + lo) & (lane < base + lo + n)
                total = jnp.sum(jnp.where(inside, sq, 0.0), axis=-1, keepdims=True) * (1.0 / n)
                mean = jnp.where(inside, total, mean)
        pn = p * lax.rsqrt(mean + EPSILON) * chan_ref[7:8, :]
        pnbuf[...] = pn
        pre = mm(pn.astype(BF16), w_dt2[...])
        bias = chan_ref[5:6, :]
        pre = pre + jnp.concatenate([bias, bias], axis=1)
        delta = jnp.maximum(pre, 0.0) + jnp.log1p(jnp.exp(-jnp.abs(pre)))
        dbuf[...] = delta
        dxbuf[...] = delta * xcbuf[ch].astype(F32)

    def stage_ssm(ch, pnbuf, dbuf, dxbuf):
        pn = pnbuf[...]
        lane = lax.broadcasted_iota(jnp.int32, pn.shape, 1)
        is_c = (lane % p_dim) >= dt_rank + state_dim
        first = pn.astype(BF16).astype(F32)
        second = (pn - first).astype(BF16).astype(F32)
        third = pn - first - second
        parts = [jnp.where(is_c, v, 0.0) for v in (first, second, third)]
        split = (parts[0] + pltpu.roll(parts[1], state_dim, 1) + pltpu.roll(parts[2], 2 * state_dim, 1)).astype(BF16)
        skip = chan_ref[6:7, :]

        def at(s):
            return slice((s % 2) * rows, (s % 2 + 1) * rows), slice((s // 2) * inner, (s // 2 + 1) * inner)

        for s in range(steps):
            yacc[s * rows:(s + 1) * rows, :] = skip * xcbuf[(ch, *at(s))].astype(F32)
        for n in range(state_dim):
            c_all = mm(split, spread[:, 2 * n * inner:2 * (n + 1) * inner])
            b_all = [jnp.broadcast_to(pn[:, k:k + 1], (half_rows, inner)) for k in (dt_rank + n, p_dim + dt_rank + n)]
            where = pl.ds(ch * rows * state_dim + n, rows, stride=state_dim)
            h = hbuf[where, :]
            a_n = a2[n:n + 1, :]
            for s in range(steps):
                r, c = at(s)
                h = jnp.exp2(dbuf[r, c] * a_n) * h + dxbuf[r, c] * b_all[s // 2][r]
                yacc[s * rows:(s + 1) * rows, :] += h * c_all[r, c]
            h_ref[where, :] = h
        yg_all[ch, core * 4 + chip] = (yacc[...] * silu(zbuf[ch].astype(F32))).astype(BF16)

    def mid_one(ch):
        mix = mm(jnp.concatenate([yg_all[ch, k] for k in range(yg_all.shape[1])], axis=1), wo_all[...])
        xf = x_ref[:, chunk_rows(ch), :].reshape(tokens, d_model).astype(F32)
        u = (xf + mix).astype(BF16)
        ubuf[ch] = u

    def mid_two(ch, mbuf):
        uf = ubuf[ch].astype(F32)
        scale = lax.rsqrt(jnp.mean(uf * uf, axis=-1, keepdims=True) + EPSILON)
        mbuf[...] = (uf * scale * vec_ref[1:2, :]).astype(BF16)

    def mid_three(ch, mbuf, prob):
        logits = nt_dot(mbuf[...], w_router_ref[...])
        peak = jnp.max(logits, axis=-1, keepdims=True)
        ex = jnp.exp(logits - peak)
        ids = idbuf[:, chunk_rows(ch), 0:experts].reshape(tokens, experts)
        hit = ids == lax.broadcasted_iota(jnp.int32, (tokens, experts), 1)
        chosen = jnp.sum(jnp.where(hit, ex, 0.0), axis=-1, keepdims=True) / jnp.sum(ex, axis=-1, keepdims=True)
        prob[...] = jnp.broadcast_to(chosen, prob.shape)

    def mid_parts(ch, mbuf, prob):
        return [lambda: mid_one(ch), lambda: mid_two(ch, mbuf), lambda: mid_three(ch, mbuf, prob)]

    def stage_experts(ch, g, mbuf, prob, between=()):
        m = mbuf[...]
        ids = idbuf[:, chunk_rows(ch), :].reshape(tokens, inner)
        ids = jnp.concatenate([ids] * (f_loc // inner), axis=1)
        for j in range(GROUP):
            e = g * GROUP + j
            q = silu(mm(m, wg[e])) * mm(m, wu[e])
            qbuf[:, j * f_loc:(j + 1) * f_loc] = jnp.where(ids == e, q, 0.0).astype(BF16)
            if j < len(between):
                between[j]()
        part = mm(qbuf[...], wd[g * GROUP * f_loc:(g + 1) * GROUP * f_loc, :])
        if g == 0:
            acc[...] = part
        elif g < experts // GROUP - 1:
            acc[...] += part
        else:
            total = acc[...] + part
            weight = jnp.concatenate([prob[...]] * (d_model // inner), axis=1)
            y_part[ch] = (total * weight).astype(BF16)

    def when_chunk(ch, fn):
        pl.when((ch >= 0) & (ch < chunks))(lambda: fn(ch))

    def loop(n, body):
        def step(i, carry):
            body(i)
            return carry
        lax.fori_loop(0, n, step, 0)

    w_xp2[...] = jnp.zeros_like(w_xp2)
    w_dt2[...] = jnp.zeros_like(w_dt2)
    for k in range(2):
        w_xp2[k * p_dim:(k + 1) * p_dim, k * inner:(k + 1) * inner] = w_xp_ref[...]
        w_dt2[k * p_dim:k * p_dim + dt_rank, k * inner:(k + 1) * inner] = w_dt_ref[...]
    a2[...] = jnp.exp(a_log_ref[...]) * (-LOG2E)
    w_tmp[...] = w_in_ref[...].astype(F32)
    for k in range(2):
        w_in2[:, k * inner:(k + 1) * inner] = w_tmp[pl.ds(k, d_model, stride=2), :].astype(BF16)
    vec_ref[0:1, :] = g_in_ref[...].astype(F32).reshape(1, d_model)
    vec_ref[1:2, :] = g_ff_ref[...].astype(F32).reshape(1, d_model)
    chan_ref[0:4, :] = conv_w_ref[...].astype(F32)
    chan_ref[4:5, :] = conv_b_ref[...].astype(F32).reshape(1, inner)
    chan_ref[5:6, :] = b_dt_ref[...].astype(F32).reshape(1, inner)
    chan_ref[6:7, :] = d_skip_ref[...].reshape(1, inner)
    gains = [g[...].astype(F32).reshape(1, g.shape[0]) for g in (g_dt_ref, g_b_ref, g_c_ref)]
    chan_ref[7:8, :] = jnp.concatenate(gains + gains, axis=1)
    row = lax.broadcasted_iota(jnp.int32, (2 * p_dim, inner), 0)
    for k in range(2 * state_dim):
        at = (k % 2) * p_dim + dt_rank + state_dim + k // 2
        hit = (row == at) | (row == (at + state_dim) % (2 * p_dim)) | (row == (at + 2 * state_dim) % (2 * p_dim))
        spread[:, k * inner:(k + 1) * inner] = jnp.where(hit, 1.0, 0.0).astype(BF16)
    for s in range(steps):
        idbuf[s] = jnp.broadcast_to(ids_ref[s].astype(F32), (inner, batch)).T.astype(jnp.int32)
    pl.semaphore_wait(barrier, 3)
    wo_first()
    for cp in (h_in, *w_ins):
        cp.start()

    def first_body(t):
        stage_in(t)
        when_chunk(t - 3, p_one)

    loop(chunks, first_body)
    for ch in range(chunks - 3, chunks):
        p_one(ch)
    for ch in range(chunks):
        p_two(ch)
    for ch in range(3):
        p_three(ch)
    ag_relay(wo_block, chunks)
    h_in.wait()

    even, odd = (pn_a, d_a, dx_a), (pn_b, d_b, dx_b)

    def p_done(ch):
        p_ar(ch)[0]["back"].wait_recv()

    gather_plan = (
        [(ag_first, 0)],
        [(ag_first, 1)],
        [],
        [(ag_relay, 0), (ag_first, 2)],
        [(ag_first, 3), (ag_far, None)],
        [(ag_relay, 1), (ag_first, 4)],
        [(ag_first, 5), (ag_far, 0)],
        [(ag_relay, 2)] + [(ag_first, ch) for ch in range(6, chunks)],
    )

    def ssm_tick(t, now, later, parity):
        when_chunk(t + 1, p_done)
        stage_ssm(t, *now)
        stage_norm(jnp.minimum(t + 1, chunks - 1), *later)
        when_chunk(t + 3, p_three)
        for tick, events in enumerate(gather_plan):
            if tick % 2 == parity and events:
                def run(events=events):
                    for fn, ch in events:
                        if ch is None:
                            fn(wo_block, chunks)
                        else:
                            fn(yg_block(ch), ch)
                pl.when(t == tick)(run)

    def ssm_body(t):
        ssm_tick(2 * t, even, odd, 0)
        ssm_tick(2 * t + 1, odd, even, 1)

    p_done(0)
    stage_norm(0, *even)
    loop(chunks // 2, ssm_body)
    wo_in.wait()
    for cp in w_ins:
        cp.wait()
    ag_done(wo_block, chunks)

    def got_yg(ch):
        ag_done(yg_block(ch), ch)

    def moe_tick(t, now, later):
        for g in range(experts // GROUP - 1):
            stage_experts(t, g, *now)
            if g == 0:
                if t >= 1 and 2 * t + 2 < chunks:
                    ag_relay(yg_block(2 * t + 2), 2 * t + 2)
                if t >= 1 and t + 1 < chunks:
                    ag_far(yg_block(t + 1), t + 1)
                if t >= 4:
                    y_three(t - 4)
            elif g == 1:
                if t == 0:
                    ag_far(yg_block(1), 1)
                if 2 * t + 3 < chunks:
                    ag_relay(yg_block(2 * t + 3), 2 * t + 3)
                if t >= 1:
                    y_one(t - 1)
            elif t >= 2:
                y_two(t - 2)
        if later is not None:
            got_yg(t + 1)
        stage_experts(t, experts // GROUP - 1, *now, mid_parts(t + 1, *later) if later is not None else ())
        y_ar(t)[0]["swap"].start()

    even, odd = (m_a, prob_a), (m_b, prob_b)

    got_yg(0)
    for part in mid_parts(0, *even):
        part()
    for t in range(chunks):
        now, later = (even, odd) if t % 2 == 0 else (odd, even)
        pl.when(core >= 0)(functools.partial(moe_tick, t, now, later if t + 1 < chunks else None))
    last = chunks - 1
    quarter = tokens // 4
    pieces = 2
    piece = quarter // pieces

    def last_copy(step, i, src, dst, peers):
        for part, peer in enumerate(peers):
            at = pl.ds(part * quarter + i * piece, piece)
            yield copy_to(src.at[last, at], dst.at[last, at], y_send.at[last], l_recv.at[step, part, i], peer)

    def last_one():
        cs, keep = y_ar(last)
        cs["swap"].wait_recv()
        y_s1[last] = (y_part[last, keep].astype(F32) + y_r0[last].astype(F32)).astype(BF16)
        for i in range(pieces):
            for cp in last_copy(0, i, y_s1, y_r1, (peer_a, peer_b)):
                cp.start()

    def last_two():
        for i in range(pieces):
            for cp in last_copy(0, i, y_s1, y_r1, (peer_a, peer_b)):
                cp.wait_recv()
            for part in range(2):
                at = pl.ds(part * quarter + i * piece, piece)
                y_s2[last, at] = (y_s1[last, at].astype(F32) + y_r1[last, at].astype(F32)).astype(BF16)
            for cp in last_copy(1, i, y_s2, y_r2, (peer_b, peer_a)):
                cp.start()

    def last_three():
        for i in range(pieces):
            for cp in last_copy(1, i, y_s2, y_r2, (peer_b, peer_a)):
                cp.wait_recv()
        cs, keep = y_ar(last)
        moe_sum = y_s2[last].astype(F32) + y_r2[last].astype(F32)
        y_new = (ubuf[last, keep].astype(F32) + moe_sum).astype(BF16)
        y_ref[pl.ds(core * (steps // 2), steps // 2), chunk_rows(last), :] = y_new.reshape(steps // 2, rows, d_model)
        cs["out"].start()

    y_three(last - 3)
    last_one()
    y_two(last - 1)
    y_three(last - 2)
    last_two()
    y_three(last - 1)
    last_three()

    def drain(ch):
        y_four(ch)
        ag_drain(yg_block(ch), ch)
        for cs, _ in (p_ar(ch), y_ar(ch)):
            cs["sent"].wait_send()

    loop(chunks, drain)
    ag_drain(wo_block, chunks)


def store_kernel(y_in, h_in, conv_in, y_out, h_out, conv_out, sem):
    pairs = ((h_in, h_out), (y_in, y_out), (conv_in, conv_out))
    copies = [pltpu.make_async_copy(src, dst, sem.at[i]) for i, (src, dst) in enumerate(pairs)]
    for cp in copies:
        cp.start()
    for cp in copies:
        cp.wait()


def solution(mesh):
    act_spec = P(None, "dp", None)
    state_spec = P("dp", "tp", None)
    in_specs = (act_spec, state_spec, state_spec, act_spec, P(None), P(None, None, "tp"), P("tp", None), P("tp"), P("tp", None), P(None), P(None), P(None), P(None, "tp"), P("tp"), P("tp", None), P("tp"), P("tp", None), P(None), P(None, None), P(None, None, "tp"), P(None, None, "tp"), P(None, "tp", None))
    out_specs = (act_spec, state_spec, state_spec)

    def layer_steps(x_steps, conv_state, ssm_state, expert_ids, g_in, w_in, conv_w, conv_b, w_xp, g_dt, g_b, g_c, w_dt, b_dt, a_log, d_skip, w_out, g_ff, w_router, w_gate, w_up, w_down):
        steps, batch, d_model = x_steps.shape
        inner = w_in.shape[2]
        state_dim = a_log.shape[1]
        experts, _, f_loc = w_gate.shape
        p_dim = w_xp.shape[1]
        rows = CHUNK_ROWS
        chunks = batch // rows
        tokens = steps * rows
        group_inner = w_out.shape[0] * mesh.shape["tp"]

        h_flat = jnp.swapaxes(ssm_state, 1, 2).reshape(batch * state_dim, inner)
        conv_t = jnp.transpose(conv_state, (2, 0, 1))

        any_spec = pl.BlockSpec(memory_space=pl.ANY)
        vmem_spec = pl.BlockSpec(memory_space=pltpu.VMEM)
        half = tokens // 2
        p_half = (chunks, half // 2, 2 * p_dim)
        y_half = (chunks, half, d_model)
        dma = pltpu.SemaphoreType.DMA
        scratch = [
            pltpu.VMEM(h_flat.shape, F32),
            pltpu.VMEM((steps, batch, inner), jnp.int32),
            pltpu.VMEM(w_gate.shape, BF16),
            pltpu.VMEM(w_up.shape, BF16),
            pltpu.VMEM((experts * f_loc, d_model), BF16),
            pltpu.VMEM((d_model, 2 * inner), BF16),
            pltpu.VMEM((2 * d_model, inner), F32),
            pltpu.VMEM((2, d_model), F32),
            pltpu.VMEM((8, inner), F32),
            pltpu.VMEM((2 * p_dim, 2 * inner), BF16),
            pltpu.VMEM((2 * p_dim, 2 * inner), BF16),
            pltpu.VMEM((state_dim, inner), F32),
            pltpu.VMEM((2 * p_dim, 2 * state_dim * inner), BF16),
            pltpu.VMEM((chunks, tokens, inner), BF16),
            pltpu.VMEM((chunks, half, 2 * inner), BF16),
            pltpu.VMEM((tokens, inner), F32),
            pltpu.VMEM((half, 2 * p_dim), F32),
            pltpu.VMEM((half, 2 * inner), F32),
            pltpu.VMEM((half, 2 * inner), F32),
            pltpu.VMEM((half, 2 * p_dim), F32),
            pltpu.VMEM((half, 2 * inner), F32),
            pltpu.VMEM((half, 2 * inner), F32),
            pltpu.VMEM((chunks, half, 2 * p_dim), F32),
            pltpu.VMEM(p_half, F32),
            pltpu.VMEM(p_half, F32),
            pltpu.VMEM(p_half, F32),
            pltpu.VMEM(p_half, F32),
            pltpu.VMEM(p_half, F32),
            pltpu.VMEM((chunks, half, 2 * p_dim), F32),
            pltpu.VMEM((chunks, group_inner // inner, tokens, inner), BF16),
            pltpu.VMEM((group_inner, d_model), BF16),
            pltpu.VMEM((chunks, tokens, d_model), BF16),
            pltpu.VMEM((tokens, d_model), BF16),
            pltpu.VMEM((tokens, d_model), BF16),
            pltpu.VMEM((tokens, GROUP * f_loc), BF16),
            pltpu.VMEM((tokens, d_model), F32),
            pltpu.VMEM((tokens, inner), F32),
            pltpu.VMEM((tokens, inner), F32),
            pltpu.VMEM((chunks, tokens, d_model), BF16),
            pltpu.VMEM(y_half, BF16),
            pltpu.VMEM(y_half, BF16),
            pltpu.VMEM(y_half, BF16),
            pltpu.VMEM(y_half, BF16),
            pltpu.VMEM(y_half, BF16),
            dma((6,)),
            dma((chunks,)),
            dma((chunks, 4)),
            dma((chunks,)),
            dma((chunks, 4)),
            dma((2, 2, 2)),
            dma((chunks + 1,)),
            dma((chunks + 1, 4)),
        ]
        y, h_new, conv_new = pl.pallas_call(
            layer_kernel,
            out_shape=(
                pltpu.VMEM(x_steps.shape, BF16),
                pltpu.VMEM(h_flat.shape, F32),
                pltpu.VMEM(conv_t.shape, BF16),
            ),
            in_specs=[vmem_spec] + [any_spec] * 5 + [vmem_spec] * 16,
            out_specs=(vmem_spec,) * 3,
            scratch_shapes=scratch,
            compiler_params=pltpu.CompilerParams(collective_id=0, has_side_effects=True, vmem_limit_bytes=57 * 1024 * 1024),
        )(
            x_steps, h_flat, w_gate, w_up, w_down.reshape(experts * f_loc, d_model), w_out,
            jnp.transpose(expert_ids, (0, 2, 1)), conv_t, w_in.reshape(2 * d_model, inner), g_in, g_ff, conv_w.T, conv_b, b_dt, d_skip,
            g_dt, g_b, g_c, w_xp.T, w_dt, a_log.T, w_router.T,
        )
        y, h_new, conv_new = pl.pallas_call(
            store_kernel,
            out_shape=[jax.ShapeDtypeStruct(v.shape, v.dtype) for v in (y, h_new, conv_new)],
            in_specs=[vmem_spec] * 3,
            out_specs=[any_spec] * 3,
            scratch_shapes=[dma((3,))],
            compiler_params=pltpu.CompilerParams(vmem_limit_bytes=1024 * 1024),
        )(*(pltpu.with_memory_space_constraint(v, pltpu.VMEM) for v in (y, h_new, conv_new)))
        h_new = jnp.swapaxes(h_new.reshape(batch, state_dim, inner), 1, 2)
        return y, jnp.transpose(conv_new, (1, 2, 0)), h_new

    return jax.shard_map(layer_steps, mesh=mesh, in_specs=in_specs, out_specs=out_specs, check_vma=False)
```

```python
import functools
import math

import jax
import jax.numpy as jnp
from jax import lax
from jax.experimental import pallas as pl
from jax.experimental.pallas import tpu as pltpu
from jax.sharding import PartitionSpec as P

EPSILON = 1e-6
F32 = jnp.float32
BF16 = jnp.bfloat16
CHUNK_ROWS = 64
GROUP = 4
LOG2E = math.log2(math.e)


class Lazy:
    def __init__(self, **makers):
        self.makers = makers

    def __getitem__(self, name):
        return self.makers[name]()


def silu(v):
    return v * jax.nn.sigmoid(v)


def nt_dot(lhs, rhs_t):
    return lax.dot_general(lhs, rhs_t, (((1,), (1,)), ((), ())), preferred_element_type=F32)


def mm(lhs, rhs):
    return jnp.dot(lhs, rhs, preferred_element_type=F32)


def layer_kernel(
    x_ref, h_hbm, wg_hbm, wu_hbm, wd_hbm, w_out_hbm,
    ids_ref, conv_ref, w_in_ref, g_in_ref, g_ff_ref, conv_w_ref, conv_b_ref, b_dt_ref, d_skip_ref,
    g_dt_ref, g_b_ref, g_c_ref, w_xp_ref, w_dt_ref, a_log_ref, w_router_ref,
    y_ref, h_ref, conv_out_ref,
    hbuf, idbuf, wg, wu, wd, w_in2, w_tmp, vec_ref, chan_ref, w_xp2, w_dt2, a2, spread,
    zbuf, xcbuf, yacc, pn_a, d_a, dx_a, pn_b, d_b, dx_b,
    p_part, p_r0, p_s1, p_r1, p_s2, p_r2, p_sum,
    yg_all, wo_all, ubuf, m_a, m_b, qbuf, acc, prob_a, prob_b,
    y_part, y_r0, y_s1, y_r1, y_s2, y_r2,
    in_sem, p_send, p_recv, y_send, y_recv, l_recv, g_send, g_recv,
):
    steps, batch, d_model = x_ref.shape
    state_dim, inner = a_log_ref.shape
    dt_rank = w_dt_ref.shape[0]
    p_dim = w_xp_ref.shape[0]
    experts = wg_hbm.shape[0]
    f_loc = wg_hbm.shape[2]
    rows = CHUNK_ROWS
    chunks = batch // rows
    tokens = steps * rows
    half_rows = tokens // 2

    tp = lax.axis_index("tp")
    core = tp % 2
    chip = tp // 2
    other = 1 - core
    chip_a = chip + 1 - 2 * (chip % 2)
    chip_b = 3 - chip
    chip_far = (chip + 2) % 4
    mate = {"tp": 2 * chip + other}
    peer_a = {"tp": 2 * chip_a + core}
    peer_b = {"tp": 2 * chip_b + core}

    def copy_to(src, dst, send_sem, recv_sem, peer):
        return pltpu.make_async_remote_copy(
            src_ref=src, dst_ref=dst, send_sem=send_sem, recv_sem=recv_sem, device_id=peer, device_id_type=pl.DeviceIdType.MESH
        )

    h_in = pltpu.make_async_copy(h_hbm, hbuf, in_sem.at[1])
    w_ins = [pltpu.make_async_copy(src, dst, in_sem.at[2 + i]) for i, (src, dst) in enumerate(((wg_hbm, wg), (wu_hbm, wu), (wd_hbm, wd)))]
    my_rows = pl.ds(pl.multiple_of((core * 4 + chip) * inner, inner), inner)
    wo_in = pltpu.make_async_copy(w_out_hbm, wo_all.at[my_rows, :], in_sem.at[5])
    barrier = pltpu.get_barrier_semaphore()
    for peer in (mate, peer_a, peer_b):
        pl.semaphore_signal(barrier, inc=1, device_id=peer, device_id_type=pl.DeviceIdType.MESH)
    wo_in.start()

    def wo_block(c, x):
        return wo_all, lambda lo, n, blocks: (pl.ds(pl.multiple_of((c * 4 + x) * inner + lo, n), n * blocks), slice(None)), inner

    def yg_block(ch):
        def block(c, x):
            return yg_all, lambda lo, n, blocks: (ch, pl.ds(c * 4 + x, blocks), pl.ds(lo, n)), tokens
        return block

    def ag_copies(block, k):
        def cut(c, x, part=None, blocks=1):
            ref, index, n = block(c, x)
            if part is None:
                return ref.at[index(0, n, blocks)]
            return ref.at[index(part * (n // 2), n // 2, 1)]

        def make(idx, c, src, peer, part=None, blocks=1):
            ref = cut(c, src, part, blocks)
            return copy_to(ref, ref, g_send.at[k], g_recv.at[k, idx], peer)

        return Lazy(
            own_a=lambda: make(0, core, chip, peer_a), own_b=lambda: make(1, core, chip, peer_b),
            fwd_b=lambda: make(2, core, chip_a, peer_b, 0), fwd_a=lambda: make(2, core, chip_b, peer_a, 1),
            m_own=lambda: make(3, core, chip, mate), m_a=lambda: make(3, core, chip_a, mate),
            m_b=lambda: make(3, core, chip_b, mate), m_far=lambda: make(3, core, chip_far, mate),
            got_a=lambda: make(0, core, chip_a, mate), got_b=lambda: make(1, core, chip_b, mate),
            got_far=lambda: make(2, core, chip_far, mate), got_mate=lambda: make(3, other, 0, mate, blocks=4),
            sent=lambda: make(3, 0, 0, mate, blocks=7),
        )

    def wo_first():
        for idx, peer in ((0, peer_a), (1, peer_b), (3, mate)):
            copy_to(w_out_hbm, wo_all.at[my_rows, :], g_send.at[chunks], g_recv.at[chunks, idx], peer).start()

    def ag_first(block, k):
        cs = ag_copies(block, k)
        cs["own_a"].start()
        cs["own_b"].start()
        cs["m_own"].start()

    def ag_relay(block, k):
        cs = ag_copies(block, k)
        cs["got_a"].wait_recv()
        cs["fwd_b"].start()
        cs["got_b"].wait_recv()
        cs["fwd_a"].start()
        cs["m_a"].start()
        cs["m_b"].start()

    def ag_far(block, k):
        cs = ag_copies(block, k)
        cs["got_far"].wait_recv()
        cs["m_far"].start()

    def ag_done(block, k):
        ag_copies(block, k)["got_mate"].wait_recv()

    def ag_drain(block, k):
        ag_copies(block, k)["sent"].wait_send()

    def ar_copies(part, r0, s1, r1, s2, r2, total_keep, total_give, send, recv, ch, n):
        q = n // 4
        keep = pl.ds(pl.multiple_of(core * (n // 2), n // 2), n // 2)
        give = pl.ds(pl.multiple_of(other * (n // 2), n // 2), n // 2)
        lo, hi = pl.ds(0, q), pl.ds(q, q)

        def make(idx, src, dst, peer):
            return copy_to(src, dst, send.at[ch], recv.at[ch, idx], peer)

        return Lazy(
            swap=lambda: make(0, part.at[ch, give], r0.at[ch], mate),
            a1=lambda: make(1, s1.at[ch, lo], r1.at[ch, lo], peer_a), b1=lambda: make(1, s1.at[ch, hi], r1.at[ch, hi], peer_b),
            a2=lambda: make(2, s2.at[ch, lo], r2.at[ch, lo], peer_b), b2=lambda: make(2, s2.at[ch, hi], r2.at[ch, hi], peer_a),
            out=lambda: make(3, total_keep(), total_keep(), mate),
            got_1=lambda: make(1, s1.at[ch], r1.at[ch], mate), got_2=lambda: make(2, s2.at[ch], r2.at[ch], mate),
            back=lambda: make(3, total_give(), total_give(), mate),
            sent=lambda: make(0, part.at[pl.ds(0, 2)], part.at[pl.ds(0, 2)], mate),
        ), keep

    def p_ar(ch):
        def total(c):
            return lambda: p_sum.at[ch, pl.ds(pl.multiple_of(c * (half_rows // 2), half_rows // 2), half_rows // 2)]
        return ar_copies(p_part, p_r0, p_s1, p_r1, p_s2, p_r2, total(core), total(other), p_send, p_recv, ch, half_rows)

    def y_ar(ch):
        def total(c):
            return lambda: y_ref.at[pl.ds(c * (steps // 2), steps // 2), chunk_rows(ch)]
        return ar_copies(y_part, y_r0, y_s1, y_r1, y_s2, y_r2, total(core), total(other), y_send, y_recv, ch, tokens)

    def ar_one(cs, keep, part, r0, s1, ch):
        cs["swap"].wait_recv()
        s1[ch] = (part[ch, keep].astype(F32) + r0[ch].astype(F32)).astype(s1.dtype)
        cs["a1"].start()
        cs["b1"].start()

    def ar_two(cs, s1, r1, s2, ch):
        cs["got_1"].wait_recv()
        s2[ch] = (s1[ch].astype(F32) + r1[ch].astype(F32)).astype(s2.dtype)
        cs["a2"].start()
        cs["b2"].start()

    def p_one(ch):
        cs, keep = p_ar(ch)
        ar_one(cs, keep, p_part, p_r0, p_s1, ch)

    def p_two(ch):
        cs, _ = p_ar(ch)
        ar_two(cs, p_s1, p_r1, p_s2, ch)

    def p_three(ch):
        cs, keep = p_ar(ch)
        cs["got_2"].wait_recv()
        p_sum[ch, keep] = p_s2[ch] + p_r2[ch]
        cs["out"].start()

    def y_one(ch):
        cs, keep = y_ar(ch)
        ar_one(cs, keep, y_part, y_r0, y_s1, ch)

    def y_two(ch):
        cs, _ = y_ar(ch)
        ar_two(cs, y_s1, y_r1, y_s2, ch)

    def y_three(ch):
        cs, keep = y_ar(ch)
        cs["got_2"].wait_recv()
        moe_sum = y_s2[ch].astype(F32) + y_r2[ch].astype(F32)
        y_new = (ubuf[ch, keep].astype(F32) + moe_sum).astype(BF16)
        y_ref[pl.ds(core * (steps // 2), steps // 2), chunk_rows(ch), :] = y_new.reshape(steps // 2, rows, d_model)
        cs["out"].start()

    def y_four(ch):
        cs, _ = y_ar(ch)
        cs["back"].wait_recv()

    def chunk_rows(ch):
        return pl.ds(pl.multiple_of(ch * rows, rows), rows)

    def stage_in(ch):
        xf = x_ref[:, chunk_rows(ch), :].reshape(tokens, d_model).astype(F32)
        scale = lax.rsqrt(jnp.mean(xf * xf, axis=-1, keepdims=True) + EPSILON)
        norm = (xf * scale * vec_ref[0:1, :]).astype(BF16)
        proj = mm(norm, w_in2[...]).astype(BF16)
        zbuf[ch] = proj[:, inner:]
        xi = proj[:, :inner]
        win = [conv_ref[j, chunk_rows(ch), :].astype(F32) for j in range(3)]
        win += [xi[s * rows:(s + 1) * rows].astype(F32) for s in range(steps)]
        for s in range(steps):
            pre = chan_ref[4:5, :]
            for j in range(4):
                pre = pre + win[s + j] * chan_ref[j:j + 1, :]
            lane = (s // 2) * inner
            xcbuf[ch, (s % 2) * rows:(s % 2 + 1) * rows, lane:lane + inner] = silu(pre).astype(BF16)
        for j in range(3):
            conv_out_ref[j, chunk_rows(ch), :] = xi[(j + 1) * rows:(j + 2) * rows]
        p_part[ch] = nt_dot(xcbuf[ch], w_xp2[...])
        cs, _ = p_ar(ch)
        cs["swap"].start()

    def stage_norm(ch, pnbuf, dbuf, dxbuf):
        p = p_sum[ch]
        lane = lax.broadcasted_iota(jnp.int32, p.shape, 1)
        sq = p * p
        mean = jnp.zeros_like(p)
        for base in (0, p_dim):
            for lo, n in ((0, dt_rank), (dt_rank, state_dim), (dt_rank + state_dim, state_dim)):
                inside = (lane >= base + lo) & (lane < base + lo + n)
                total = jnp.sum(jnp.where(inside, sq, 0.0), axis=-1, keepdims=True) * (1.0 / n)
                mean = jnp.where(inside, total, mean)
        pn = p * lax.rsqrt(mean + EPSILON) * chan_ref[7:8, :]
        pnbuf[...] = pn
        pre = mm(pn.astype(BF16), w_dt2[...])
        bias = chan_ref[5:6, :]
        pre = pre + jnp.concatenate([bias, bias], axis=1)
        delta = jnp.maximum(pre, 0.0) + jnp.log1p(jnp.exp(-jnp.abs(pre)))
        dbuf[...] = delta
        dxbuf[...] = delta * xcbuf[ch].astype(F32)

    def stage_ssm(ch, pnbuf, dbuf, dxbuf):
        pn = pnbuf[...]
        lane = lax.broadcasted_iota(jnp.int32, pn.shape, 1)
        is_c = (lane % p_dim) >= dt_rank + state_dim
        first = pn.astype(BF16).astype(F32)
        second = (pn - first).astype(BF16).astype(F32)
        third = pn - first - second
        parts = [jnp.where(is_c, v, 0.0) for v in (first, second, third)]
        split = (parts[0] + pltpu.roll(parts[1], state_dim, 1) + pltpu.roll(parts[2], 2 * state_dim, 1)).astype(BF16)
        skip = chan_ref[6:7, :]

        def at(s):
            return slice((s % 2) * rows, (s % 2 + 1) * rows), slice((s // 2) * inner, (s // 2 + 1) * inner)

        for s in range(steps):
            yacc[s * rows:(s + 1) * rows, :] = skip * xcbuf[(ch, *at(s))].astype(F32)
        for n in range(state_dim):
            c_all = mm(split, spread[:, 2 * n * inner:2 * (n + 1) * inner])
            b_all = [jnp.broadcast_to(pn[:, k:k + 1], (half_rows, inner)) for k in (dt_rank + n, p_dim + dt_rank + n)]
            where = pl.ds(ch * rows * state_dim + n, rows, stride=state_dim)
            h = hbuf[where, :]
            a_n = a2[n:n + 1, :]
            for s in range(steps):
                r, c = at(s)
                h = jnp.exp2(dbuf[r, c] * a_n) * h + dxbuf[r, c] * b_all[s // 2][r]
                yacc[s * rows:(s + 1) * rows, :] += h * c_all[r, c]
            h_ref[where, :] = h
        yg_all[ch, core * 4 + chip] = (yacc[...] * silu(zbuf[ch].astype(F32))).astype(BF16)

    def mid_one(ch):
        mix = mm(jnp.concatenate([yg_all[ch, k] for k in range(yg_all.shape[1])], axis=1), wo_all[...])
        xf = x_ref[:, chunk_rows(ch), :].reshape(tokens, d_model).astype(F32)
        u = (xf + mix).astype(BF16)
        ubuf[ch] = u

    def mid_two(ch, mbuf):
        uf = ubuf[ch].astype(F32)
        scale = lax.rsqrt(jnp.mean(uf * uf, axis=-1, keepdims=True) + EPSILON)
        mbuf[...] = (uf * scale * vec_ref[1:2, :]).astype(BF16)

    def mid_three(ch, mbuf, prob):
        logits = nt_dot(mbuf[...], w_router_ref[...])
        peak = jnp.max(logits, axis=-1, keepdims=True)
        ex = jnp.exp(logits - peak)
        ids = idbuf[:, chunk_rows(ch), 0:experts].reshape(tokens, experts)
        hit = ids == lax.broadcasted_iota(jnp.int32, (tokens, experts), 1)
        chosen = jnp.sum(jnp.where(hit, ex, 0.0), axis=-1, keepdims=True) / jnp.sum(ex, axis=-1, keepdims=True)
        prob[...] = jnp.broadcast_to(chosen, prob.shape)

    def mid_parts(ch, mbuf, prob):
        return [lambda: mid_one(ch), lambda: mid_two(ch, mbuf), lambda: mid_three(ch, mbuf, prob)]

    def stage_experts(ch, g, mbuf, prob, between=()):
        m = mbuf[...]
        ids = idbuf[:, chunk_rows(ch), :].reshape(tokens, inner)
        ids = jnp.concatenate([ids] * (f_loc // inner), axis=1)
        for j in range(GROUP):
            e = g * GROUP + j
            q = silu(mm(m, wg[e])) * mm(m, wu[e])
            qbuf[:, j * f_loc:(j + 1) * f_loc] = jnp.where(ids == e, q, 0.0).astype(BF16)
            if j < len(between):
                between[j]()
        part = mm(qbuf[...], wd[g * GROUP * f_loc:(g + 1) * GROUP * f_loc, :])
        if g == 0:
            acc[...] = part
        elif g < experts // GROUP - 1:
            acc[...] += part
        else:
            total = acc[...] + part
            weight = jnp.concatenate([prob[...]] * (d_model // inner), axis=1)
            y_part[ch] = (total * weight).astype(BF16)

    def when_chunk(ch, fn):
        pl.when((ch >= 0) & (ch < chunks))(lambda: fn(ch))

    def loop(n, body):
        def step(i, carry):
            body(i)
            return carry
        lax.fori_loop(0, n, step, 0)

    w_xp2[...] = jnp.zeros_like(w_xp2)
    w_dt2[...] = jnp.zeros_like(w_dt2)
    for k in range(2):
        w_xp2[k * p_dim:(k + 1) * p_dim, k * inner:(k + 1) * inner] = w_xp_ref[...]
        w_dt2[k * p_dim:k * p_dim + dt_rank, k * inner:(k + 1) * inner] = w_dt_ref[...]
    a2[...] = jnp.exp(a_log_ref[...]) * (-LOG2E)
    w_tmp[...] = w_in_ref[...].astype(F32)
    for k in range(2):
        w_in2[:, k * inner:(k + 1) * inner] = w_tmp[pl.ds(k, d_model, stride=2), :].astype(BF16)
    vec_ref[0:1, :] = g_in_ref[...].astype(F32).reshape(1, d_model)
    vec_ref[1:2, :] = g_ff_ref[...].astype(F32).reshape(1, d_model)
    chan_ref[0:4, :] = conv_w_ref[...].astype(F32)
    chan_ref[4:5, :] = conv_b_ref[...].astype(F32).reshape(1, inner)
    chan_ref[5:6, :] = b_dt_ref[...].astype(F32).reshape(1, inner)
    chan_ref[6:7, :] = d_skip_ref[...].reshape(1, inner)
    gains = [g[...].astype(F32).reshape(1, g.shape[0]) for g in (g_dt_ref, g_b_ref, g_c_ref)]
    chan_ref[7:8, :] = jnp.concatenate(gains + gains, axis=1)
    row = lax.broadcasted_iota(jnp.int32, (2 * p_dim, inner), 0)
    for k in range(2 * state_dim):
        at = (k % 2) * p_dim + dt_rank + state_dim + k // 2
        hit = (row == at) | (row == (at + state_dim) % (2 * p_dim)) | (row == (at + 2 * state_dim) % (2 * p_dim))
        spread[:, k * inner:(k + 1) * inner] = jnp.where(hit, 1.0, 0.0).astype(BF16)
    for s in range(steps):
        idbuf[s] = jnp.broadcast_to(ids_ref[s].astype(F32), (inner, batch)).T.astype(jnp.int32)
    pl.semaphore_wait(barrier, 3)
    wo_first()
    for cp in (h_in, *w_ins):
        cp.start()

    def first_body(t):
        stage_in(t)
        when_chunk(t - 3, p_one)

    loop(chunks, first_body)
    for ch in range(chunks - 3, chunks):
        p_one(ch)
    for ch in range(chunks):
        p_two(ch)
    for ch in range(3):
        p_three(ch)
    ag_relay(wo_block, chunks)
    h_in.wait()

    even, odd = (pn_a, d_a, dx_a), (pn_b, d_b, dx_b)

    def p_done(ch):
        p_ar(ch)[0]["back"].wait_recv()

    gather_plan = (
        [(ag_first, 0)],
        [(ag_first, 1)],
        [],
        [(ag_relay, 0), (ag_first, 2)],
        [(ag_first, 3), (ag_far, None)],
        [(ag_relay, 1), (ag_first, 4)],
        [(ag_first, 5), (ag_far, 0)],
        [(ag_relay, 2)] + [(ag_first, ch) for ch in range(6, chunks)],
    )

    def ssm_tick(t, now, later, parity):
        when_chunk(t + 1, p_done)
        stage_ssm(t, *now)
        stage_norm(jnp.minimum(t + 1, chunks - 1), *later)
        when_chunk(t + 3, p_three)
        for tick, events in enumerate(gather_plan):
            if tick % 2 == parity and events:
                def run(events=events):
                    for fn, ch in events:
                        if ch is None:
                            fn(wo_block, chunks)
                        else:
                            fn(yg_block(ch), ch)
                pl.when(t == tick)(run)

    def ssm_body(t):
        ssm_tick(2 * t, even, odd, 0)
        ssm_tick(2 * t + 1, odd, even, 1)

    p_done(0)
    stage_norm(0, *even)
    loop(chunks // 2, ssm_body)
    wo_in.wait()
    for cp in w_ins:
        cp.wait()
    ag_done(wo_block, chunks)

    def got_yg(ch):
        ag_done(yg_block(ch), ch)

    def moe_tick(t, now, later):
        for g in range(experts // GROUP - 1):
            stage_experts(t, g, *now)
            if g == 0:
                if t >= 1 and 2 * t + 2 < chunks:
                    ag_relay(yg_block(2 * t + 2), 2 * t + 2)
                if t >= 1 and t + 1 < chunks:
                    ag_far(yg_block(t + 1), t + 1)
                if t >= 3:
                    y_two(t - 3)
            elif g == 1:
                if t == 0:
                    ag_far(yg_block(1), 1)
                if 2 * t + 3 < chunks:
                    ag_relay(yg_block(2 * t + 3), 2 * t + 3)
                if t >= 1:
                    y_one(t - 1)
                if t == chunks - 1:
                    y_two(t - 2)
            elif t >= 4:
                y_three(t - 4)
        if later is not None:
            got_yg(t + 1)
        stage_experts(t, experts // GROUP - 1, *now, mid_parts(t + 1, *later) if later is not None else ())
        y_ar(t)[0]["swap"].start()

    even, odd = (m_a, prob_a), (m_b, prob_b)

    got_yg(0)
    for part in mid_parts(0, *even):
        part()
    for t in range(chunks):
        now, later = (even, odd) if t % 2 == 0 else (odd, even)
        pl.when(core >= 0)(functools.partial(moe_tick, t, now, later if t + 1 < chunks else None))
    last = chunks - 1
    quarter = tokens // 4
    pieces = 2
    piece = quarter // pieces

    def last_copy(step, i, src, dst, peers):
        for part, peer in enumerate(peers):
            at = pl.ds(part * quarter + i * piece, piece)
            yield copy_to(src.at[last, at], dst.at[last, at], y_send.at[last], l_recv.at[step, part, i], peer)

    def last_one():
        cs, keep = y_ar(last)
        cs["swap"].wait_recv()
        y_s1[last] = (y_part[last, keep].astype(F32) + y_r0[last].astype(F32)).astype(BF16)
        for i in range(pieces):
            for cp in last_copy(0, i, y_s1, y_r1, (peer_a, peer_b)):
                cp.start()

    def last_two():
        for i in range(pieces):
            for cp in last_copy(0, i, y_s1, y_r1, (peer_a, peer_b)):
                cp.wait_recv()
            for part in range(2):
                at = pl.ds(part * quarter + i * piece, piece)
                y_s2[last, at] = (y_s1[last, at].astype(F32) + y_r1[last, at].astype(F32)).astype(BF16)
            for cp in last_copy(1, i, y_s2, y_r2, (peer_b, peer_a)):
                cp.start()

    def last_three():
        for i in range(pieces):
            for cp in last_copy(1, i, y_s2, y_r2, (peer_b, peer_a)):
                cp.wait_recv()
        cs, keep = y_ar(last)
        moe_sum = y_s2[last].astype(F32) + y_r2[last].astype(F32)
        y_new = (ubuf[last, keep].astype(F32) + moe_sum).astype(BF16)
        y_ref[pl.ds(core * (steps // 2), steps // 2), chunk_rows(last), :] = y_new.reshape(steps // 2, rows, d_model)
        cs["out"].start()

    y_three(last - 3)
    last_one()
    y_two(last - 1)
    y_three(last - 2)
    last_two()
    y_three(last - 1)
    last_three()

    def drain(ch):
        y_four(ch)
        ag_drain(yg_block(ch), ch)
        for cs, _ in (p_ar(ch), y_ar(ch)):
            cs["sent"].wait_send()

    loop(chunks, drain)
    ag_drain(wo_block, chunks)


def store_kernel(y_in, h_in, conv_in, y_out, h_out, conv_out, sem):
    pairs = ((h_in, h_out), (y_in, y_out), (conv_in, conv_out))
    copies = [pltpu.make_async_copy(src, dst, sem.at[i]) for i, (src, dst) in enumerate(pairs)]
    for cp in copies:
        cp.start()
    for cp in copies:
        cp.wait()


def solution(mesh):
    act_spec = P(None, "dp", None)
    state_spec = P("dp", "tp", None)
    in_specs = (act_spec, state_spec, state_spec, act_spec, P(None), P(None, None, "tp"), P("tp", None), P("tp"), P("tp", None), P(None), P(None), P(None), P(None, "tp"), P("tp"), P("tp", None), P("tp"), P("tp", None), P(None), P(None, None), P(None, None, "tp"), P(None, None, "tp"), P(None, "tp", None))
    out_specs = (act_spec, state_spec, state_spec)

    def layer_steps(x_steps, conv_state, ssm_state, expert_ids, g_in, w_in, conv_w, conv_b, w_xp, g_dt, g_b, g_c, w_dt, b_dt, a_log, d_skip, w_out, g_ff, w_router, w_gate, w_up, w_down):
        steps, batch, d_model = x_steps.shape
        inner = w_in.shape[2]
        state_dim = a_log.shape[1]
        experts, _, f_loc = w_gate.shape
        p_dim = w_xp.shape[1]
        rows = CHUNK_ROWS
        chunks = batch // rows
        tokens = steps * rows
        group_inner = w_out.shape[0] * mesh.shape["tp"]

        h_flat = jnp.swapaxes(ssm_state, 1, 2).reshape(batch * state_dim, inner)
        conv_t = jnp.transpose(conv_state, (2, 0, 1))

        any_spec = pl.BlockSpec(memory_space=pl.ANY)
        vmem_spec = pl.BlockSpec(memory_space=pltpu.VMEM)
        half = tokens // 2
        p_half = (chunks, half // 2, 2 * p_dim)
        y_half = (chunks, half, d_model)
        dma = pltpu.SemaphoreType.DMA
        scratch = [
            pltpu.VMEM(h_flat.shape, F32),
            pltpu.VMEM((steps, batch, inner), jnp.int32),
            pltpu.VMEM(w_gate.shape, BF16),
            pltpu.VMEM(w_up.shape, BF16),
            pltpu.VMEM((experts * f_loc, d_model), BF16),
            pltpu.VMEM((d_model, 2 * inner), BF16),
            pltpu.VMEM((2 * d_model, inner), F32),
            pltpu.VMEM((2, d_model), F32),
            pltpu.VMEM((8, inner), F32),
            pltpu.VMEM((2 * p_dim, 2 * inner), BF16),
            pltpu.VMEM((2 * p_dim, 2 * inner), BF16),
            pltpu.VMEM((state_dim, inner), F32),
            pltpu.VMEM((2 * p_dim, 2 * state_dim * inner), BF16),
            pltpu.VMEM((chunks, tokens, inner), BF16),
            pltpu.VMEM((chunks, half, 2 * inner), BF16),
            pltpu.VMEM((tokens, inner), F32),
            pltpu.VMEM((half, 2 * p_dim), F32),
            pltpu.VMEM((half, 2 * inner), F32),
            pltpu.VMEM((half, 2 * inner), F32),
            pltpu.VMEM((half, 2 * p_dim), F32),
            pltpu.VMEM((half, 2 * inner), F32),
            pltpu.VMEM((half, 2 * inner), F32),
            pltpu.VMEM((chunks, half, 2 * p_dim), F32),
            pltpu.VMEM(p_half, F32),
            pltpu.VMEM(p_half, F32),
            pltpu.VMEM(p_half, F32),
            pltpu.VMEM(p_half, F32),
            pltpu.VMEM(p_half, F32),
            pltpu.VMEM((chunks, half, 2 * p_dim), F32),
            pltpu.VMEM((chunks, group_inner // inner, tokens, inner), BF16),
            pltpu.VMEM((group_inner, d_model), BF16),
            pltpu.VMEM((chunks, tokens, d_model), BF16),
            pltpu.VMEM((tokens, d_model), BF16),
            pltpu.VMEM((tokens, d_model), BF16),
            pltpu.VMEM((tokens, GROUP * f_loc), BF16),
            pltpu.VMEM((tokens, d_model), F32),
            pltpu.VMEM((tokens, inner), F32),
            pltpu.VMEM((tokens, inner), F32),
            pltpu.VMEM((chunks, tokens, d_model), BF16),
            pltpu.VMEM(y_half, BF16),
            pltpu.VMEM(y_half, BF16),
            pltpu.VMEM(y_half, BF16),
            pltpu.VMEM(y_half, BF16),
            pltpu.VMEM(y_half, BF16),
            dma((6,)),
            dma((chunks,)),
            dma((chunks, 4)),
            dma((chunks,)),
            dma((chunks, 4)),
            dma((2, 2, 2)),
            dma((chunks + 1,)),
            dma((chunks + 1, 4)),
        ]
        y, h_new, conv_new = pl.pallas_call(
            layer_kernel,
            out_shape=(
                pltpu.VMEM(x_steps.shape, BF16),
                pltpu.VMEM(h_flat.shape, F32),
                pltpu.VMEM(conv_t.shape, BF16),
            ),
            in_specs=[vmem_spec] + [any_spec] * 5 + [vmem_spec] * 16,
            out_specs=(vmem_spec,) * 3,
            scratch_shapes=scratch,
            compiler_params=pltpu.CompilerParams(collective_id=0, has_side_effects=True, vmem_limit_bytes=57 * 1024 * 1024),
        )(
            x_steps, h_flat, w_gate, w_up, w_down.reshape(experts * f_loc, d_model), w_out,
            jnp.transpose(expert_ids, (0, 2, 1)), conv_t, w_in.reshape(2 * d_model, inner), g_in, g_ff, conv_w.T, conv_b, b_dt, d_skip,
            g_dt, g_b, g_c, w_xp.T, w_dt, a_log.T, w_router.T,
        )
        y, h_new, conv_new = pl.pallas_call(
            store_kernel,
            out_shape=[jax.ShapeDtypeStruct(v.shape, v.dtype) for v in (y, h_new, conv_new)],
            in_specs=[vmem_spec] * 3,
            out_specs=[any_spec] * 3,
            scratch_shapes=[dma((3,))],
            compiler_params=pltpu.CompilerParams(vmem_limit_bytes=1024 * 1024),
        )(*(pltpu.with_memory_space_constraint(v, pltpu.VMEM) for v in (y, h_new, conv_new)))
        h_new = jnp.swapaxes(h_new.reshape(batch, state_dim, inner), 1, 2)
        return y, jnp.transpose(conv_new, (1, 2, 0)), h_new

    return jax.shard_map(layer_steps, mesh=mesh, in_specs=in_specs, out_specs=out_specs, check_vma=False)
```
